16 devices in a mesh: col: 4 (over z, y), row: 4 (over x, core).
Axes of the slice: x: 2, y: 2, z: 2, core: 2. Of those that a mesh axis runs over, the one named last changes fastest.
Arguments:
- vel_x: float32 [60, 2, 128, 1024], P(None, None, 'row', 'col')
- vel_y: float32 [60, 2, 128, 1024], P(None, None, 'row', 'col')
- pot_temp: float32 [60, 2, 128, 1024], P(None, None, 'row', 'col')
- salinity: float32 [60, 2, 128, 1024], P(None, None, 'row', 'col')
- surf_eta: float32 [2, 128, 1024], P(None, 'row', 'col')
- trans_x: float32 [2, 128, 1024], P(None, 'row', 'col')
- trans_y: float32 [2, 128, 1024], P(None, 'row', 'col')
- col_depth: float32 [128, 1024], P('row', 'col')
- wet_levels: int32 [128, 1024], P('row', 'col')
- avg_weights: float32 [40], replicated
Outputs:
- output 1: float32 [2, 128, 1024], P(None, 'row', 'col')
- output 2: float32 [2, 128, 1024], P(None, 'row', 'col')
- output 3: float32 [2, 128, 1024], P(None, 'row', 'col')
- output 4: float32 [60, 2, 128, 1024], P(None, None, 'row', 'col')
- output 5: float32 [60, 2, 128, 1024], P(None, None, 'row', 'col')
- output 6: float32 [60, 2, 128, 1024], P(None, None, 'row', 'col')
- output 7: float32 [60, 2, 128, 1024], P(None, None, 'row', 'col')
All inputs are finite; a program needn't handle non-finite values.
Results may differ from the reference program's by a relative error of at most 0.001.
Values sent between devices are 32-bit elements.
A program may use at most 1 GiB of HBM per device.

```python
import jax
import jax.numpy as jnp
from jax import lax

MEMBERS = 2
LEVELS = 60
SUBCYCLES = 40
GRID_Y = 128
GRID_X = 1024

WAVE_COURANT = 0.4
THERM_EXP = 0.2
HALINE_CON = 0.15
PRESS_SCALE = 0.5
VISC_NUMBER = 1.0
DIFF_NUMBER = 0.5


def east_of(field_in):
    return jnp.roll(field_in, -1, axis=-1)


def west_of(field_in):
    return jnp.roll(field_in, 1, axis=-1)


def north_of(field_in):
    return jnp.concatenate([field_in[..., 1:, :], jnp.zeros_like(field_in[..., :1, :])], axis=-2)


def south_of(field_in):
    return jnp.concatenate([jnp.zeros_like(field_in[..., :1, :]), field_in[..., :-1, :]], axis=-2)


def wet_masks(wet_levels, level_total):
    levels = jnp.arange(level_total).reshape(level_total, 1, 1, 1)
    cell_mask = (levels < wet_levels).astype(jnp.float32)
    xface_mask = cell_mask * (levels < east_of(wet_levels)).astype(jnp.float32)
    yface_mask = cell_mask * (levels < north_of(wet_levels)).astype(jnp.float32)
    return cell_mask, xface_mask, yface_mask


def setup_inputs(seed: int = 0) -> dict:
    key_list = jax.random.split(jax.random.key(seed), 12)
    shape_3d = (LEVELS, MEMBERS, GRID_Y, GRID_X)
    shape_2d = (MEMBERS, GRID_Y, GRID_X)
    land_draw = jax.random.randint(key_list[0], (GRID_Y, GRID_X), 0, 10)
    depth_draw = jax.random.randint(key_list[1], (GRID_Y, GRID_X), 1, LEVELS + 1)
    wet_levels = jnp.where(land_draw == 0, 0, jnp.where(land_draw < 5, LEVELS, depth_draw)).astype(jnp.int32)
    cell_mask, xface_mask, yface_mask = wet_masks(wet_levels, LEVELS)
    profile = jnp.cos(jnp.pi * (jnp.arange(LEVELS) + 0.5) / LEVELS).reshape(LEVELS, 1, 1, 1)

    def tracer_field(key_pair):
        key_a, key_b, key_c = jax.random.split(key_pair, 3)
        base_field = jax.random.normal(key_a, shape_2d, jnp.float32)
        mode_field = jax.random.normal(key_b, shape_2d, jnp.float32)
        noise_3d = jax.random.normal(key_c, shape_3d, jnp.float32)
        return cell_mask * (base_field + mode_field * profile + 0.3 * noise_3d)

    vel_x = xface_mask * 0.3 * jax.random.normal(key_list[2], shape_3d, jnp.float32)
    vel_y = yface_mask * 0.3 * jax.random.normal(key_list[3], shape_3d, jnp.float32)
    pot_temp = tracer_field(key_list[4])
    salinity = tracer_field(key_list[5])
    surf_eta = cell_mask[0] * 0.3 * jax.random.normal(key_list[6], shape_2d, jnp.float32)
    trans_x = xface_mask[0] * 0.3 * jax.random.normal(key_list[7], shape_2d, jnp.float32)
    trans_y = yface_mask[0] * 0.3 * jax.random.normal(key_list[8], shape_2d, jnp.float32)
    col_depth = 0.5 + 1.5 * jax.random.uniform(key_list[9], (GRID_Y, GRID_X), jnp.float32)
    step_frac = (jnp.arange(SUBCYCLES) + 1.0) / SUBCYCLES
    raw_weights = step_frac * step_frac * (2.0 - step_frac * step_frac) * (0.3 + 1.4 * jax.random.uniform(key_list[10], (SUBCYCLES,), jnp.float32))
    avg_weights = raw_weights / jnp.sum(raw_weights)
    return {"vel_x": vel_x, "vel_y": vel_y, "pot_temp": pot_temp, "salinity": salinity, "surf_eta": surf_eta, "trans_x": trans_x, "trans_y": trans_y, "col_depth": col_depth, "wet_levels": wet_levels, "avg_weights": avg_weights}


def vertical_solve(right_side, face_mask, strength):
    mask_below = jnp.concatenate([face_mask[1:], jnp.zeros_like(face_mask[:1])], axis=0)
    face_up = face_mask * mask_below
    face_down = jnp.concatenate([jnp.zeros_like(face_up[:1]), face_up[:-1]], axis=0)
    lower_diag = -strength * face_down
    upper_diag = -strength * face_up
    main_diag = 1.0 + strength * (face_down + face_up)

    def forward(state_prev, level_row):
        upper_prev, side_prev = state_prev
        low_k, diag_k, up_k, side_k = level_row
        divisor = diag_k - low_k * upper_prev
        upper_new = up_k / divisor
        side_new = (side_k - low_k * side_prev) / divisor
        return (upper_new, side_new), (upper_new, side_new)

    zero_level = jnp.zeros_like(right_side[0])
    upper_all, side_all = lax.scan(forward, (zero_level, zero_level), (lower_diag, main_diag, upper_diag, right_side))[1]

    def backward(sol_next, level_row):
        up_k, side_k = level_row
        sol_k = side_k - up_k * sol_next
        return sol_k, sol_k

    return lax.scan(backward, zero_level, (upper_all, side_all), reverse=True)[1]


def tracer_step(tracer, vel_x, vel_y, cell_mask):
    flux_x = vel_x * 0.5 * (tracer + east_of(tracer))
    flux_y = vel_y * 0.5 * (tracer + north_of(tracer))
    advected = cell_mask * (tracer - (flux_x - west_of(flux_x) + flux_y - south_of(flux_y)))
    return vertical_solve(advected, cell_mask, DIFF_NUMBER)


def barotropic(surf_eta, trans_x, trans_y, force_x, force_y, depth_x, depth_y, wet_top, xface_top, yface_top, avg_weights):
    sub_count = avg_weights.shape[0]
    step_x = force_x / sub_count
    step_y = force_y / sub_count

    def subcycle(sub_state, weight):
        eta_now, tx_now, ty_now, eta_avg, tx_avg, ty_avg = sub_state
        eta_now = wet_top * (eta_now - WAVE_COURANT * (tx_now - west_of(tx_now) + ty_now - south_of(ty_now)))
        tx_now = xface_top * (tx_now + step_x - WAVE_COURANT * depth_x * (east_of(eta_now) - eta_now))
        ty_now = yface_top * (ty_now + step_y - WAVE_COURANT * depth_y * (north_of(eta_now) - eta_now))
        return (eta_now, tx_now, ty_now, eta_avg + weight * eta_now, tx_avg + weight * tx_now, ty_avg + weight * ty_now), None

    zero_field = jnp.zeros_like(surf_eta)
    end_state = lax.scan(subcycle, (surf_eta, trans_x, trans_y, zero_field, zero_field, zero_field), avg_weights)[0]
    return end_state[3], end_state[4], end_state[5]


def reference(vel_x, vel_y, pot_temp, salinity, surf_eta, trans_x, trans_y, col_depth, wet_levels, avg_weights):
    level_count = vel_x.shape[0]
    cell_mask, xface_mask, yface_mask = wet_masks(wet_levels, level_count)
    density = HALINE_CON * salinity - THERM_EXP * pot_temp
    pressure = (PRESS_SCALE / level_count) * (jnp.cumsum(density, axis=0) - 0.5 * density)
    vy_south = south_of(vel_y)
    vx_north = north_of(vel_x)
    vy_at_x = 0.25 * (vel_y + vy_south + east_of(vel_y) + east_of(vy_south))
    vx_at_y = 0.25 * (vel_x + west_of(vel_x) + vx_north + west_of(vx_north))
    tend_x = xface_mask * (pressure - east_of(pressure) - 0.5 * vel_x * (east_of(vel_x) - west_of(vel_x)) - 0.5 * vy_at_x * (vx_north - south_of(vel_x)))
    tend_y = yface_mask * (pressure - north_of(pressure) - 0.5 * vx_at_y * (east_of(vel_y) - west_of(vel_y)) - 0.5 * vel_y * (north_of(vel_y) - vy_south))
    count_x = jnp.maximum(jnp.sum(xface_mask, axis=0), 1.0)
    count_y = jnp.maximum(jnp.sum(yface_mask, axis=0), 1.0)
    depth_x = 0.5 * (col_depth + east_of(col_depth)) * xface_mask[0]
    depth_y = 0.5 * (col_depth + north_of(col_depth)) * yface_mask[0]
    force_x = depth_x * jnp.sum(tend_x, axis=0) / count_x
    force_y = depth_y * jnp.sum(tend_y, axis=0) / count_y
    pred_x = vertical_solve(vel_x + tend_x, xface_mask, VISC_NUMBER)
    pred_y = vertical_solve(vel_y + tend_y, yface_mask, VISC_NUMBER)
    temp_new = tracer_step(pot_temp, vel_x, vel_y, cell_mask)
    salt_new = tracer_step(salinity, vel_x, vel_y, cell_mask)
    eta_new, trans_x_new, trans_y_new = barotropic(surf_eta, trans_x, trans_y, force_x, force_y, depth_x, depth_y, cell_mask[0], xface_mask[0], yface_mask[0], avg_weights)
    vel_x_new = xface_mask * (pred_x - jnp.sum(pred_x, axis=0) / count_x + trans_x_new / (depth_x + 1.0 - xface_mask[0]))
    vel_y_new = yface_mask * (pred_y - jnp.sum(pred_y, axis=0) / count_y + trans_y_new / (depth_y + 1.0 - yface_mask[0]))
    return eta_new, trans_x_new, trans_y_new, vel_x_new, vel_y_new, temp_new, salt_new
```

```python
import functools
import jax
import jax.numpy as jnp
import numpy as np
from jax import lax
from jax.experimental import pallas as pl
from jax.experimental.pallas import tpu as pltpu
from jax.sharding import PartitionSpec as P

MESH = pl.DeviceIdType.MESH
F32 = jnp.float32
NK = 60
NM = 2
NY = 32
NL = 128
NS = 8
VR = (NS, NL)
NX = 256
NT = NX // NL
NJ = NY // 8
CH = 10
NC = NK // CH
HALO = 40
WY = 2 * NY + HALO
WJ = WY // 8
WT = 3
NSUB = 40
COURANT = 0.4
VMEM_LIMIT = 42 << 20
SIDE = 40

VM = pl.BlockSpec(memory_space=pltpu.VMEM)
SM = pl.BlockSpec(memory_space=pltpu.SMEM)
ANY = pl.BlockSpec(memory_space=pl.ANY)


def level_table():
    rows = np.zeros((4, NK), np.float64)
    for row, strength in ((0, 1.0), (2, 0.5)):
        scale = 1.0 if strength == 1.0 else 0.5
        div_prev = 0.0
        for k in range(NK):
            if k == 0:
                div = 1.0 + strength
            else:
                div = 1.0 + 2.0 * strength - strength * strength / div_prev
            rows[row, k] = scale / div
            rows[row + 1, k] = scale / (div - strength)
            div_prev = div
    return jnp.asarray(rows, F32)


def lanes_iota():
    return lax.broadcasted_iota(jnp.int32, VR, 1)


def subl_iota():
    return lax.broadcasted_iota(jnp.int32, VR, 0)


def device(col, row):
    return {"col": col, "row": row}


def greet(col, row):
    barrier = pltpu.get_barrier_semaphore()
    count = 0
    for dc in (0, 1, 3):
        for dr in range(4):
            if dc == 0 and dr == 0:
                continue
            pl.semaphore_signal(barrier, inc=1, device_id=device(lax.rem(col + dc, 4), lax.rem(row + dr, 4)), device_id_type=MESH)
            count += 1
    pl.semaphore_wait(barrier, count)


class Exchange:
    def __init__(self, src_main, src_side, main, side, send_sem, recv_sem, col, row):
        chip = row // 2
        core = lax.rem(row, 2)
        east = lax.rem(col + 1, 4)
        west = lax.rem(col + 3, 4)
        self.full = chip != core
        self.main, self.side, self.recv_sem = main, side, recv_sem
        own = pl.ds(pl.multiple_of(core * NY, NS), NY)
        at_full = pl.ds(pl.multiple_of(jnp.where(chip == 1, 2 * NY, NY + HALO), NS), NY)
        at_part = pl.ds(pl.multiple_of(jnp.where(chip == 1, 3 * NY, 2 * NY), NS), NS)
        from_part = pl.ds(pl.multiple_of(jnp.where(chip == 1, 0, NY - NS), NS), NS)
        self.count = 0

        def remote(s, d, kind, dev):
            return pltpu.make_async_remote_copy(src_ref=s, dst_ref=d, send_sem=send_sem.at[self.count], recv_sem=recv_sem.at[kind], device_id=dev, device_id_type=MESH)

        self.always, self.whole, self.part = [], [], []
        self.local = pltpu.make_async_copy(src_main.at[core], main.at[:, :, own], recv_sem.at[0])
        self.always.append(remote(src_main.at[1 - core], main.at[:, :, own], 0, device(col, chip * 2 + 1 - core)))
        for mm in range(NM):
            near, far = chip * 2 + mm, (1 - chip) * 2 + mm
            self.count += 1
            self.whole.append(remote(src_main.at[mm], main.at[:, :, at_full], 0, device(col, far)))
            self.part.append(remote(src_main.at[mm, :, :, from_part], main.at[:, :, at_part], 0, device(col, far)))
            for e, dev in enumerate((west, east)):
                self.count += 1
                self.whole.append(remote(src_side.at[mm, e], side.at[e, :, at_full], 1, device(dev, far)))
                self.part.append(remote(src_side.at[mm, e, :, from_part], side.at[e, :, at_part], 1, device(dev, far)))
                self.count += 1
                self.always.append(remote(src_side.at[mm, e], side.at[e, :, own], 1, device(dev, near)))

    def branch(self, op):
        @pl.when(self.full)
        def _():
            for copy in self.whole:
                getattr(copy, op)()

        @pl.when(jnp.logical_not(self.full))
        def _():
            for copy in self.part:
                getattr(copy, op)()

    def start(self):
        self.branch("start")
        for copy in self.always:
            copy.start()
        self.local.start()

    def wait(self):
        pltpu.make_async_copy(self.main, self.main, self.recv_sem.at[0]).wait()
        pltpu.make_async_copy(self.side, self.side, self.recv_sem.at[1]).wait()
        for copy in self.always:
            copy.wait_send()
        self.branch("wait_send")


def pack_side(dst, m, group, fields, lane):
    for i in range(NY // NS):
        rows = pl.ds(i * NS, NS)
        first = fields[0](0, rows)
        last = fields[0](NT - 1, rows)
        for n in range(1, len(fields)):
            first = jnp.where(lane < n * SIDE, first, pltpu.roll(fields[n](0, rows), n * SIDE, 1))
            last = jnp.where(lane >= NL - n * SIDE, last, pltpu.roll(fields[n](NT - 1, rows), NL - n * SIDE, 1))
        dst[m, 0, group, rows] = first
        dst[m, 1, group, rows] = last


def window_tile(main, side, f, j, t, lane, group, place):
    here = pl.ds(j, NS, stride=WJ)
    if t < NT:
        return main.at[f, t][here, :]
    e, w = side.at[0, group][here, :], side.at[1, group][here, :]
    if place:
        e, w = pltpu.roll(e, NL - place * SIDE, 1), pltpu.roll(w, place * SIDE, 1)
    return jnp.where(lane < SIDE, e, jnp.where(lane >= NL - SIDE, w, 0.0))


PA = 0.15 * 0.5 / NK * 0.5
PB = 0.2 * 0.5 / NK * 0.5
MOM_UNROLL = 1
TRC_UNROLL = 3


def step_kernel(u, v, temp, salt, eta, tx, ty, depth, wet, weights, tab,
                sbuf, bsum, kl, rl, out,
                inb, hE, hW, hN, hS, hSE, hNW, colF, colL, rowF, rowL, ksrc, kE, kN,
                wmain, wside, main, side, gsum, fmain, fside, fwin, fwside, wi, nat, state, res,
                in_sem, sendC, recvE, recvW, sendR, recvN, recvS, corn_send, corn_recv, k_send, k_recv,
                w_send, w_recv, f_send, f_recv, out_send, out_recv, loc_sem):
    col = lax.axis_index("col")
    row = lax.axis_index("row")
    chip = row // 2
    core = lax.rem(row, 2)
    east_dev = lax.rem(col + 1, 4)
    west_dev = lax.rem(col + 3, 4)
    north_dev = jnp.minimum(row + 1, 3)
    south_dev = jnp.maximum(row - 1, 0)
    has_north = row < 3
    has_south = row > 0
    fields = (u, v, temp, salt)
    lane = lanes_iota()
    subl = subl_iota()
    l_last, l_first = lane == NL - 1, lane == 0
    s_last, s_first = subl == NS - 1, subl == 0
    zero = jnp.zeros(VR, F32)

    def load(f, m, t, c):
        part = pl.ds(c * CH, CH)
        return pltpu.make_async_copy(fields[f].at[part, m, :, pl.ds(t * NL, NL)], inb.at[f, m, t, part], in_sem.at[f, m, t, c])

    def each_load(f, c, op):
        for m in range(NM):
            for t in range(NT):
                getattr(load(f, m, t, c), op)()

    for f in range(4):
        for c in range(NC):
            each_load(f, c, "start")

    for t in range(NT):
        ksrc[t] = wet[:, pl.ds(t * NL, NL)].astype(F32)

    greet(col, row)

    def remote(s, d, ssem, rsem, dc, dr):
        return pltpu.make_async_remote_copy(src_ref=s, dst_ref=d, send_sem=ssem, recv_sem=rsem, device_id=device(dc, dr), device_id_type=MESH)

    k_west = remote(ksrc.at[0], kE, k_send.at[0], k_recv.at[0], west_dev, row)
    k_south = remote(ksrc.at[:, pl.ds(0, NS)], kN, k_send.at[1], k_recv.at[1], col, south_dev)

    def col_copies(f):
        return (remote(colF.at[f], hE.at[f], sendC.at[0, f], recvE.at[f], west_dev, row),
                remote(colL.at[f], hW.at[f], sendC.at[1, f], recvW.at[f], east_dev, row))

    def to_south(f):
        return remote(rowF.at[f], hN.at[f], sendR.at[0, f], recvN.at[f], col, south_dev)

    def to_north(f):
        return remote(rowL.at[f], hS.at[f], sendR.at[1, f], recvS.at[f], col, north_dev)

    corner_north = remote(colF.at[1, pl.ds(NY - NS, NS)], hSE, corn_send.at[0], corn_recv.at[0], west_dev, north_dev)
    corner_south = remote(colL.at[0, pl.ds(0, NS)], hNW, corn_send.at[1], corn_recv.at[1], east_dev, south_dev)

    k_west.start()

    @pl.when(has_south)
    def _():
        k_south.start()

    half_lane = NL // 2
    for f in range(4):
        def chunk(c, acc, f=f):
            each_load(f, c, "wait")
            acc = list(acc)
            for q in range(CH):
                k = c * CH + q
                for m in range(NM):
                    spot = k + half_lane * m
                    hit = lane == spot
                    for i in range(NJ):
                        rows = pl.ds(i * NS, NS)
                        first = pltpu.roll(inb[f, m, 0, k, rows], spot, 1)
                        last = pltpu.roll(inb[f, m, NT - 1, k, rows], lax.rem(spot + 1, NL), 1)
                        acc[2 * i] = jnp.where(hit, first, acc[2 * i])
                        acc[2 * i + 1] = jnp.where(hit, last, acc[2 * i + 1])
                    for t in range(NT):
                        rowF[f, t, pl.ds(m * NK + k, 1), :] = inb[f, m, t, k, 0:1]
                        rowL[f, t, pl.ds(m * NK + k, 1), :] = inb[f, m, t, k, NY - 1:NY]
            return tuple(acc)

        acc = lax.fori_loop(0, NC, chunk, (zero,) * (2 * NJ))
        for i in range(NJ):
            colF[f, pl.ds(i * NS, NS)] = acc[2 * i]
            colL[f, pl.ds(i * NS, NS)] = acc[2 * i + 1]

        @pl.when(has_south)
        def _():
            to_south(f).start()

        @pl.when(has_north)
        def _():
            to_north(f).start()
        for copy in col_copies(f):
            copy.start()
        if f == 0:
            @pl.when(has_south)
            def _():
                corner_south.start()
        if f == 1:
            @pl.when(has_north)
            def _():
                corner_north.start()

    for m in range(NM):
        for t in range(NT):
            cols = pl.ds(t * NL, NL)
            for i, arr in enumerate((eta, tx, ty)):
                wmain[m, i, t] = arr[m, :, cols]
            wmain[m, 3, t] = depth[:, cols]
            wmain[m, 4, t] = ksrc[t]
        reads = [lambda t, rows, m=m, i=i: wmain[m, i, t, rows] for i in range(5)]
        pack_side(wside, m, 0, reads[:3], lane)
        pack_side(wside, m, 1, reads[3:], lane)
    windows = Exchange(wmain, wside, main, side, w_send, w_recv, col, row)
    windows.start()

    @pl.when(jnp.logical_not(has_north))
    def _():
        hN[...] = jnp.zeros(hN.shape, F32)
        hNW[...] = jnp.zeros(hNW.shape, F32)
        kN[...] = jnp.zeros(kN.shape, F32)

    @pl.when(jnp.logical_not(has_south))
    def _():
        hS[...] = jnp.zeros(hS.shape, F32)
        hSE[...] = jnp.zeros(hSE.shape, F32)

    for f in range(4):
        for m in range(NM):
            for i in range(NJ * NT):
                sbuf[f, m, 0, i] = zero
    for f in range(2):
        for m in range(NM):
            for i in range(NJ * NT):
                gsum[f, m, i] = zero
                bsum[f, m, i] = zero

    k_west.wait()

    @pl.when(has_south)
    def _():
        k_south.wait_send()
        corner_south.wait_send()
        corner_north.wait_recv()

    @pl.when(has_north)
    def _():
        k_south.wait_recv()
        corner_north.wait_send()
        corner_south.wait_recv()

    for f in range(4):
        for copy in col_copies(f):
            copy.wait()

        @pl.when(has_south)
        def _():
            to_south(f).wait_send()
            to_north(f).wait_recv()

        @pl.when(has_north)
        def _():
            to_north(f).wait_send()
            to_south(f).wait_recv()

    def rolls(x, amount):
        return [[pltpu.roll(x[j][t], amount, 1) for t in range(NT)] for j in range(NJ)]

    def east(x, halo):
        r = rolls(x, NL - 1)
        return [[jnp.where(l_last, r[j][1] if t == 0 else halo[j], r[j][t]) for t in range(NT)] for j in range(NJ)]

    def west(x, halo):
        r = rolls(x, 1)
        return [[jnp.where(l_first, r[j][0] if t == 1 else halo[j], r[j][t]) for t in range(NT)] for j in range(NJ)]

    def north(x, halo):
        return x[1:] + [[jnp.where(s_last, halo[t], pltpu.roll(x[0][t], NS - 1, 0)) for t in range(NT)]]

    def south(x, halo):
        return [[jnp.where(s_first, halo[t], pltpu.roll(x[NJ - 1][t], 1, 0)) for t in range(NT)]] + x[:-1]

    def zipped(fn, *xs):
        return [[fn(*[x[j][t] for x in xs]) for t in range(NT)] for j in range(NJ)]

    def strided(ref):
        return [ref[pl.ds(j, NS, stride=NJ), :] for j in range(NJ)]

    k_mid = zipped(lambda x: x, [list(pair) for pair in zip(*[strided(ksrc.at[t]) for t in range(NT)])])
    k_east = zipped(jnp.minimum, k_mid, east(k_mid, [pltpu.roll(x, NL - 1, 1) for x in strided(kE)]))
    k_north = zipped(jnp.minimum, k_mid, north(k_mid, [kN.at[t][pl.ds(0, NS, stride=0), :] for t in range(NT)]))
    for n, mask in enumerate((k_mid, k_east, k_north)):
        for j in range(NJ):
            for t in range(NT):
                kl[n, j * NT + t] = mask[j][t].astype(jnp.int32)

    def read_mask(n):
        return [[kl[n, j * NT + t] for t in range(NT)] for j in range(NJ)]

    def factors(mask, k, a, b):
        return zipped(lambda n: jnp.where(n > k + 1, a, jnp.where(n == k + 1, b, 0.0)), mask)

    def block(f, m, k):
        return [[inb.at[f, m, t, k][pl.ds(j, NS, stride=NJ), :] for t in range(NT)] for j in range(NJ)]

    def line(ref, f, m, k):
        return [ref.at[f, t][pl.ds(m * NK + k, NS, stride=0), :] for t in range(NT)]

    def amounts(m, k):
        return NL - 1 - half_lane * m - k, lax.rem(NL - half_lane * m - k, NL)

    def edge(ref, f, amount):
        return [pltpu.roll(x, amount, 1) for x in strided(ref.at[f])]

    def solve(f, m, k, side_k, scale):
        for j in range(NJ):
            for t in range(NT):
                i = j * NT + t
                sbuf[f, m, k + 1, i] = (side_k[j][t] + sbuf[f, m, k, i]) * scale[j][t]

    def momentum(m, k, carry, wet_x, wet_y, inv_x, inv_y):
        cs, cs_n, cs_e = carry
        uu, vv, tt, ss = (block(f, m, k) for f in range(4))
        to_last, to_first = amounts(m, k)
        eu, ev, et, es = (edge(hE, f, to_last) for f in range(4))
        wu, wv = (edge(hW, f, to_first) for f in range(2))
        nu, nv, nt, ns = (line(hN, f, m, k) for f in range(4))
        su, sv = (line(hS, f, m, k) for f in range(2))
        c_se = pltpu.roll(hSE[pl.ds(NS - 1, NS, stride=0), :], to_last, 1)
        c_nw = pltpu.roll(hNW[pl.ds(0, NS, stride=0), :], to_first, 1)

        half = zipped(lambda s, t: PA * s - PB * t, ss, tt)
        p = zipped(jnp.add, cs, half)
        cs = zipped(jnp.add, p, half)
        half_n = [PA * ns[t] - PB * nt[t] for t in range(NT)]
        p_n = [cs_n[t] + half_n[t] for t in range(NT)]
        cs_n = [p_n[t] + half_n[t] for t in range(NT)]
        half_e = [PA * es[j] - PB * et[j] for j in range(NJ)]
        p_e = [cs_e[j] + half_e[j] for j in range(NJ)]
        cs_e = [p_e[j] + half_e[j] for j in range(NJ)]

        u_e, u_w, v_e, v_w = east(uu, eu), west(uu, wu), east(vv, ev), west(vv, wv)
        u_n, u_s, v_n, v_s = north(uu, nu), south(uu, su), north(vv, nv), south(vv, sv)
        r = [pltpu.roll(sv[t], NL - 1, 1) for t in range(NT)]
        sve = [jnp.where(l_last, r[1], r[0]), jnp.where(l_last, c_se, r[1])]
        r = [pltpu.roll(nu[t], 1, 1) for t in range(NT)]
        nuw = [jnp.where(l_first, c_nw, r[0]), jnp.where(l_first, r[0], r[1])]
        a = zipped(jnp.add, vv, v_e)
        v_sum = zipped(jnp.add, a, south(a, [sv[t] + sve[t] for t in range(NT)]))
        b = zipped(jnp.add, uu, u_w)
        u_sum = zipped(jnp.add, b, north(b, [nu[t] + nuw[t] for t in range(NT)]))
        p_e = east(p, p_e)
        p_n = north(p, p_n)

        gu = zipped(lambda w, p, pe, u, ue, uw, vs, un, us: jnp.where(w, (p - pe) - 0.5 * (u * (ue - uw)) - 0.125 * (vs * (un - us)), 0.0),
                    wet_x, p, p_e, uu, u_e, u_w, v_sum, u_n, u_s)
        gv = zipped(lambda w, p, pn, us, ve, vw, v, vn, vs: jnp.where(w, (p - pn) - 0.125 * (us * (ve - vw)) - 0.5 * (v * (vn - vs)), 0.0),
                    wet_y, p, p_n, u_sum, v_e, v_w, vv, v_n, v_s)
        bu = zipped(jnp.add, uu, gu)
        bv = zipped(jnp.add, vv, gv)
        solve(0, m, k, bu, inv_x)
        solve(1, m, k, bv, inv_y)
        for f, (g, b) in enumerate(((gu, bu), (gv, bv))):
            for j in range(NJ):
                for t in range(NT):
                    i = j * NT + t
                    gsum[f, m, i] = gsum[f, m, i] + g[j][t]
                    bsum[f, m, i] = bsum[f, m, i] + b[j][t]
        return cs, cs_n, cs_e

    def momentum_levels(q, carry):
        for h in range(MOM_UNROLL):
            k = q * MOM_UNROLL + h
            mask_x, mask_y = read_mask(1), read_mask(2)
            a1, b1 = tab[0, k], tab[1, k]
            inv = factors(mask_x, k, a1, b1), factors(mask_y, k, a1, b1)
            wet_k = [zipped(lambda n: n > k, mask) for mask in (mask_x, mask_y)]
            carry = tuple(momentum(m, k, carry[m], *wet_k, *inv) for m in range(NM))
        return carry

    start = ([[zero] * NT for _ in range(NJ)], [zero] * NT, [zero] * NJ)
    lax.fori_loop(0, NK // MOM_UNROLL, momentum_levels, (start, start))

    for f in range(2):
        for m in range(NM):
            for t in range(NT):
                for j in range(NJ):
                    fmain.at[m, f, t][pl.ds(j, NS, stride=NJ), :] = gsum[f, m, j * NT + t]
    for m in range(NM):
        pack_side(fside, m, 0, [lambda t, rows, m=m, f=f: fmain[m, f, t, rows] for f in range(2)], lane)
    forces = Exchange(fmain, fside, fwin, fwside, f_send, f_recv, col, row)
    forces.start()

    def tracer(f, m, k, uu, vv, wu, sv, inv_c):
        to_last, to_first = amounts(m, k)
        x = block(f, m, k)
        x_e = east(x, edge(hE, f, to_last))
        x_n = north(x, line(hN, f, m, k))
        w_halo, s_halo = edge(hW, f, to_first), line(hS, f, m, k)
        fx = zipped(lambda u, a, b: u * (a + b), uu, x, x_e)
        fy = zipped(lambda v, a, b: v * (a + b), vv, x, x_n)
        fx_w = west(fx, [wu[j] * (w_halo[j] + x[j][0]) for j in range(NJ)])
        fy_s = south(fy, [sv[t] * (s_halo[t] + x[0][t]) for t in range(NT)])
        solve(f, m, k, zipped(lambda a, f, fw, g, gs: (a + a) - (f - fw) - (g - gs), x, fx, fx_w, fy, fy_s), inv_c)

    def tracer_levels(q, carry):
        for h in range(TRC_UNROLL):
            k = q * TRC_UNROLL + h
            inv_c = factors(read_mask(0), k, tab[2, k], tab[3, k])
            for m in range(NM):
                uu, vv = block(0, m, k), block(1, m, k)
                wu, sv = edge(hW, 0, amounts(m, k)[1]), line(hS, 1, m, k)
                for f in (2, 3):
                    tracer(f, m, k, uu, vv, wu, sv, inv_c)
        return carry

    lax.fori_loop(0, NK // TRC_UNROLL, tracer_levels, 0)

    windows.wait()
    dep = [[window_tile(main, side, 3, j, t, lane, 1, 0) for t in range(WT)] for j in range(WJ)]
    lev = [[window_tile(main, side, 4, j, t, lane, 1, 1) for t in range(WT)] for j in range(WJ)]
    for j in range(WJ):
        row_here = WJ * subl + j
        wall = jnp.logical_and(row_here == 2 * NY - 1, chip == 1)
        dr = [pltpu.roll(dep[j][t], NL - 1, 1) for t in range(WT)]
        lr = [pltpu.roll(lev[j][t], NL - 1, 1) for t in range(WT)]
        for t in range(WT):
            d, k = dep[j][t], lev[j][t]
            de = jnp.where(l_last, dr[(t + 1) % WT], dr[t])
            ke = jnp.where(l_last, lr[(t + 1) % WT], lr[t])
            if j < WJ - 1:
                dn, kn = dep[j + 1][t], lev[j + 1][t]
            else:
                dn, kn = pltpu.roll(dep[0][t], NS - 1, 0), pltpu.roll(lev[0][t], NS - 1, 0)
            kx = jnp.minimum(k, ke)
            ky = jnp.where(wall, 0.0, jnp.minimum(k, kn))
            hx = jnp.where(kx > 0.0, 0.5 * (d + de), 0.0)
            hy = jnp.where(ky > 0.0, 0.5 * (d + dn), 0.0)
            ix = 1.0 / jnp.maximum(kx, 1.0)
            iy = 1.0 / jnp.maximum(ky, 1.0)
            n = j * WT + t
            state[0, n] = window_tile(main, side, 0, j, t, lane, 0, 0)
            for i in (1, 2):
                first = COURANT * window_tile(main, side, i, j, t, lane, 0, i)
                state[i, n] = first
                wi[1 + i, n] = first
            wi[0, n] = (COURANT * COURANT) * hx
            wi[1, n] = (COURANT * COURANT) * hy
            state[3, n] = (COURANT / NSUB) * hx * ix
            state[4, n] = (COURANT / NSUB) * hy * iy
            state[5, n] = zero
            state[6, n] = zero
            if t < NT:
                here = pl.ds(j, NS, stride=WJ)
                nat.at[0, t][here, :] = ix
                nat.at[1, t][here, :] = iy
                nat.at[2, t][here, :] = 1.0 / jnp.where(kx > 0.0, hx, 1.0)
                nat.at[3, t][here, :] = 1.0 / jnp.where(ky > 0.0, hy, 1.0)
    own = pl.ds(pl.multiple_of(core * NY, NS), NY)
    for t in range(NT):
        for i in range(4):
            rl[i, t] = nat[i, t, own]

    def tail(i, carry):
        s1, s2, n = carry
        w = weights[NSUB - 1 - i]
        return s1 + w, s2 + n * w, n - 1.0

    total, moment, _ = lax.fori_loop(0, NSUB, tail, (0.0, 0.0, float(NSUB)))
    edge_wall = jnp.where(jnp.logical_and(s_first, chip == 0), 0.0, 1.0)
    forces.wait()
    for j in range(WJ):
        for t in range(WT):
            n = j * WT + t
            for f in range(2):
                state[3 + f, n] = state[3 + f, n] * window_tile(fwin, fwside, f, j, t, lane, 0, f)

    def subcycle(i, remain):
        w = weights[i]
        for j in range(WJ):
            r = [pltpu.roll(state[1, j * WT + t], 1, 1) for t in range(WT)]
            for t in range(WT):
                n = j * WT + t
                uw = jnp.where(l_first, r[(t + WT - 1) % WT], r[t])
                if j == 0:
                    vs = pltpu.roll(state[2, (WJ - 1) * WT + t], 1, 0) * edge_wall
                else:
                    vs = state[2, n - WT]
                e = state[0, n] - ((state[1, n] - uw) + (state[2, n] - vs))
                state[0, n] = e
                state[5, n] = state[5, n] + w * e
                state[6, n] = state[6, n] + remain * e
        for j in range(WJ):
            e = [state[0, j * WT + t] for t in range(WT)]
            r = [pltpu.roll(e[t], NL - 1, 1) for t in range(WT)]
            for t in range(WT):
                n = j * WT + t
                ee = jnp.where(l_last, r[(t + 1) % WT], r[t])
                if j == WJ - 1:
                    en = pltpu.roll(state[0, t], NS - 1, 0)
                else:
                    en = state[0, n + WT]
                state[1, n] = (state[1, n] + state[3, n]) - wi[0, n] * (ee - e[t])
                state[2, n] = (state[2, n] + state[4, n]) - wi[1, n] * (en - e[t])
        return remain - w

    lax.fori_loop(0, NSUB, subcycle, total)

    scale = 1.0 / COURANT
    for j in range(WJ):
        q = [state[6, j * WT + t] for t in range(WT)]
        r = [pltpu.roll(q[t], NL - 1, 1) for t in range(WT)]
        for t in range(NT):
            n = j * WT + t
            qe = jnp.where(l_last, r[t + 1], r[t])
            qn = pltpu.roll(state[6, t], NS - 1, 0) if j == WJ - 1 else state[6, n + WT]
            here = pl.ds(j, NS, stride=WJ)
            res.at[0, t][here, :] = state[5, n]
            res.at[1, t][here, :] = scale * (total * wi[2, n] + moment * state[3, n] - wi[0, n] * (qe - q[t]))
            res.at[2, t][here, :] = scale * (total * wi[3, n] + moment * state[4, n] - wi[1, n] * (qn - q[t]))
    other = 1 - core
    send = remote(res.at[:, :, pl.ds(pl.multiple_of(other * NY, NS), NY)], out.at[core], out_send, out_recv, col, chip * 2 + other)
    send.start()
    keep = pltpu.make_async_copy(res.at[:, :, pl.ds(pl.multiple_of(core * NY, NS), NY)], out.at[core], loc_sem)
    keep.start()
    keep.wait()
    send.wait()


def step_call(vel_x, vel_y, pot_temp, salinity, surf_eta, trans_x, trans_y, col_depth, wet_levels, weights, tab):
    dma = pltpu.SemaphoreType.DMA
    nreg = NJ * NT
    nwin = WJ * WT

    def vm(*shape):
        return pltpu.VMEM(shape, F32)

    return pl.pallas_call(
        step_kernel,
        out_shape=(
            vm(4, NM, NK + 1, nreg, *VR),
            vm(2, NM, nreg, *VR),
            pltpu.VMEM((3, nreg, *VR), jnp.int32),
            vm(4, NT, NY, NL),
            vm(NM, 3, NT, NY, NL),
        ),
        in_specs=[ANY] * 4 + [VM] * 5 + [SM] * 2,
        out_specs=(VM,) * 5,
        scratch_shapes=[
            vm(4, NM, NT, NK, NY, NL),
            vm(4, NY, NL), vm(4, NY, NL), vm(4, NT, NM * NK, NL), vm(4, NT, NM * NK, NL), vm(*VR), vm(*VR),
            vm(4, NY, NL), vm(4, NY, NL), vm(4, NT, NM * NK, NL), vm(4, NT, NM * NK, NL),
            vm(NT, NY, NL), vm(NY, NL), vm(NT, *VR),
            vm(NM, 5, NT, NY, NL), vm(NM, 2, 2, NY, NL), vm(5, NT, WY, NL), vm(2, 2, WY, NL),
            vm(2, NM, nreg, *VR),
            vm(NM, 2, NT, NY, NL), vm(NM, 2, 1, NY, NL), vm(2, NT, WY, NL), vm(2, 1, WY, NL),
            vm(4, nwin, *VR), vm(4, NT, WY, NL), vm(7, nwin, *VR), vm(3, NT, WY, NL),
            dma((4, NM, NT, NC)), dma((2, 4)), dma((4,)), dma((4,)), dma((2, 4)), dma((4,)), dma((4,)), dma((2,)), dma((2,)), dma((2,)), dma((2,)),
            dma((16,)), dma((2,)), dma((16,)), dma((2,)), dma, dma, dma,
        ],
        compiler_params=pltpu.CompilerParams(collective_id=0, has_side_effects=True, vmem_limit_bytes=VMEM_LIMIT),
        name="ocean_step",
    )(vel_x, vel_y, pot_temp, salinity, surf_eta, trans_x, trans_y, col_depth, wet_levels, weights, tab)


def final_kernel(sbuf, bsum, kl, rl, bo, tab, eta_out, tx_out, ty_out, u_out, v_out, temp_out, salt_out, xbuf, cor, out_sem):
    outs = (u_out, v_out, temp_out, salt_out)

    def store(f, m, t, c):
        part = pl.ds(c * CH, CH)
        return pltpu.make_async_copy(xbuf.at[f, m, t, part], outs[f].at[part, m, :, pl.ds(t * NL, NL)], out_sem.at[f, m, t, c])

    def each_store(fs, c, op):
        for f in fs:
            for m in range(NM):
                for t in range(NT):
                    getattr(store(f, m, t, c), op)()

    zero = jnp.zeros(VR, F32)
    for m in range(NM):
        for t in range(NT):
            cols = pl.ds(t * NL, NL)
            eta_out[m, :, cols] = bo[m, 0, t]
            tx_out[m, :, cols] = bo[m, 1, t]
            ty_out[m, :, cols] = bo[m, 2, t]
            for f in range(2):
                for j in range(NJ):
                    here = pl.ds(j, NS, stride=NJ)
                    i = j * NT + t
                    cor[f, m, i] = bo.at[m, 1 + f, t][here, :] * rl.at[2 + f, t][here, :] - bsum[f, m, i] * rl.at[f, t][here, :]

    def back(fs):
        def chunk(c2, xs):
            c = NC - 1 - c2

            def step(q, xs):
                xs = list(xs)
                for h in range(2):
                    k = c * CH + CH - 1 - 2 * q - h
                    n = 0
                    for f in fs:
                        g = tab[f // 2 * 2, k]
                        for j in range(NJ):
                            for t in range(NT):
                                here = pl.ds(j, NS, stride=NJ)
                                i = j * NT + t
                                if f < 2:
                                    wet = kl[1 + f, i] > k
                                for m in range(NM):
                                    x = sbuf[f, m, k + 1, i] + g * xs[n]
                                    xs[n] = x
                                    n += 1
                                    xbuf.at[f, m, t, k][here, :] = jnp.where(wet, x + cor[f, m, i], 0.0) if f < 2 else x
                return tuple(xs)

            xs = lax.fori_loop(0, CH // 2, step, xs)
            each_store(fs, c, "start")
            return xs

        lax.fori_loop(0, NC, chunk, (zero,) * (len(fs) * NM * NJ * NT))

    back((2, 3))
    back((0, 1))

    def drain(c, _):
        each_store(range(4), c, "wait")
        return 0

    lax.fori_loop(0, NC, drain, 0)


def final_call(sbuf, bsum, kl, rl, bo, tab):
    flat = jax.ShapeDtypeStruct((NM, NY, NX), F32)
    block = jax.ShapeDtypeStruct((NK, NM, NY, NX), F32)
    held = [pltpu.with_memory_space_constraint(x, pltpu.VMEM) for x in (sbuf, bsum, kl, rl, bo)]
    return pl.pallas_call(
        final_kernel,
        out_shape=(flat,) * 3 + (block,) * 4,
        in_specs=[VM] * 5 + [SM],
        out_specs=(VM,) * 3 + (ANY,) * 4,
        scratch_shapes=[
            pltpu.VMEM((4, NM, NT, NK, NY, NL), F32),
            pltpu.VMEM((2, NM, NJ * NT, *VR), F32),
            pltpu.SemaphoreType.DMA((4, NM, NT, NC)),
        ],
        compiler_params=pltpu.CompilerParams(vmem_limit_bytes=VMEM_LIMIT),
        name="back_substitution",
    )(*held, tab)


def solution(mesh):
    def local_step(*args):
        tab = level_table()
        sbuf, bsum, kl, rl, bo = step_call(*args, tab)
        return final_call(sbuf, bsum, kl, rl, bo, tab)

    spec_3d = P(None, None, "row", "col")
    spec_2d = P(None, "row", "col")
    spec_map = P("row", "col")
    return jax.shard_map(local_step, mesh=mesh, in_specs=(spec_3d,) * 4 + (spec_2d,) * 3 + (spec_map,) * 2 + (P(),), out_specs=(spec_2d,) * 3 + (spec_3d,) * 4, check_vma=False)
```

```python
import functools
import jax
import jax.numpy as jnp
import numpy as np
from jax import lax
from jax.experimental import pallas as pl
from jax.experimental.pallas import tpu as pltpu
from jax.sharding import PartitionSpec as P

MESH = pl.DeviceIdType.MESH
F32 = jnp.float32
NK = 60
NM = 2
NY = 32
NL = 128
NS = 8
VR = (NS, NL)
NX = 256
NT = NX // NL
NJ = NY // 8
CH = 10
NC = NK // CH
HALO = 40
WY = 2 * NY + HALO
WJ = WY // 8
WT = 3
NSUB = 40
COURANT = 0.4
VMEM_LIMIT = 42 << 20
SIDE = 40

VM = pl.BlockSpec(memory_space=pltpu.VMEM)
SM = pl.BlockSpec(memory_space=pltpu.SMEM)
ANY = pl.BlockSpec(memory_space=pl.ANY)


def level_table():
    rows = np.zeros((4, NK), np.float64)
    for row, strength in ((0, 1.0), (2, 0.5)):
        scale = 1.0 if strength == 1.0 else 0.5
        div_prev = 0.0
        for k in range(NK):
            if k == 0:
                div = 1.0 + strength
            else:
                div = 1.0 + 2.0 * strength - strength * strength / div_prev
            rows[row, k] = scale / div
            rows[row + 1, k] = scale / (div - strength)
            div_prev = div
    return jnp.asarray(rows, F32)


def lanes_iota():
    return lax.broadcasted_iota(jnp.int32, VR, 1)


def subl_iota():
    return lax.broadcasted_iota(jnp.int32, VR, 0)


def device(col, row):
    return {"col": col, "row": row}


def greet(col, row):
    barrier = pltpu.get_barrier_semaphore()
    count = 0
    for dc in (0, 1, 3):
        for dr in range(4):
            if dc == 0 and dr == 0:
                continue
            pl.semaphore_signal(barrier, inc=1, device_id=device(lax.rem(col + dc, 4), lax.rem(row + dr, 4)), device_id_type=MESH)
            count += 1
    pl.semaphore_wait(barrier, count)


class Exchange:
    def __init__(self, src_main, src_side, main, side, send_sem, recv_sem, col, row):
        chip = row // 2
        core = lax.rem(row, 2)
        east = lax.rem(col + 1, 4)
        west = lax.rem(col + 3, 4)
        self.full = chip != core
        self.main, self.side, self.recv_sem = main, side, recv_sem
        own = pl.ds(pl.multiple_of(core * NY, NS), NY)
        at_full = pl.ds(pl.multiple_of(jnp.where(chip == 1, 2 * NY, NY + HALO), NS), NY)
        at_part = pl.ds(pl.multiple_of(jnp.where(chip == 1, 3 * NY, 2 * NY), NS), NS)
        from_part = pl.ds(pl.multiple_of(jnp.where(chip == 1, 0, NY - NS), NS), NS)
        self.count = 0

        def remote(s, d, kind, dev):
            return pltpu.make_async_remote_copy(src_ref=s, dst_ref=d, send_sem=send_sem.at[self.count], recv_sem=recv_sem.at[kind], device_id=dev, device_id_type=MESH)

        self.always, self.whole, self.part = [], [], []
        self.local = pltpu.make_async_copy(src_main.at[core], main.at[:, :, own], recv_sem.at[0])
        self.always.append(remote(src_main.at[1 - core], main.at[:, :, own], 0, device(col, chip * 2 + 1 - core)))
        for mm in range(NM):
            near, far = chip * 2 + mm, (1 - chip) * 2 + mm
            self.count += 1
            self.whole.append(remote(src_main.at[mm], main.at[:, :, at_full], 0, device(col, far)))
            self.part.append(remote(src_main.at[mm, :, :, from_part], main.at[:, :, at_part], 0, device(col, far)))
            for e, dev in enumerate((west, east)):
                self.count += 1
                self.whole.append(remote(src_side.at[mm, e], side.at[e, :, at_full], 1, device(dev, far)))
                self.part.append(remote(src_side.at[mm, e, :, from_part], side.at[e, :, at_part], 1, device(dev, far)))
                self.count += 1
                self.always.append(remote(src_side.at[mm, e], side.at[e, :, own], 1, device(dev, near)))

    def branch(self, op):
        @pl.when(self.full)
        def _():
            for copy in self.whole:
                getattr(copy, op)()

        @pl.when(jnp.logical_not(self.full))
        def _():
            for copy in self.part:
                getattr(copy, op)()

    def start(self):
        self.branch("start")
        for copy in self.always:
            copy.start()
        self.local.start()

    def wait(self):
        pltpu.make_async_copy(self.main, self.main, self.recv_sem.at[0]).wait()
        pltpu.make_async_copy(self.side, self.side, self.recv_sem.at[1]).wait()
        for copy in self.always:
            copy.wait_send()
        self.branch("wait_send")


def pack_side(dst, m, group, fields, lane):
    for i in range(NY // NS):
        rows = pl.ds(i * NS, NS)
        first = fields[0](0, rows)
        last = fields[0](NT - 1, rows)
        for n in range(1, len(fields)):
            first = jnp.where(lane < n * SIDE, first, pltpu.roll(fields[n](0, rows), n * SIDE, 1))
            last = jnp.where(lane >= NL - n * SIDE, last, pltpu.roll(fields[n](NT - 1, rows), NL - n * SIDE, 1))
        dst[m, 0, group, rows] = first
        dst[m, 1, group, rows] = last


def window_tile(main, side, f, j, t, lane, group, place):
    here = pl.ds(j, NS, stride=WJ)
    if t < NT:
        return main.at[f, t][here, :]
    e, w = side.at[0, group][here, :], side.at[1, group][here, :]
    if place:
        e, w = pltpu.roll(e, NL - place * SIDE, 1), pltpu.roll(w, place * SIDE, 1)
    return jnp.where(lane < SIDE, e, jnp.where(lane >= NL - SIDE, w, 0.0))


PA = 0.15 * 0.5 / NK * 0.5
PB = 0.2 * 0.5 / NK * 0.5
MOM_UNROLL = 2
TRC_UNROLL = 2


def step_kernel(u, v, temp, salt, eta, tx, ty, depth, wet, weights, tab,
                sbuf, bsum, kl, rl, out,
                inb, ew, ends, corner, sv_east, nu_west, uw_all, hE, hW, hN, hS, hSE, hNW, colF, colL, rowF, rowL, ksrc, kE, kN,
                wmain, wside, main, side, gsum, fmain, fside, fwin, fwside, wi, nat, state, res,
                in_sem, sendC, recvE, recvW, sendR, recvN, recvS, corn_send, corn_recv, k_send, k_recv,
                w_send, w_recv, f_send, f_recv, out_send, out_recv, loc_sem):
    col = lax.axis_index("col")
    row = lax.axis_index("row")
    chip = row // 2
    core = lax.rem(row, 2)
    east_dev = lax.rem(col + 1, 4)
    west_dev = lax.rem(col + 3, 4)
    north_dev = jnp.minimum(row + 1, 3)
    south_dev = jnp.maximum(row - 1, 0)
    has_north = row < 3
    has_south = row > 0
    fields = (u, v, temp, salt)
    lane = lanes_iota()
    subl = subl_iota()
    l_last, l_first = lane == NL - 1, lane == 0
    s_last, s_first = subl == NS - 1, subl == 0
    zero = jnp.zeros(VR, F32)

    def load(f, m, t, c):
        part = pl.ds(c * CH, CH)
        return pltpu.make_async_copy(fields[f].at[part, m, :, pl.ds(t * NL, NL)], inb.at[f, m, t, part], in_sem.at[f, m, t, c])

    def each_load(f, c, op):
        for m in range(NM):
            for t in range(NT):
                getattr(load(f, m, t, c), op)()

    for f in range(4):
        for c in range(NC):
            each_load(f, c, "start")

    for t in range(NT):
        ksrc[t] = wet[:, pl.ds(t * NL, NL)].astype(F32)

    greet(col, row)

    def remote(s, d, ssem, rsem, dc, dr):
        return pltpu.make_async_remote_copy(src_ref=s, dst_ref=d, send_sem=ssem, recv_sem=rsem, device_id=device(dc, dr), device_id_type=MESH)

    k_west = remote(ksrc.at[0], kE, k_send.at[0], k_recv.at[0], west_dev, row)
    k_south = remote(ksrc.at[:, pl.ds(0, NS)], kN, k_send.at[1], k_recv.at[1], col, south_dev)

    def col_copies(f):
        return (remote(colF.at[f], hE.at[f], sendC.at[0, f], recvE.at[f], west_dev, row),
                remote(colL.at[f], hW.at[f], sendC.at[1, f], recvW.at[f], east_dev, row))

    def to_south(f):
        return remote(rowF.at[f], hN.at[f], sendR.at[0, f], recvN.at[f], col, south_dev)

    def to_north(f):
        return remote(rowL.at[f], hS.at[f], sendR.at[1, f], recvS.at[f], col, north_dev)

    corner_north = remote(colF.at[1, pl.ds(NY - NS, NS)], hSE, corn_send.at[0], corn_recv.at[0], west_dev, north_dev)
    corner_south = remote(colL.at[0, pl.ds(0, NS)], hNW, corn_send.at[1], corn_recv.at[1], east_dev, south_dev)

    k_west.start()

    @pl.when(has_south)
    def _():
        k_south.start()

    for f in range(4):
        def chunk(c, acc, f=f):
            each_load(f, c, "wait")
            acc = list(acc)
            for q in range(CH):
                k = c * CH + q
                for m in range(NM):
                    spot = 2 * k + m
                    hit = lane == spot
                    for i in range(NJ):
                        rows = pl.ds(i * NS, NS)
                        first = pltpu.roll(inb[f, m, 0, k, rows], spot, 1)
                        last = pltpu.roll(inb[f, m, NT - 1, k, rows], lax.rem(spot + 1, NL), 1)
                        acc[2 * i] = jnp.where(hit, first, acc[2 * i])
                        acc[2 * i + 1] = jnp.where(hit, last, acc[2 * i + 1])
                    for t in range(NT):
                        rowF[f, t, pl.ds(m * NK + k, 1), :] = inb[f, m, t, k, 0:1]
                        rowL[f, t, pl.ds(m * NK + k, 1), :] = inb[f, m, t, k, NY - 1:NY]
            return tuple(acc)

        acc = lax.fori_loop(0, NC, chunk, (zero,) * (2 * NJ))
        for i in range(NJ):
            colF[f, pl.ds(i * NS, NS)] = acc[2 * i]
            colL[f, pl.ds(i * NS, NS)] = acc[2 * i + 1]

        @pl.when(has_south)
        def _():
            to_south(f).start()

        @pl.when(has_north)
        def _():
            to_north(f).start()
        for copy in col_copies(f):
            copy.start()
        if f == 0:
            @pl.when(has_south)
            def _():
                corner_south.start()
        if f == 1:
            @pl.when(has_north)
            def _():
                corner_north.start()

    for m in range(NM):
        for t in range(NT):
            cols = pl.ds(t * NL, NL)
            for i, arr in enumerate((eta, tx, ty)):
                wmain[m, i, t] = arr[m, :, cols]
            wmain[m, 3, t] = depth[:, cols]
            wmain[m, 4, t] = ksrc[t]
        reads = [lambda t, rows, m=m, i=i: wmain[m, i, t, rows] for i in range(5)]
        pack_side(wside, m, 0, reads[:3], lane)
        pack_side(wside, m, 1, reads[3:], lane)
    windows = Exchange(wmain, wside, main, side, w_send, w_recv, col, row)
    windows.start()

    @pl.when(jnp.logical_not(has_north))
    def _():
        hN[...] = jnp.zeros(hN.shape, F32)
        hNW[...] = jnp.zeros(hNW.shape, F32)
        kN[...] = jnp.zeros(kN.shape, F32)

    @pl.when(jnp.logical_not(has_south))
    def _():
        hS[...] = jnp.zeros(hS.shape, F32)
        hSE[...] = jnp.zeros(hSE.shape, F32)

    for f in range(4):
        for m in range(NM):
            for i in range(NJ * NT):
                sbuf[f, m, 0, i] = zero
    for f in range(2):
        for m in range(NM):
            for i in range(NJ * NT):
                gsum[f, m, i] = zero
                bsum[f, m, i] = zero

    k_west.wait()

    @pl.when(has_south)
    def _():
        k_south.wait_send()
        corner_south.wait_send()
        corner_north.wait_recv()

    @pl.when(has_north)
    def _():
        k_south.wait_recv()
        corner_north.wait_send()
        corner_south.wait_recv()

    for f in range(4):
        for copy in col_copies(f):
            copy.wait()

        @pl.when(has_south)
        def _():
            to_south(f).wait_send()
            to_north(f).wait_recv()

        @pl.when(has_north)
        def _():
            to_north(f).wait_send()
            to_south(f).wait_recv()

    odd = lax.rem(lane, 2)
    for m in range(NM):
        for f in range(4):
            for i in range(NJ):
                rows = pl.ds(i * NS, NS)
                ew[f, m, rows] = jnp.where(odd == m, hE[f, rows], pltpu.roll(hW[f, rows], 1, 1))
        corner[m] = jnp.where(odd == m, hSE[pl.ds(NS - 1, NS, stride=0), :], pltpu.roll(hNW[pl.ds(0, NS, stride=0), :], 1, 1))
    for i in range(NM * NK // NS):
        rows = pl.ds(i * NS, NS)
        r = [pltpu.roll(hS[1, t, rows], NL - 1, 1) for t in range(NT)]
        sv_east[0, rows] = jnp.where(l_last, r[1], r[0])
        sv_east[1, rows] = r[1]
        r = [pltpu.roll(hN[0, t, rows], 1, 1) for t in range(NT)]
        nu_west[0, rows] = r[0]
        nu_west[1, rows] = jnp.where(l_first, r[0], r[1])

    def rolls(x, amount):
        return [[pltpu.roll(x[j][t], amount, 1) for t in range(NT)] for j in range(NJ)]

    def east(x, halo):
        r = rolls(x, NL - 1)
        return [[jnp.where(l_last, r[j][1] if t == 0 else halo[j], r[j][t]) for t in range(NT)] for j in range(NJ)]

    def west(x, halo):
        r = rolls(x, 1)
        return [[jnp.where(l_first, r[j][0] if t == 1 else halo[j], r[j][t]) for t in range(NT)] for j in range(NJ)]

    def north(x, halo):
        return x[1:] + [[jnp.where(s_last, halo[t], pltpu.roll(x[0][t], NS - 1, 0)) for t in range(NT)]]

    def south(x, halo):
        return [[jnp.where(s_first, halo[t], pltpu.roll(x[NJ - 1][t], 1, 0)) for t in range(NT)]] + x[:-1]

    def zipped(fn, *xs):
        return [[fn(*[x[j][t] for x in xs]) for t in range(NT)] for j in range(NJ)]

    def strided(ref):
        return [ref[pl.ds(j, NS, stride=NJ), :] for j in range(NJ)]

    k_mid = zipped(lambda x: x, [list(pair) for pair in zip(*[strided(ksrc.at[t]) for t in range(NT)])])
    k_east = zipped(jnp.minimum, k_mid, east(k_mid, [pltpu.roll(x, NL - 1, 1) for x in strided(kE)]))
    k_north = zipped(jnp.minimum, k_mid, north(k_mid, [kN.at[t][pl.ds(0, NS, stride=0), :] for t in range(NT)]))
    for n, mask in enumerate((k_mid, k_east, k_north)):
        for j in range(NJ):
            for t in range(NT):
                kl[n, j * NT + t] = mask[j][t].astype(jnp.int32)

    def read_mask(n):
        return [[kl[n, j * NT + t] for t in range(NT)] for j in range(NJ)]

    def factors(mask, k, a, b):
        return zipped(lambda n: jnp.where(n > k + 1, a, jnp.where(n == k + 1, b, 0.0)), mask)

    def block(f, m, k):
        return [[inb.at[f, m, t, k][pl.ds(j, NS, stride=NJ), :] for t in range(NT)] for j in range(NJ)]

    def line(ref, m, k):
        return [ref.at[t][pl.ds(m * NK + k, NS, stride=0), :] for t in range(NT)]

    def solve(f, m, k, side_k, scale):
        for j in range(NJ):
            for t in range(NT):
                i = j * NT + t
                sbuf[f, m, k + 1, i] = (side_k[j][t] + sbuf[f, m, k, i]) * scale[j][t]

    def momentum(m, k, carry, wet_x, wet_y, inv_x, inv_y):
        cs, cs_n, cs_e = carry
        uu, vv, tt, ss = (block(f, m, k) for f in range(4))
        amount = NL - 1 - m - 2 * k
        eu, ev, et, es = ([pltpu.roll(x, amount, 1) for x in strided(ew.at[f, m])] for f in range(4))
        c = pltpu.roll(corner[m], amount, 1)
        for j in range(NJ):
            ends[0, m, k, j] = et[j]
            ends[1, m, k, j] = es[j]
        nu, nv, nt, ns = (line(hN.at[f], m, k) for f in range(4))
        su, sv = (line(hS.at[f], m, k) for f in range(2))

        half = zipped(lambda s, t: PA * s - PB * t, ss, tt)
        p = zipped(jnp.add, cs, half)
        cs = zipped(jnp.add, p, half)
        half_n = [PA * ns[t] - PB * nt[t] for t in range(NT)]
        p_n = [cs_n[t] + half_n[t] for t in range(NT)]
        cs_n = [p_n[t] + half_n[t] for t in range(NT)]
        half_e = [PA * es[j] - PB * et[j] for j in range(NJ)]
        p_e = [cs_e[j] + half_e[j] for j in range(NJ)]
        cs_e = [p_e[j] + half_e[j] for j in range(NJ)]

        u_e, u_w, v_e, v_w = east(uu, eu), west(uu, eu), east(vv, ev), west(vv, ev)
        for j in range(NJ):
            for t in range(NT):
                uw_all[m, k, j * NT + t] = u_w[j][t]
        u_n, u_s, v_n, v_s = north(uu, nu), south(uu, su), north(vv, nv), south(vv, sv)
        sve, nuw = line(sv_east, m, k), line(nu_west, m, k)
        sve[1] = jnp.where(l_last, c, sve[1])
        nuw[0] = jnp.where(l_first, c, nuw[0])
        a = zipped(jnp.add, vv, v_e)
        v_sum = zipped(jnp.add, a, south(a, [sv[t] + sve[t] for t in range(NT)]))
        b = zipped(jnp.add, uu, u_w)
        u_sum = zipped(jnp.add, b, north(b, [nu[t] + nuw[t] for t in range(NT)]))
        p_e = east(p, p_e)
        p_n = north(p, p_n)

        gu = zipped(lambda w, p, pe, u, ue, uw, vs, un, us: jnp.where(w, (p - pe) - 0.5 * (u * (ue - uw)) - 0.125 * (vs * (un - us)), 0.0),
                    wet_x, p, p_e, uu, u_e, u_w, v_sum, u_n, u_s)
        gv = zipped(lambda w, p, pn, us, ve, vw, v, vn, vs: jnp.where(w, (p - pn) - 0.125 * (us * (ve - vw)) - 0.5 * (v * (vn - vs)), 0.0),
                    wet_y, p, p_n, u_sum, v_e, v_w, vv, v_n, v_s)
        bu = zipped(jnp.add, uu, gu)
        bv = zipped(jnp.add, vv, gv)
        solve(0, m, k, bu, inv_x)
        solve(1, m, k, bv, inv_y)
        for f, (g, b) in enumerate(((gu, bu), (gv, bv))):
            for j in range(NJ):
                for t in range(NT):
                    i = j * NT + t
                    gsum[f, m, i] = gsum[f, m, i] + g[j][t]
                    bsum[f, m, i] = bsum[f, m, i] + b[j][t]
        return cs, cs_n, cs_e

    def momentum_levels(q, carry):
        for h in range(MOM_UNROLL):
            k = q * MOM_UNROLL + h
            mask_x, mask_y = read_mask(1), read_mask(2)
            a1, b1 = tab[0, k], tab[1, k]
            inv = factors(mask_x, k, a1, b1), factors(mask_y, k, a1, b1)
            wet_k = [zipped(lambda n: n > k, mask) for mask in (mask_x, mask_y)]
            carry = tuple(momentum(m, k, carry[m], *wet_k, *inv) for m in range(NM))
        return carry

    start = ([[zero] * NT for _ in range(NJ)], [zero] * NT, [zero] * NJ)
    lax.fori_loop(0, NK // MOM_UNROLL, momentum_levels, (start, start))

    for f in range(2):
        for m in range(NM):
            for t in range(NT):
                for j in range(NJ):
                    fmain.at[m, f, t][pl.ds(j, NS, stride=NJ), :] = gsum[f, m, j * NT + t]
    for m in range(NM):
        pack_side(fside, m, 0, [lambda t, rows, m=m, f=f: fmain[m, f, t, rows] for f in range(2)], lane)
    forces = Exchange(fmain, fside, fwin, fwside, f_send, f_recv, col, row)
    forces.start()

    def tracer(f, m, k, uu, vv, u_w, sv, inv_c):
        x = block(f, m, k)
        halo = [ends[f - 2, m, k, j] for j in range(NJ)]
        x_e, x_w = east(x, halo), west(x, halo)
        x_n = north(x, line(hN.at[f], m, k))
        s_halo = line(hS.at[f], m, k)
        fx = zipped(lambda u, a, b: u * (a + b), uu, x, x_e)
        fx_w = zipped(lambda u, a, b: u * (a + b), u_w, x, x_w)
        fy = zipped(lambda v, a, b: v * (a + b), vv, x, x_n)
        fy_s = south(fy, [sv[t] * (s_halo[t] + x[0][t]) for t in range(NT)])
        solve(f, m, k, zipped(lambda a, f, fw, g, gs: (a + a) - (f - fw) - (g - gs), x, fx, fx_w, fy, fy_s), inv_c)

    def tracer_levels(q, carry):
        for h in range(TRC_UNROLL):
            k = q * TRC_UNROLL + h
            inv_c = factors(read_mask(0), k, tab[2, k], tab[3, k])
            for m in range(NM):
                uu, vv, sv = block(0, m, k), block(1, m, k), line(hS.at[1], m, k)
                u_w = [[uw_all[m, k, j * NT + t] for t in range(NT)] for j in range(NJ)]
                for f in (2, 3):
                    tracer(f, m, k, uu, vv, u_w, sv, inv_c)
        return carry

    lax.fori_loop(0, NK // TRC_UNROLL, tracer_levels, 0)

    windows.wait()
    dep = [[window_tile(main, side, 3, j, t, lane, 1, 0) for t in range(WT)] for j in range(WJ)]
    lev = [[window_tile(main, side, 4, j, t, lane, 1, 1) for t in range(WT)] for j in range(WJ)]
    for j in range(WJ):
        row_here = WJ * subl + j
        wall = jnp.logical_and(row_here == 2 * NY - 1, chip == 1)
        dr = [pltpu.roll(dep[j][t], NL - 1, 1) for t in range(WT)]
        lr = [pltpu.roll(lev[j][t], NL - 1, 1) for t in range(WT)]
        for t in range(WT):
            d, k = dep[j][t], lev[j][t]
            de = jnp.where(l_last, dr[(t + 1) % WT], dr[t])
            ke = jnp.where(l_last, lr[(t + 1) % WT], lr[t])
            if j < WJ - 1:
                dn, kn = dep[j + 1][t], lev[j + 1][t]
            else:
                dn, kn = pltpu.roll(dep[0][t], NS - 1, 0), pltpu.roll(lev[0][t], NS - 1, 0)
            kx = jnp.minimum(k, ke)
            ky = jnp.where(wall, 0.0, jnp.minimum(k, kn))
            hx = jnp.where(kx > 0.0, 0.5 * (d + de), 0.0)
            hy = jnp.where(ky > 0.0, 0.5 * (d + dn), 0.0)
            ix = 1.0 / jnp.maximum(kx, 1.0)
            iy = 1.0 / jnp.maximum(ky, 1.0)
            n = j * WT + t
            state[0, n] = window_tile(main, side, 0, j, t, lane, 0, 0)
            for i in (1, 2):
                first = COURANT * window_tile(main, side, i, j, t, lane, 0, i)
                state[i, n] = first
                wi[1 + i, n] = first
            wi[0, n] = (COURANT * COURANT) * hx
            wi[1, n] = (COURANT * COURANT) * hy
            state[3, n] = (COURANT / NSUB) * hx * ix
            state[4, n] = (COURANT / NSUB) * hy * iy
            state[5, n] = zero
            state[6, n] = zero
            if t < NT:
                here = pl.ds(j, NS, stride=WJ)
                nat.at[0, t][here, :] = ix
                nat.at[1, t][here, :] = iy
                nat.at[2, t][here, :] = 1.0 / jnp.where(kx > 0.0, hx, 1.0)
                nat.at[3, t][here, :] = 1.0 / jnp.where(ky > 0.0, hy, 1.0)
    own = pl.ds(pl.multiple_of(core * NY, NS), NY)
    for t in range(NT):
        for i in range(4):
            rl[i, t] = nat[i, t, own]

    def tail(i, carry):
        s1, s2, n = carry
        w = weights[NSUB - 1 - i]
        return s1 + w, s2 + n * w, n - 1.0

    total, moment, _ = lax.fori_loop(0, NSUB, tail, (0.0, 0.0, float(NSUB)))
    edge_wall = jnp.where(jnp.logical_and(s_first, chip == 0), 0.0, 1.0)
    forces.wait()
    for j in range(WJ):
        for t in range(WT):
            n = j * WT + t
            for f in range(2):
                state[3 + f, n] = state[3 + f, n] * window_tile(fwin, fwside, f, j, t, lane, 0, f)

    def subcycle(i, remain):
        w = weights[i]
        for j in range(WJ):
            r = [pltpu.roll(state[1, j * WT + t], 1, 1) for t in range(WT)]
            for t in range(WT):
                n = j * WT + t
                uw = jnp.where(l_first, r[(t + WT - 1) % WT], r[t])
                if j == 0:
                    vs = pltpu.roll(state[2, (WJ - 1) * WT + t], 1, 0) * edge_wall
                else:
                    vs = state[2, n - WT]
                e = state[0, n] - ((state[1, n] - uw) + (state[2, n] - vs))
                state[0, n] = e
                state[5, n] = state[5, n] + w * e
                state[6, n] = state[6, n] + remain * e
        for j in range(WJ):
            e = [state[0, j * WT + t] for t in range(WT)]
            r = [pltpu.roll(e[t], NL - 1, 1) for t in range(WT)]
            for t in range(WT):
                n = j * WT + t
                ee = jnp.where(l_last, r[(t + 1) % WT], r[t])
                if j == WJ - 1:
                    en = pltpu.roll(state[0, t], NS - 1, 0)
                else:
                    en = state[0, n + WT]
                state[1, n] = (state[1, n] + state[3, n]) - wi[0, n] * (ee - e[t])
                state[2, n] = (state[2, n] + state[4, n]) - wi[1, n] * (en - e[t])
        return remain - w

    lax.fori_loop(0, NSUB, subcycle, total)

    scale = 1.0 / COURANT
    for j in range(WJ):
        q = [state[6, j * WT + t] for t in range(WT)]
        r = [pltpu.roll(q[t], NL - 1, 1) for t in range(WT)]
        for t in range(NT):
            n = j * WT + t
            qe = jnp.where(l_last, r[t + 1], r[t])
            qn = pltpu.roll(state[6, t], NS - 1, 0) if j == WJ - 1 else state[6, n + WT]
            here = pl.ds(j, NS, stride=WJ)
            res.at[0, t][here, :] = state[5, n]
            res.at[1, t][here, :] = scale * (total * wi[2, n] + moment * state[3, n] - wi[0, n] * (qe - q[t]))
            res.at[2, t][here, :] = scale * (total * wi[3, n] + moment * state[4, n] - wi[1, n] * (qn - q[t]))
    other = 1 - core
    send = remote(res.at[:, :, pl.ds(pl.multiple_of(other * NY, NS), NY)], out.at[core], out_send, out_recv, col, chip * 2 + other)
    send.start()
    keep = pltpu.make_async_copy(res.at[:, :, pl.ds(pl.multiple_of(core * NY, NS), NY)], out.at[core], loc_sem)
    keep.start()
    keep.wait()
    send.wait()


def step_call(vel_x, vel_y, pot_temp, salinity, surf_eta, trans_x, trans_y, col_depth, wet_levels, weights, tab):
    dma = pltpu.SemaphoreType.DMA
    nreg = NJ * NT
    nwin = WJ * WT

    def vm(*shape):
        return pltpu.VMEM(shape, F32)

    return pl.pallas_call(
        step_kernel,
        out_shape=(
            vm(4, NM, NK + 1, nreg, *VR),
            vm(2, NM, nreg, *VR),
            pltpu.VMEM((3, nreg, *VR), jnp.int32),
            vm(4, NT, NY, NL),
            vm(NM, 3, NT, NY, NL),
        ),
        in_specs=[ANY] * 4 + [VM] * 5 + [SM] * 2,
        out_specs=(VM,) * 5,
        scratch_shapes=[
            vm(4, NM, NT, NK, NY, NL),
            vm(4, NM, NY, NL), vm(2, NM, NK, NJ, *VR), vm(NM, *VR), vm(NT, NM * NK, NL), vm(NT, NM * NK, NL), vm(NM, NK, nreg, *VR),
            vm(4, NY, NL), vm(4, NY, NL), vm(4, NT, NM * NK, NL), vm(4, NT, NM * NK, NL), vm(*VR), vm(*VR),
            vm(4, NY, NL), vm(4, NY, NL), vm(4, NT, NM * NK, NL), vm(4, NT, NM * NK, NL),
            vm(NT, NY, NL), vm(NY, NL), vm(NT, *VR),
            vm(NM, 5, NT, NY, NL), vm(NM, 2, 2, NY, NL), vm(5, NT, WY, NL), vm(2, 2, WY, NL),
            vm(2, NM, nreg, *VR),
            vm(NM, 2, NT, NY, NL), vm(NM, 2, 1, NY, NL), vm(2, NT, WY, NL), vm(2, 1, WY, NL),
            vm(4, nwin, *VR), vm(4, NT, WY, NL), vm(7, nwin, *VR), vm(3, NT, WY, NL),
            dma((4, NM, NT, NC)), dma((2, 4)), dma((4,)), dma((4,)), dma((2, 4)), dma((4,)), dma((4,)), dma((2,)), dma((2,)), dma((2,)), dma((2,)),
            dma((16,)), dma((2,)), dma((16,)), dma((2,)), dma, dma, dma,
        ],
        compiler_params=pltpu.CompilerParams(collective_id=0, has_side_effects=True, vmem_limit_bytes=VMEM_LIMIT),
        name="ocean_step",
    )(vel_x, vel_y, pot_temp, salinity, surf_eta, trans_x, trans_y, col_depth, wet_levels, weights, tab)


def final_kernel(sbuf, bsum, kl, rl, bo, tab, eta_out, tx_out, ty_out, u_out, v_out, temp_out, salt_out, xbuf, cor, out_sem):
    outs = (u_out, v_out, temp_out, salt_out)

    def store(f, m, t, c):
        part = pl.ds(c * CH, CH)
        return pltpu.make_async_copy(xbuf.at[f, m, t, part], outs[f].at[part, m, :, pl.ds(t * NL, NL)], out_sem.at[f, m, t, c])

    def each_store(fs, c, op):
        for f in fs:
            for m in range(NM):
                for t in range(NT):
                    getattr(store(f, m, t, c), op)()

    zero = jnp.zeros(VR, F32)
    for m in range(NM):
        for t in range(NT):
            cols = pl.ds(t * NL, NL)
            eta_out[m, :, cols] = bo[m, 0, t]
            tx_out[m, :, cols] = bo[m, 1, t]
            ty_out[m, :, cols] = bo[m, 2, t]
            for f in range(2):
                for j in range(NJ):
                    here = pl.ds(j, NS, stride=NJ)
                    i = j * NT + t
                    cor[f, m, i] = bo.at[m, 1 + f, t][here, :] * rl.at[2 + f, t][here, :] - bsum[f, m, i] * rl.at[f, t][here, :]

    def back(fs):
        def chunk(c2, xs):
            c = NC - 1 - c2

            def step(q, xs):
                xs = list(xs)
                for h in range(2):
                    k = c * CH + CH - 1 - 2 * q - h
                    n = 0
                    for f in fs:
                        g = tab[f // 2 * 2, k]
                        for j in range(NJ):
                            for t in range(NT):
                                here = pl.ds(j, NS, stride=NJ)
                                i = j * NT + t
                                if f < 2:
                                    wet = kl[1 + f, i] > k
                                for m in range(NM):
                                    x = sbuf[f, m, k + 1, i] + g * xs[n]
                                    xs[n] = x
                                    n += 1
                                    xbuf.at[f, m, t, k][here, :] = jnp.where(wet, x + cor[f, m, i], 0.0) if f < 2 else x
                return tuple(xs)

            xs = lax.fori_loop(0, CH // 2, step, xs)
            each_store(fs, c, "start")
            return xs

        lax.fori_loop(0, NC, chunk, (zero,) * (len(fs) * NM * NJ * NT))

    back((2, 3))
    back((0, 1))

    def drain(c, _):
        each_store(range(4), c, "wait")
        return 0

    lax.fori_loop(0, NC, drain, 0)


def final_call(sbuf, bsum, kl, rl, bo, tab):
    flat = jax.ShapeDtypeStruct((NM, NY, NX), F32)
    block = jax.ShapeDtypeStruct((NK, NM, NY, NX), F32)
    held = [pltpu.with_memory_space_constraint(x, pltpu.VMEM) for x in (sbuf, bsum, kl, rl, bo)]
    return pl.pallas_call(
        final_kernel,
        out_shape=(flat,) * 3 + (block,) * 4,
        in_specs=[VM] * 5 + [SM],
        out_specs=(VM,) * 3 + (ANY,) * 4,
        scratch_shapes=[
            pltpu.VMEM((4, NM, NT, NK, NY, NL), F32),
            pltpu.VMEM((2, NM, NJ * NT, *VR), F32),
            pltpu.SemaphoreType.DMA((4, NM, NT, NC)),
        ],
        compiler_params=pltpu.CompilerParams(vmem_limit_bytes=VMEM_LIMIT),
        name="back_substitution",
    )(*held, tab)


def solution(mesh):
    def local_step(*args):
        tab = level_table()
        sbuf, bsum, kl, rl, bo = step_call(*args, tab)
        return final_call(sbuf, bsum, kl, rl, bo, tab)

    spec_3d = P(None, None, "row", "col")
    spec_2d = P(None, "row", "col")
    spec_map = P("row", "col")
    return jax.shard_map(local_step, mesh=mesh, in_specs=(spec_3d,) * 4 + (spec_2d,) * 3 + (spec_map,) * 2 + (P(),), out_specs=(spec_2d,) * 3 + (spec_3d,) * 4, check_vma=False)
```

```python
import functools
import jax
import jax.numpy as jnp
import numpy as np
from jax import lax
from jax.experimental import pallas as pl
from jax.experimental.pallas import tpu as pltpu
from jax.sharding import PartitionSpec as P

MESH = pl.DeviceIdType.MESH
F32 = jnp.float32
NK = 60
NM = 2
NY = 32
NL = 128
NS = 8
VR = (NS, NL)
NF = 4
NX = 256
NT = NX // NL
NJ = NY // 8
CH = 10
NC = NK // CH
HALO = 40
WY = 2 * NY + HALO
WJ = WY // 8
WT = 3
NSUB = 40
COURANT = 0.4
VMEM_LIMIT = 28 << 20
STEP_LIMIT = 28 << 20
SIDE = 40

VM = pl.BlockSpec(memory_space=pltpu.VMEM)
SM = pl.BlockSpec(memory_space=pltpu.SMEM)
HBM = pl.BlockSpec(memory_space=pl.ANY)


def level_table():
    rows = np.zeros((4, NK), np.float64)
    for row, strength in ((0, 1.0), (2, 0.5)):
        scale = 1.0 if strength == 1.0 else 0.5
        div_prev = 0.0
        for k in range(NK):
            if k == 0:
                div = 1.0 + strength
            else:
                div = 1.0 + 2.0 * strength - strength * strength / div_prev
            rows[row, k] = scale / div
            rows[row + 1, k] = scale / (div - strength)
            div_prev = div
    return jnp.asarray(rows, F32)


def lanes_iota():
    return lax.broadcasted_iota(jnp.int32, VR, 1)


def subl_iota():
    return lax.broadcasted_iota(jnp.int32, VR, 0)


def device(col, row):
    return {"col": col, "row": row}


def greet(col, row):
    barrier = pltpu.get_barrier_semaphore()
    count = 0
    for dc in (0, 1, 3):
        for dr in range(NF):
            if dc == 0 and dr == 0:
                continue
            pl.semaphore_signal(barrier, inc=1, device_id=device(lax.rem(col + dc, 4), lax.rem(row + dr, 4)), device_id_type=MESH)
            count += 1
    return lambda: pl.semaphore_wait(barrier, count)


class Exchange:
    def __init__(self, src_main, src_side, main, side, send_sem, recv_sem, col, row):
        chip = row // 2
        core = lax.rem(row, 2)
        east = lax.rem(col + 1, 4)
        west = lax.rem(col + 3, 4)
        self.full = chip != core
        self.main, self.side, self.recv_sem = main, side, recv_sem
        own = pl.ds(pl.multiple_of(core * NY, NS), NY)
        at_full = pl.ds(pl.multiple_of(jnp.where(chip == 1, 2 * NY, NY + HALO), NS), NY)
        at_part = pl.ds(pl.multiple_of(jnp.where(chip == 1, 3 * NY, 2 * NY), NS), NS)
        from_part = pl.ds(pl.multiple_of(jnp.where(chip == 1, 0, NY - NS), NS), NS)
        self.count = 0

        def remote(s, d, kind, dev):
            return pltpu.make_async_remote_copy(src_ref=s, dst_ref=d, send_sem=send_sem.at[self.count], recv_sem=recv_sem.at[kind], device_id=dev, device_id_type=MESH)

        self.always, self.whole, self.part = [], [], []
        self.local = pltpu.make_async_copy(src_main.at[core], main.at[:, :, own], recv_sem.at[0])
        self.always.append(remote(src_main.at[1 - core], main.at[:, :, own], 0, device(col, chip * 2 + 1 - core)))
        for mm in range(NM):
            near, far = chip * 2 + mm, (1 - chip) * 2 + mm
            self.count += 1
            self.whole.append(remote(src_main.at[mm], main.at[:, :, at_full], 0, device(col, far)))
            self.part.append(remote(src_main.at[mm, :, :, from_part], main.at[:, :, at_part], 0, device(col, far)))
            for e, dev in enumerate((west, east)):
                self.count += 1
                self.whole.append(remote(src_side.at[mm, e], side.at[e, :, at_full], 1, device(dev, far)))
                self.part.append(remote(src_side.at[mm, e, :, from_part], side.at[e, :, at_part], 1, device(dev, far)))
                self.count += 1
                self.always.append(remote(src_side.at[mm, e], side.at[e, :, own], 1, device(dev, near)))

    def branch(self, op):
        @pl.when(self.full)
        def _():
            for copy in self.whole:
                getattr(copy, op)()

        @pl.when(jnp.logical_not(self.full))
        def _():
            for copy in self.part:
                getattr(copy, op)()

    def start(self):
        self.branch("start")
        for copy in self.always:
            copy.start()
        self.local.start()

    def wait(self):
        pltpu.make_async_copy(self.main, self.main, self.recv_sem.at[0]).wait()
        pltpu.make_async_copy(self.side, self.side, self.recv_sem.at[1]).wait()
        for copy in self.always:
            copy.wait_send()
        self.branch("wait_send")


def pack_side(dst, m, group, fields, lane):
    for i in range(NY // NS):
        rows = pl.ds(i * NS, NS)
        first = fields[0](0, rows)
        last = fields[0](NT - 1, rows)
        for n in range(1, len(fields)):
            first = jnp.where(lane < n * SIDE, first, pltpu.roll(fields[n](0, rows), n * SIDE, 1))
            last = jnp.where(lane >= NL - n * SIDE, last, pltpu.roll(fields[n](NT - 1, rows), NL - n * SIDE, 1))
        dst[m, 0, group, rows] = first
        dst[m, 1, group, rows] = last


def window_tile(main, side, f, j, t, lane, group, place):
    here = pl.ds(j, NS, stride=WJ)
    if t < NT:
        return main.at[f, t][here, :]
    e, w = side.at[0, group][here, :], side.at[1, group][here, :]
    if place:
        e, w = pltpu.roll(e, NL - place * SIDE, 1), pltpu.roll(w, place * SIDE, 1)
    return jnp.where(lane < SIDE, e, jnp.where(lane >= NL - SIDE, w, 0.0))


PA = 0.15 * 0.5 / NK * 0.5
PB = 0.2 * 0.5 / NK * 0.5
MOM_UNROLL = 2
TRC_UNROLL = 4
SUB_UNROLL = 1


def rolls(x, amount):
    return [[pltpu.roll(x[j][t], amount, 1) for t in range(NT)] for j in range(NJ)]


def east(x, halo):
    edge, r = lanes_iota() == NL - 1, rolls(x, NL - 1)
    return [[jnp.where(edge, r[j][1] if t == 0 else halo[j], r[j][t]) for t in range(NT)] for j in range(NJ)]


def west(x, halo):
    edge, r = lanes_iota() == 0, rolls(x, 1)
    return [[jnp.where(edge, r[j][0] if t == 1 else halo[j], r[j][t]) for t in range(NT)] for j in range(NJ)]


def north(x, halo):
    edge = subl_iota() == NS - 1
    return x[1:] + [[jnp.where(edge, halo[t], pltpu.roll(x[0][t], NS - 1, 0)) for t in range(NT)]]


def south(x, halo):
    edge = subl_iota() == 0
    return [[jnp.where(edge, halo[t], pltpu.roll(x[NJ - 1][t], 1, 0)) for t in range(NT)]] + x[:-1]


def zipped(fn, *xs):
    return [[fn(*[x[j][t] for x in xs]) for t in range(NT)] for j in range(NJ)]


def strided(ref):
    return [ref[pl.ds(j, NS, stride=NJ), :] for j in range(NJ)]


def read_mask(kl, n):
    return [[kl[n, j * NT + t] for t in range(NT)] for j in range(NJ)]


def factors(mask, k, a, b):
    return zipped(lambda n: jnp.where(n > k + 1, a, jnp.where(n == k + 1, b, 0.0)), mask)


def read_block(ref, index, k):
    return [[ref.at[(*index, t, k)][pl.ds(j, NS, stride=NJ), :] for t in range(NT)] for j in range(NJ)]


def line(ref, m, k):
    return [ref.at[t][pl.ds(m * NK + k, NS, stride=0), :] for t in range(NT)]


def solve(sbuf, f, m, k, side, scale):
    for j in range(NJ):
        for t in range(NT):
            i = j * NT + t
            sbuf[f, m, k + 1, i] = (side[j][t] + sbuf[f, m, k, i]) * scale[j][t]


def tracer_pass(inb, field, ends, uw_all, north_rows, south_rows, south_v, kl, tab, sbuf, f):
    def level(m, k, inv_c):
        uu, vv, sv = read_block(inb, (0, m), k), read_block(inb, (1, m), k), line(south_v, m, k)
        u_w = [[uw_all[m, k, j * NT + t] for t in range(NT)] for j in range(NJ)]
        x = read_block(*field(m), k)
        halo = [ends[m, k, j] for j in range(NJ)]
        x_e, x_w = east(x, halo), west(x, halo)
        x_n = north(x, line(north_rows, m, k))
        x_s = line(south_rows, m, k)
        fx = zipped(lambda u, a, b: u * (a + b), uu, x, x_e)
        fx_w = zipped(lambda u, a, b: u * (a + b), u_w, x, x_w)
        fy = zipped(lambda v, a, b: v * (a + b), vv, x, x_n)
        fy_s = south(fy, [sv[t] * (x_s[t] + x[0][t]) for t in range(NT)])
        solve(sbuf, f, m, k, zipped(lambda a, b, bw, g, gs: (a + a) - (b - bw) - (g - gs), x, fx, fx_w, fy, fy_s), inv_c)

    def levels(q, carry):
        for h in range(TRC_UNROLL):
            k = q * TRC_UNROLL + h
            inv_c = factors(read_mask(kl, 0), k, tab[2, k], tab[3, k])
            for m in range(NM):
                level(m, k, inv_c)
        return carry

    lax.fori_loop(0, NK // TRC_UNROLL, levels, 0)


def step_kernel(u, v, temp, salt, eta, tx, ty, depth, wet, weights, tab,
                sbuf, bsum, kl, rl, out, inb, ends_s, uw_all, hN, hS,
                inb_t, ew, ends_t, corner, sv_east, nu_west, hE, hW, hSE, hNW, colF, colL, rowF, rowL, ksrc, kE, kN,
                wmain, wside, main, side, gsum, fmain, fside, fwin, fwside, wi, nat, state, res,
                in_sem, sendC, recvE, recvW, sendR, recvN, recvS, corn_send, corn_recv, k_send, k_recv,
                w_send, w_recv, f_send, f_recv, out_send, out_recv, loc_sem):
    col = lax.axis_index("col")
    row = lax.axis_index("row")
    chip = row // 2
    core = lax.rem(row, 2)
    east_dev = lax.rem(col + 1, 4)
    west_dev = lax.rem(col + 3, 4)
    north_dev = jnp.minimum(row + 1, 3)
    south_dev = jnp.maximum(row - 1, 0)
    has_north = row < 3
    has_south = row > 0
    fields = (u, v, temp, salt)
    lane = lanes_iota()
    subl = subl_iota()
    l_last, l_first = lane == NL - 1, lane == 0
    s_last, s_first = subl == NS - 1, subl == 0
    zero = jnp.zeros(VR, F32)

    def place(f, *index):
        return inb_t.at[index] if f == 2 else inb.at[(min(f, 2), *index)]

    def held(f, *index):
        return inb_t[index] if f == 2 else inb[(min(f, 2), *index)]

    def load(f, m, t, c):
        part = pl.ds(c * CH, CH)
        return pltpu.make_async_copy(fields[f].at[part, m, :, pl.ds(t * NL, NL)], place(f, m, t, part), in_sem.at[f, m, t, c])

    def each_load(f, c, op):
        for m in range(NM):
            for t in range(NT):
                getattr(load(f, m, t, c), op)()

    for f in range(NF):
        for c in range(NC):
            each_load(f, c, "start")

    for t in range(NT):
        ksrc[t] = wet[:, pl.ds(t * NL, NL)].astype(F32)

    greet(col, row)()

    def remote(s, d, ssem, rsem, dc, dr):
        return pltpu.make_async_remote_copy(src_ref=s, dst_ref=d, send_sem=ssem, recv_sem=rsem, device_id=device(dc, dr), device_id_type=MESH)

    k_west = remote(ksrc.at[0], kE, k_send.at[0], k_recv.at[0], west_dev, row)
    k_south = remote(ksrc.at[:, pl.ds(0, NS)], kN, k_send.at[1], k_recv.at[1], col, south_dev)

    def col_copies(f):
        return (remote(colF.at[f], hE.at[f], sendC.at[0, f], recvE.at[f], west_dev, row),
                remote(colL.at[f], hW.at[f], sendC.at[1, f], recvW.at[f], east_dev, row))

    def to_south(f):
        return remote(rowF.at[f], hN.at[f], sendR.at[0, f], recvN.at[f], col, south_dev)

    def to_north(f):
        return remote(rowL.at[f], hS.at[f], sendR.at[1, f], recvS.at[f], col, north_dev)

    corner_north = remote(colF.at[1, pl.ds(NY - NS, NS)], hSE, corn_send.at[0], corn_recv.at[0], west_dev, north_dev)
    corner_south = remote(colL.at[0, pl.ds(0, NS)], hNW, corn_send.at[1], corn_recv.at[1], east_dev, south_dev)

    lane_next = lax.rem(lane + 1, NL)
    for f in range(NF):
        def chunk(c, acc, f=f):
            each_load(f, c, "wait")
            acc = list(acc)
            for q in range(CH):
                k = c * CH + q
                for m in range(NM):
                    spot = 2 * k + m
                    hit, hit_last = lane == spot, lane_next == spot
                    for i in range(NJ):
                        rows = pl.ds(i * NS, NS)
                        both = pltpu.roll(jnp.where(l_first, held(f, m, 0, k, rows), held(f, m, NT - 1, k, rows)), spot, 1)
                        acc[2 * i] = jnp.where(hit, both, acc[2 * i])
                        acc[2 * i + 1] = jnp.where(hit_last, both, acc[2 * i + 1])
                    for t in range(NT):
                        rowF[f, t, pl.ds(m * NK + k, 1), :] = held(f, m, t, k, pl.ds(0, 1))
                        rowL[f, t, pl.ds(m * NK + k, 1), :] = held(f, m, t, k, pl.ds(NY - 1, 1))
            return tuple(acc)

        acc = lax.fori_loop(0, NC, chunk, (zero,) * (2 * NJ))
        for i in range(NJ):
            colF[f, pl.ds(i * NS, NS)] = acc[2 * i]
            colL[f, pl.ds(i * NS, NS)] = acc[2 * i + 1]
        if f == 0:
            k_west.start()

            @pl.when(has_south)
            def _():
                k_south.start()

        @pl.when(has_south)
        def _():
            to_south(f).start()

        @pl.when(has_north)
        def _():
            to_north(f).start()
        for copy in col_copies(f):
            copy.start()
        if f == 0:
            @pl.when(has_south)
            def _():
                corner_south.start()
        if f == 1:
            @pl.when(has_north)
            def _():
                corner_north.start()

    for m in range(NM):
        for t in range(NT):
            cols = pl.ds(t * NL, NL)
            for i, arr in enumerate((eta, tx, ty)):
                wmain[m, i, t] = arr[m, :, cols]
            wmain[m, 3, t] = depth[:, cols]
            wmain[m, 4, t] = ksrc[t]
        reads = [lambda t, rows, m=m, i=i: wmain[m, i, t, rows] for i in range(5)]
        pack_side(wside, m, 0, reads[:3], lane)
        pack_side(wside, m, 1, reads[3:], lane)
    windows = Exchange(wmain, wside, main, side, w_send, w_recv, col, row)
    windows.start()

    @pl.when(jnp.logical_not(has_north))
    def _():
        hN[...] = jnp.zeros(hN.shape, F32)
        hNW[...] = jnp.zeros(hNW.shape, F32)
        kN[...] = jnp.zeros(kN.shape, F32)

    @pl.when(jnp.logical_not(has_south))
    def _():
        hS[...] = jnp.zeros(hS.shape, F32)
        hSE[...] = jnp.zeros(hSE.shape, F32)

    for f in range(3):
        for m in range(NM):
            for i in range(NJ * NT):
                sbuf[f, m, 0, i] = zero
    for f in range(2):
        for m in range(NM):
            for i in range(NJ * NT):
                gsum[f, m, i] = zero
                bsum[f, m, i] = zero

    k_west.wait()

    @pl.when(has_south)
    def _():
        k_south.wait_send()
        corner_south.wait_send()
        corner_north.wait_recv()

    @pl.when(has_north)
    def _():
        k_south.wait_recv()
        corner_north.wait_send()
        corner_south.wait_recv()

    for f in range(NF):
        for copy in col_copies(f):
            copy.wait()

        @pl.when(has_south)
        def _():
            to_south(f).wait_send()
            to_north(f).wait_recv()

        @pl.when(has_north)
        def _():
            to_north(f).wait_send()
            to_south(f).wait_recv()

    odd = lax.rem(lane, 2)
    for m in range(NM):
        for f in range(NF):
            for i in range(NJ):
                rows = pl.ds(i * NS, NS)
                ew[f, m, rows] = jnp.where(odd == m, hE[f, rows], pltpu.roll(hW[f, rows], 2, 1))
        corner[m] = jnp.where(odd == m, hSE[pl.ds(NS - 1, NS, stride=0), :], pltpu.roll(hNW[pl.ds(0, NS, stride=0), :], 2, 1))
    for i in range(NM * NK // NS):
        rows = pl.ds(i * NS, NS)
        r = [pltpu.roll(hS[1, t, rows], NL - 1, 1) for t in range(NT)]
        sv_east[0, rows] = jnp.where(l_last, r[1], r[0])
        sv_east[1, rows] = r[1]
        r = [pltpu.roll(hN[0, t, rows], 1, 1) for t in range(NT)]
        nu_west[0, rows] = r[0]
        nu_west[1, rows] = jnp.where(l_first, r[0], r[1])

    k_mid = zipped(lambda x: x, [list(pair) for pair in zip(*[strided(ksrc.at[t]) for t in range(NT)])])
    k_east = zipped(jnp.minimum, k_mid, east(k_mid, [pltpu.roll(x, NL - 1, 1) for x in strided(kE)]))
    k_north = zipped(jnp.minimum, k_mid, north(k_mid, [kN.at[t][pl.ds(0, NS, stride=0), :] for t in range(NT)]))
    for n, mask in enumerate((k_mid, k_east, k_north)):
        for j in range(NJ):
            for t in range(NT):
                kl[n, j * NT + t] = mask[j][t].astype(jnp.int32)

    def block(f, m, k):
        return [[place(f, m, t, k)[pl.ds(j, NS, stride=NJ), :] for t in range(NT)] for j in range(NJ)]

    def momentum(m, k, carry, wet_x, wet_y, inv_x, inv_y):
        cs, cs_n, cs_e = carry
        uu, vv, tt, ss = (block(f, m, k) for f in range(NF))
        amount = NL - 1 - m - 2 * k
        eu, ev, et, es = ([pltpu.roll(x, amount, 1) for x in strided(ew.at[f, m])] for f in range(NF))
        c = pltpu.roll(corner[m], amount, 1)
        for j in range(NJ):
            ends_t[m, k, j] = et[j]
            ends_s[m, k, j] = es[j]
        nu, nv, nt, ns = (line(hN.at[f], m, k) for f in range(NF))
        su, sv = (line(hS.at[f], m, k) for f in range(2))

        half = zipped(lambda s, t: PA * s - PB * t, ss, tt)
        p = zipped(jnp.add, cs, half)
        cs = zipped(jnp.add, p, half)
        half_n = [PA * ns[t] - PB * nt[t] for t in range(NT)]
        p_n = [cs_n[t] + half_n[t] for t in range(NT)]
        cs_n = [p_n[t] + half_n[t] for t in range(NT)]
        half_e = [PA * es[j] - PB * et[j] for j in range(NJ)]
        p_e = [cs_e[j] + half_e[j] for j in range(NJ)]
        cs_e = [p_e[j] + half_e[j] for j in range(NJ)]

        u_e, u_w, v_e, v_w = east(uu, eu), west(uu, eu), east(vv, ev), west(vv, ev)
        for j in range(NJ):
            for t in range(NT):
                uw_all[m, k, j * NT + t] = u_w[j][t]
        u_n, u_s, v_n, v_s = north(uu, nu), south(uu, su), north(vv, nv), south(vv, sv)
        sve, nuw = line(sv_east, m, k), line(nu_west, m, k)
        sve[1] = jnp.where(l_last, c, sve[1])
        nuw[0] = jnp.where(l_first, c, nuw[0])
        a = zipped(jnp.add, vv, v_e)
        v_sum = zipped(jnp.add, a, south(a, [sv[t] + sve[t] for t in range(NT)]))
        b = zipped(jnp.add, uu, u_w)
        u_sum = zipped(jnp.add, b, north(b, [nu[t] + nuw[t] for t in range(NT)]))
        p_e = east(p, p_e)
        p_n = north(p, p_n)

        gu = zipped(lambda w, p, pe, u, ue, uw, vs, un, us: jnp.where(w, (p - pe) - 0.5 * (u * (ue - uw)) - 0.125 * (vs * (un - us)), 0.0),
                    wet_x, p, p_e, uu, u_e, u_w, v_sum, u_n, u_s)
        gv = zipped(lambda w, p, pn, us, ve, vw, v, vn, vs: jnp.where(w, (p - pn) - 0.125 * (us * (ve - vw)) - 0.5 * (v * (vn - vs)), 0.0),
                    wet_y, p, p_n, u_sum, v_e, v_w, vv, v_n, v_s)
        bu = zipped(jnp.add, uu, gu)
        bv = zipped(jnp.add, vv, gv)
        solve(sbuf, 0, m, k, bu, inv_x)
        solve(sbuf, 1, m, k, bv, inv_y)
        for f, (g, b) in enumerate(((gu, bu), (gv, bv))):
            for j in range(NJ):
                for t in range(NT):
                    i = j * NT + t
                    gsum[f, m, i] = gsum[f, m, i] + g[j][t]
                    bsum[f, m, i] = bsum[f, m, i] + b[j][t]
        return cs, cs_n, cs_e

    def momentum_levels(q, carry):
        for h in range(MOM_UNROLL):
            k = q * MOM_UNROLL + h
            mask_x, mask_y = read_mask(kl, 1), read_mask(kl, 2)
            a1, b1 = tab[0, k], tab[1, k]
            inv = factors(mask_x, k, a1, b1), factors(mask_y, k, a1, b1)
            wet_k = [zipped(lambda n: n > k, mask) for mask in (mask_x, mask_y)]
            carry = tuple(momentum(m, k, carry[m], *wet_k, *inv) for m in range(NM))
        return carry

    start = ([[zero] * NT for _ in range(NJ)], [zero] * NT, [zero] * NJ)
    lax.fori_loop(0, NK // MOM_UNROLL, momentum_levels, (start, start))

    for f in range(2):
        for m in range(NM):
            for t in range(NT):
                for j in range(NJ):
                    fmain.at[m, f, t][pl.ds(j, NS, stride=NJ), :] = gsum[f, m, j * NT + t]
    for m in range(NM):
        pack_side(fside, m, 0, [lambda t, rows, m=m, f=f: fmain[m, f, t, rows] for f in range(2)], lane)
    forces = Exchange(fmain, fside, fwin, fwside, f_send, f_recv, col, row)
    forces.start()

    tracer_pass(inb, lambda m: (inb_t, (m,)), ends_t, uw_all, hN.at[2], hS.at[2], hS.at[1], kl, tab, sbuf, 2)

    windows.wait()
    dep = [[window_tile(main, side, 3, j, t, lane, 1, 0) for t in range(WT)] for j in range(WJ)]
    lev = [[window_tile(main, side, 4, j, t, lane, 1, 1) for t in range(WT)] for j in range(WJ)]
    for j in range(WJ):
        row_here = WJ * subl + j
        wall = jnp.logical_and(row_here == 2 * NY - 1, chip == 1)
        dr = [pltpu.roll(dep[j][t], NL - 1, 1) for t in range(WT)]
        lr = [pltpu.roll(lev[j][t], NL - 1, 1) for t in range(WT)]
        for t in range(WT):
            d, k = dep[j][t], lev[j][t]
            de = jnp.where(l_last, dr[(t + 1) % WT], dr[t])
            ke = jnp.where(l_last, lr[(t + 1) % WT], lr[t])
            if j < WJ - 1:
                dn, kn = dep[j + 1][t], lev[j + 1][t]
            else:
                dn, kn = pltpu.roll(dep[0][t], NS - 1, 0), pltpu.roll(lev[0][t], NS - 1, 0)
            kx = jnp.minimum(k, ke)
            ky = jnp.where(wall, 0.0, jnp.minimum(k, kn))
            hx = jnp.where(kx > 0.0, 0.5 * (d + de), 0.0)
            hy = jnp.where(ky > 0.0, 0.5 * (d + dn), 0.0)
            ix = 1.0 / jnp.maximum(kx, 1.0)
            iy = 1.0 / jnp.maximum(ky, 1.0)
            n = j * WT + t
            state[0, n] = window_tile(main, side, 0, j, t, lane, 0, 0)
            for i in (1, 2):
                first = COURANT * window_tile(main, side, i, j, t, lane, 0, i)
                state[i, n] = first
                wi[1 + i, n] = first
            wi[0, n] = (COURANT * COURANT) * hx
            wi[1, n] = (COURANT * COURANT) * hy
            state[3, n] = (COURANT / NSUB) * hx * ix
            state[4, n] = (COURANT / NSUB) * hy * iy
            state[5, n] = zero
            state[6, n] = zero
            if t < NT:
                here = pl.ds(j, NS, stride=WJ)
                nat.at[0, t][here, :] = ix
                nat.at[1, t][here, :] = iy
                nat.at[2, t][here, :] = 1.0 / jnp.where(kx > 0.0, hx, 1.0)
                nat.at[3, t][here, :] = 1.0 / jnp.where(ky > 0.0, hy, 1.0)
    own = pl.ds(pl.multiple_of(core * NY, NS), NY)
    for t in range(NT):
        for i in range(NF):
            rl[i, t] = nat[i, t, own]

    def tail(i, carry):
        s1, s2, n = carry
        w = weights[NSUB - 1 - i]
        return s1 + w, s2 + n * w, n - 1.0

    total, moment, _ = lax.fori_loop(0, NSUB, tail, (0.0, 0.0, float(NSUB)))
    edge_wall = jnp.where(jnp.logical_and(s_first, chip == 0), 0.0, 1.0)
    forces.wait()
    for j in range(WJ):
        for t in range(WT):
            n = j * WT + t
            for f in range(2):
                state[3 + f, n] = state[3 + f, n] * window_tile(fwin, fwside, f, j, t, lane, 0, f)

    def subcycle(i, remain):
        w = weights[i]
        for j in range(WJ):
            r = [pltpu.roll(state[1, j * WT + t], 1, 1) for t in range(WT)]
            for t in range(WT):
                n = j * WT + t
                uw = jnp.where(l_first, r[(t + WT - 1) % WT], r[t])
                if j == 0:
                    vs = pltpu.roll(state[2, (WJ - 1) * WT + t], 1, 0) * edge_wall
                else:
                    vs = state[2, n - WT]
                e = state[0, n] - ((state[1, n] - uw) + (state[2, n] - vs))
                state[0, n] = e
                state[5, n] = state[5, n] + w * e
                state[6, n] = state[6, n] + remain * e
        for j in range(WJ):
            e = [state[0, j * WT + t] for t in range(WT)]
            r = [pltpu.roll(e[t], NL - 1, 1) for t in range(WT)]
            for t in range(WT):
                n = j * WT + t
                ee = jnp.where(l_last, r[(t + 1) % WT], r[t])
                if j == WJ - 1:
                    en = pltpu.roll(state[0, t], NS - 1, 0)
                else:
                    en = state[0, n + WT]
                state[1, n] = (state[1, n] + state[3, n]) - wi[0, n] * (ee - e[t])
                state[2, n] = (state[2, n] + state[4, n]) - wi[1, n] * (en - e[t])
        return remain - w

    lax.fori_loop(0, NSUB, subcycle, total, unroll=SUB_UNROLL)

    scale = 1.0 / COURANT
    for j in range(WJ):
        q = [state[6, j * WT + t] for t in range(WT)]
        r = [pltpu.roll(q[t], NL - 1, 1) for t in range(WT)]
        for t in range(NT):
            n = j * WT + t
            qe = jnp.where(l_last, r[t + 1], r[t])
            qn = pltpu.roll(state[6, t], NS - 1, 0) if j == WJ - 1 else state[6, n + WT]
            here = pl.ds(j, NS, stride=WJ)
            res.at[0, t][here, :] = state[5, n]
            res.at[1, t][here, :] = scale * (total * wi[2, n] + moment * state[3, n] - wi[0, n] * (qe - q[t]))
            res.at[2, t][here, :] = scale * (total * wi[3, n] + moment * state[4, n] - wi[1, n] * (qn - q[t]))
    other = 1 - core
    send = remote(res.at[:, :, pl.ds(pl.multiple_of(other * NY, NS), NY)], out.at[core], out_send, out_recv, col, chip * 2 + other)
    send.start()
    keep = pltpu.make_async_copy(res.at[:, :, pl.ds(pl.multiple_of(core * NY, NS), NY)], out.at[core], loc_sem)
    keep.start()
    keep.wait()
    send.wait()


def step_call(vel_x, vel_y, pot_temp, salinity, surf_eta, trans_x, trans_y, col_depth, wet_levels, weights, tab):
    dma = pltpu.SemaphoreType.DMA
    pair = dma((NM,))
    nreg = NJ * NT
    nwin = WJ * WT

    def vm(*shape):
        return pltpu.VMEM(shape, F32)

    return pl.pallas_call(
        step_kernel,
        out_shape=(
            vm(3, NM, NK + 1, nreg, *VR),
            vm(2, NM, nreg, *VR),
            pltpu.VMEM((3, nreg, *VR), jnp.int32),
            vm(4, NT, NY, NL),
            vm(NM, 3, NT, NY, NL),
            vm(3, NM, NT, NK, NY, NL), vm(NM, NK, NJ, *VR), vm(NM, NK, nreg, *VR), vm(4, NT, NM * NK, NL), vm(4, NT, NM * NK, NL),
        ),
        in_specs=[HBM] * 4 + [VM] * 5 + [SM] * 2,
        out_specs=(VM,) * 10,
        scratch_shapes=[
            vm(NM, NT, NK, NY, NL),
            vm(4, NM, NY, NL), vm(NM, NK, NJ, *VR), vm(NM, *VR), vm(NT, NM * NK, NL), vm(NT, NM * NK, NL),
            vm(NF, NY, NL), vm(NF, NY, NL), vm(*VR), vm(*VR),
            vm(NF, NY, NL), vm(NF, NY, NL), vm(NF, NT, NM * NK, NL), vm(NF, NT, NM * NK, NL),
            vm(NT, NY, NL), vm(NY, NL), vm(NT, *VR),
            vm(NM, 5, NT, NY, NL), vm(NM, 2, 2, NY, NL), vm(5, NT, WY, NL), vm(2, 2, WY, NL),
            vm(2, NM, nreg, *VR),
            vm(NM, 2, NT, NY, NL), vm(NM, 2, 1, NY, NL), vm(2, NT, WY, NL), vm(2, 1, WY, NL),
            vm(4, nwin, *VR), vm(4, NT, WY, NL), vm(7, nwin, *VR), vm(3, NT, WY, NL),
            dma((NF, NM, NT, NC)), dma((NM, NF)), dma((NF,)), dma((NF,)), dma((NM, NF)), dma((NF,)), dma((NF,)), pair, pair, pair, pair,
            dma((NS + NS,)), pair, dma((NS + NS,)), pair, dma, dma, dma,
        ],
        compiler_params=pltpu.CompilerParams(collective_id=0, has_side_effects=True, vmem_limit_bytes=STEP_LIMIT),
        name="ocean_step",
    )(vel_x, vel_y, pot_temp, salinity, surf_eta, trans_x, trans_y, col_depth, wet_levels, weights, tab)


def final_kernel(sbuf, bsum, kl, rl, bo, inb, ends_s, uw_all, hN, hS, tab, eta_out, tx_out, ty_out, u_out, v_out, temp_out, salt_out, xbuf, s_salt, cor, out_sem):
    outs = (u_out, v_out, temp_out, salt_out)
    parts = ((sbuf, 0), (sbuf, 1), (sbuf, 2), (s_salt, 0))

    def store(f, m, t, c):
        part = pl.ds(c * CH, CH)
        return pltpu.make_async_copy(xbuf.at[f, m, t, part], outs[f].at[part, m, :, pl.ds(t * NL, NL)], out_sem.at[f, m, t, c])

    def each_store(fs, c, op):
        for f in fs:
            for m in range(NM):
                for t in range(NT):
                    getattr(store(f, m, t, c), op)()

    zero = jnp.zeros(VR, F32)
    for m in range(NM):
        for t in range(NT):
            cols = pl.ds(t * NL, NL)
            eta_out[m, :, cols] = bo[m, 0, t]
            tx_out[m, :, cols] = bo[m, 1, t]
            ty_out[m, :, cols] = bo[m, 2, t]
            for f in range(2):
                for j in range(NJ):
                    here = pl.ds(j, NS, stride=NJ)
                    i = j * NT + t
                    cor[f, m, i] = bo.at[m, 1 + f, t][here, :] * rl.at[2 + f, t][here, :] - bsum[f, m, i] * rl.at[f, t][here, :]

    def back(fs):
        def chunk(c2, xs):
            c = NC - 1 - c2

            def step(q, xs):
                xs = list(xs)
                for h in range(2):
                    k = c * CH + CH - 1 - 2 * q - h
                    n = 0
                    for f in fs:
                        g = tab[f // 2 * 2, k]
                        for j in range(NJ):
                            for t in range(NT):
                                here = pl.ds(j, NS, stride=NJ)
                                i = j * NT + t
                                if f < 2:
                                    wet = kl[1 + f, i] > k
                                for m in range(NM):
                                    x = parts[f][0][parts[f][1], m, k + 1, i] + g * xs[n]
                                    xs[n] = x
                                    n += 1
                                    xbuf.at[f, m, t, k][here, :] = jnp.where(wet, x + cor[f, m, i], 0.0) if f < 2 else x
                return tuple(xs)

            xs = lax.fori_loop(0, CH // 2, step, xs)
            each_store(fs, c, "start")
            return xs

        lax.fori_loop(0, NC, chunk, (zero,) * (len(fs) * NM * NJ * NT))

    back((2,))
    back((0, 1))
    for m in range(NM):
        for i in range(NJ * NT):
            s_salt[0, m, 0, i] = zero
    tracer_pass(inb, lambda m: (inb, (2, m)), ends_s, uw_all, hN.at[3], hS.at[3], hS.at[1], kl, tab, s_salt, 0)
    back((3,))

    def drain(c, _):
        each_store(range(NF), c, "wait")
        return 0

    lax.fori_loop(0, NC, drain, 0)


def final_call(kept, tab):
    flat = jax.ShapeDtypeStruct((NM, NY, NX), F32)
    block = jax.ShapeDtypeStruct((NK, NM, NY, NX), F32)
    held = [pltpu.with_memory_space_constraint(x, pltpu.VMEM) for x in kept]
    return pl.pallas_call(
        final_kernel,
        out_shape=(flat,) * 3 + (block,) * 4,
        in_specs=[VM] * len(held) + [SM],
        out_specs=(VM,) * 3 + (HBM,) * 4,
        scratch_shapes=[
            pltpu.VMEM((4, NM, NT, NK, NY, NL), F32),
            pltpu.VMEM((1, NM, NK + 1, NJ * NT, *VR), F32),
            pltpu.VMEM((2, NM, NJ * NT, *VR), F32),
            pltpu.SemaphoreType.DMA((4, NM, NT, NC)),
        ],
        compiler_params=pltpu.CompilerParams(vmem_limit_bytes=VMEM_LIMIT),
        name="back_substitution",
    )(*held, tab)


def solution(mesh):
    def local_step(*args):
        tab = level_table()
        return final_call(step_call(*args, tab), tab)

    spec_3d = P(None, None, "row", "col")
    spec_2d = P(None, "row", "col")
    spec_map = P("row", "col")
    return jax.shard_map(local_step, mesh=mesh, in_specs=(spec_3d,) * 4 + (spec_2d,) * 3 + (spec_map,) * 2 + (P(),), out_specs=(spec_2d,) * 3 + (spec_3d,) * 4, check_vma=False)
```

```python
import functools
import jax
import jax.numpy as jnp
import numpy as np
from jax import lax
from jax.experimental import pallas as pl
from jax.experimental.pallas import tpu as pltpu
from jax.sharding import PartitionSpec as P

MESH = pl.DeviceIdType.MESH
F32 = jnp.float32
NK = 60
NM = 2
NY = 32
NL = 128
NS = 8
VR = (NS, NL)
NF = 4
NX = 256
NT = NX // NL
NJ = NY // 8
CH = 10
NC = NK // CH
HALO = 40
WY = 2 * NY + HALO
WJ = WY // 8
WT = 3
NSUB = 40
COURANT = 0.4
VMEM_LIMIT = 28 << 20
STEP_LIMIT = 28 << 20
SIDE = 40

VM = pl.BlockSpec(memory_space=pltpu.VMEM)
SM = pl.BlockSpec(memory_space=pltpu.SMEM)
HBM = pl.BlockSpec(memory_space=pl.ANY)


def level_table():
    rows = np.zeros((4, NK), np.float64)
    for row, strength in ((0, 1.0), (2, 0.5)):
        scale = 1.0 if strength == 1.0 else 0.5
        div_prev = 0.0
        for k in range(NK):
            if k == 0:
                div = 1.0 + strength
            else:
                div = 1.0 + 2.0 * strength - strength * strength / div_prev
            rows[row, k] = scale / div
            rows[row + 1, k] = scale / (div - strength)
            div_prev = div
    return jnp.asarray(rows, F32)


def lanes_iota():
    return lax.broadcasted_iota(jnp.int32, VR, 1)


def subl_iota():
    return lax.broadcasted_iota(jnp.int32, VR, 0)


def device(col, row):
    return {"col": col, "row": row}


def greet(col, row):
    barrier = pltpu.get_barrier_semaphore()
    count = 0
    for dc in (0, 1, 3):
        for dr in range(NF):
            if dc == 0 and dr == 0:
                continue
            pl.semaphore_signal(barrier, inc=1, device_id=device(lax.rem(col + dc, 4), lax.rem(row + dr, 4)), device_id_type=MESH)
            count += 1
    return lambda: pl.semaphore_wait(barrier, count)


class Exchange:
    def __init__(self, src_main, src_side, main, side, send_sem, recv_sem, col, row):
        chip = row // 2
        core = lax.rem(row, 2)
        east = lax.rem(col + 1, 4)
        west = lax.rem(col + 3, 4)
        self.full = chip != core
        self.main, self.side, self.recv_sem = main, side, recv_sem
        own = pl.ds(pl.multiple_of(core * NY, NS), NY)
        at_full = pl.ds(pl.multiple_of(jnp.where(chip == 1, 2 * NY, NY + HALO), NS), NY)
        at_part = pl.ds(pl.multiple_of(jnp.where(chip == 1, 3 * NY, 2 * NY), NS), NS)
        from_part = pl.ds(pl.multiple_of(jnp.where(chip == 1, 0, NY - NS), NS), NS)
        self.count = 0

        def remote(s, d, kind, dev):
            return pltpu.make_async_remote_copy(src_ref=s, dst_ref=d, send_sem=send_sem.at[self.count], recv_sem=recv_sem.at[kind], device_id=dev, device_id_type=MESH)

        self.always, self.whole, self.part = [], [], []
        self.local = pltpu.make_async_copy(src_main.at[core], main.at[:, :, own], recv_sem.at[0])
        self.always.append(remote(src_main.at[1 - core], main.at[:, :, own], 0, device(col, chip * 2 + 1 - core)))
        for mm in range(NM):
            near, far = chip * 2 + mm, (1 - chip) * 2 + mm
            self.count += 1
            self.whole.append(remote(src_main.at[mm], main.at[:, :, at_full], 0, device(col, far)))
            self.part.append(remote(src_main.at[mm, :, :, from_part], main.at[:, :, at_part], 0, device(col, far)))
            for e, dev in enumerate((west, east)):
                self.count += 1
                self.whole.append(remote(src_side.at[mm, e], side.at[e, :, at_full], 1, device(dev, far)))
                self.part.append(remote(src_side.at[mm, e, :, from_part], side.at[e, :, at_part], 1, device(dev, far)))
                self.count += 1
                self.always.append(remote(src_side.at[mm, e], side.at[e, :, own], 1, device(dev, near)))

    def branch(self, op):
        @pl.when(self.full)
        def _():
            for copy in self.whole:
                getattr(copy, op)()

        @pl.when(jnp.logical_not(self.full))
        def _():
            for copy in self.part:
                getattr(copy, op)()

    def start(self):
        self.branch("start")
        for copy in self.always:
            copy.start()
        self.local.start()

    def wait(self):
        pltpu.make_async_copy(self.main, self.main, self.recv_sem.at[0]).wait()
        pltpu.make_async_copy(self.side, self.side, self.recv_sem.at[1]).wait()
        for copy in self.always:
            copy.wait_send()
        self.branch("wait_send")


def pack_side(dst, m, group, fields, lane):
    for i in range(NY // NS):
        rows = pl.ds(i * NS, NS)
        first = fields[0](0, rows)
        last = fields[0](NT - 1, rows)
        for n in range(1, len(fields)):
            first = jnp.where(lane < n * SIDE, first, pltpu.roll(fields[n](0, rows), n * SIDE, 1))
            last = jnp.where(lane >= NL - n * SIDE, last, pltpu.roll(fields[n](NT - 1, rows), NL - n * SIDE, 1))
        dst[m, 0, group, rows] = first
        dst[m, 1, group, rows] = last


def window_tile(main, side, f, j, t, lane, group, place):
    here = pl.ds(j, NS, stride=WJ)
    if t < NT:
        return main.at[f, t][here, :]
    e, w = side.at[0, group][here, :], side.at[1, group][here, :]
    if place:
        e, w = pltpu.roll(e, NL - place * SIDE, 1), pltpu.roll(w, place * SIDE, 1)
    return jnp.where(lane < SIDE, e, jnp.where(lane >= NL - SIDE, w, 0.0))


PA = 0.15 * 0.5 / NK * 0.5
PB = 0.2 * 0.5 / NK * 0.5
MOM_UNROLL = 2
TRC_UNROLL = 4
SUB_UNROLL = 1


def rolls(x, amount):
    return [[pltpu.roll(x[j][t], amount, 1) for t in range(NT)] for j in range(NJ)]


def east(x, halo):
    edge, r = lanes_iota() == NL - 1, rolls(x, NL - 1)
    return [[jnp.where(edge, r[j][1] if t == 0 else halo[j], r[j][t]) for t in range(NT)] for j in range(NJ)]


def west(x, halo):
    edge, r = lanes_iota() == 0, rolls(x, 1)
    return [[jnp.where(edge, r[j][0] if t == 1 else halo[j], r[j][t]) for t in range(NT)] for j in range(NJ)]


def north(x, halo):
    edge = subl_iota() == NS - 1
    return x[1:] + [[jnp.where(edge, halo[t], pltpu.roll(x[0][t], NS - 1, 0)) for t in range(NT)]]


def south(x, halo):
    edge = subl_iota() == 0
    return [[jnp.where(edge, halo[t], pltpu.roll(x[NJ - 1][t], 1, 0)) for t in range(NT)]] + x[:-1]


def zipped(fn, *xs):
    return [[fn(*[x[j][t] for x in xs]) for t in range(NT)] for j in range(NJ)]


def strided(ref):
    return [ref[pl.ds(j, NS, stride=NJ), :] for j in range(NJ)]


def read_mask(kl, n):
    return [[kl[n, j * NT + t] for t in range(NT)] for j in range(NJ)]


def factors(mask, k, a, b):
    return zipped(lambda n: jnp.where(n > k + 1, a, jnp.where(n == k + 1, b, 0.0)), mask)


def read_block(ref, index, k):
    return [[ref.at[(*index, t, k)][pl.ds(j, NS, stride=NJ), :] for t in range(NT)] for j in range(NJ)]


def line(ref, m, k):
    return [ref.at[t][pl.ds(m * NK + k, NS, stride=0), :] for t in range(NT)]


def solve(sbuf, f, m, k, side, scale):
    for j in range(NJ):
        for t in range(NT):
            i = j * NT + t
            sbuf[f, m, k + 1, i] = (side[j][t] + sbuf[f, m, k, i]) * scale[j][t]


def tracer_pass(inb, field, ends, uw_all, north_rows, south_rows, south_v, kl, tab, sbuf, f):
    def level(m, k, inv_c):
        uu, vv, sv = read_block(inb, (0, m), k), read_block(inb, (1, m), k), line(south_v, m, k)
        u_w = [[uw_all[m, k, j * NT + t] for t in range(NT)] for j in range(NJ)]
        x = read_block(*field(m), k)
        halo = [ends[m, k, j] for j in range(NJ)]
        x_e, x_w = east(x, halo), west(x, halo)
        x_n = north(x, line(north_rows, m, k))
        x_s = line(south_rows, m, k)
        fx = zipped(lambda u, a, b: u * (a + b), uu, x, x_e)
        fx_w = zipped(lambda u, a, b: u * (a + b), u_w, x, x_w)
        fy = zipped(lambda v, a, b: v * (a + b), vv, x, x_n)
        fy_s = south(fy, [sv[t] * (x_s[t] + x[0][t]) for t in range(NT)])
        solve(sbuf, f, m, k, zipped(lambda a, b, bw, g, gs: (a + a) - (b - bw) - (g - gs), x, fx, fx_w, fy, fy_s), inv_c)

    def levels(q, carry):
        for h in range(TRC_UNROLL):
            k = q * TRC_UNROLL + h
            inv_c = factors(read_mask(kl, 0), k, tab[2, k], tab[3, k])
            for m in range(NM):
                level(m, k, inv_c)
        return carry

    lax.fori_loop(0, NK // TRC_UNROLL, levels, 0)


def step_kernel(u, v, temp, salt, eta, tx, ty, depth, wet, weights, tab,
                sbuf, bsum, kl, rl, out, inb, ends_s, uw_all, hN, hS,
                inb_t, ew, ends_t, corner, sv_east, nu_west, hE, hW, hSE, hNW, colF, colL, rowF, rowL, ksrc, kE, kN,
                wmain, wside, main, side, gsum, fmain, fside, fwin, fwside, wi, nat, state, res,
                in_sem, sendC, recvE, recvW, sendR, recvN, recvS, corn_send, corn_recv, k_send, k_recv,
                w_send, w_recv, f_send, f_recv, out_send, out_recv, loc_sem):
    col = lax.axis_index("col")
    row = lax.axis_index("row")
    chip = row // 2
    core = lax.rem(row, 2)
    east_dev = lax.rem(col + 1, 4)
    west_dev = lax.rem(col + 3, 4)
    north_dev = jnp.minimum(row + 1, 3)
    south_dev = jnp.maximum(row - 1, 0)
    has_north = row < 3
    has_south = row > 0
    fields = (u, v, temp, salt)
    lane = lanes_iota()
    subl = subl_iota()
    l_last, l_first = lane == NL - 1, lane == 0
    s_last, s_first = subl == NS - 1, subl == 0
    zero = jnp.zeros(VR, F32)

    def place(f, *index):
        return inb_t.at[index] if f == 2 else inb.at[(min(f, 2), *index)]

    def held(f, *index):
        return inb_t[index] if f == 2 else inb[(min(f, 2), *index)]

    def load(f, m, t, c):
        part = pl.ds(c * CH, CH)
        return pltpu.make_async_copy(fields[f].at[part, m, :, pl.ds(t * NL, NL)], place(f, m, t, part), in_sem.at[f, m, t, c])

    def each_load(f, c, op):
        for m in range(NM):
            for t in range(NT):
                getattr(load(f, m, t, c), op)()

    for f in range(NF):
        for c in range(NC):
            each_load(f, c, "start")

    for t in range(NT):
        ksrc[t] = wet[:, pl.ds(t * NL, NL)].astype(F32)

    meet = greet(col, row)

    def remote(s, d, ssem, rsem, dc, dr):
        return pltpu.make_async_remote_copy(src_ref=s, dst_ref=d, send_sem=ssem, recv_sem=rsem, device_id=device(dc, dr), device_id_type=MESH)

    k_west = remote(ksrc.at[0], kE, k_send.at[0], k_recv.at[0], west_dev, row)
    k_south = remote(ksrc.at[:, pl.ds(0, NS)], kN, k_send.at[1], k_recv.at[1], col, south_dev)

    def col_copies(f):
        return (remote(colF.at[f], hE.at[f], sendC.at[0, f], recvE.at[f], west_dev, row),
                remote(colL.at[f], hW.at[f], sendC.at[1, f], recvW.at[f], east_dev, row))

    def to_south(f):
        return remote(rowF.at[f], hN.at[f], sendR.at[0, f], recvN.at[f], col, south_dev)

    def to_north(f):
        return remote(rowL.at[f], hS.at[f], sendR.at[1, f], recvS.at[f], col, north_dev)

    corner_north = remote(colF.at[1, pl.ds(NY - NS, NS)], hSE, corn_send.at[0], corn_recv.at[0], west_dev, north_dev)
    corner_south = remote(colL.at[0, pl.ds(0, NS)], hNW, corn_send.at[1], corn_recv.at[1], east_dev, south_dev)

    lane_next = lax.rem(lane + 1, NL)
    for f in range(NF):
        def chunk(c, acc, f=f):
            each_load(f, c, "wait")
            acc = list(acc)
            for q in range(CH):
                k = c * CH + q
                for m in range(NM):
                    spot = 2 * k + m
                    hit, hit_last = lane == spot, lane_next == spot
                    for i in range(NJ):
                        rows = pl.ds(i * NS, NS)
                        both = pltpu.roll(jnp.where(l_first, held(f, m, 0, k, rows), held(f, m, NT - 1, k, rows)), spot, 1)
                        acc[2 * i] = jnp.where(hit, both, acc[2 * i])
                        acc[2 * i + 1] = jnp.where(hit_last, both, acc[2 * i + 1])
                    for t in range(NT):
                        rowF[f, t, pl.ds(m * NK + k, 1), :] = held(f, m, t, k, pl.ds(0, 1))
                        rowL[f, t, pl.ds(m * NK + k, 1), :] = held(f, m, t, k, pl.ds(NY - 1, 1))
            return tuple(acc)

        acc = lax.fori_loop(0, NC, chunk, (zero,) * (2 * NJ))
        for i in range(NJ):
            colF[f, pl.ds(i * NS, NS)] = acc[2 * i]
            colL[f, pl.ds(i * NS, NS)] = acc[2 * i + 1]
        if f == 0:
            meet()
            k_west.start()

            @pl.when(has_south)
            def _():
                k_south.start()

        @pl.when(has_south)
        def _():
            to_south(f).start()

        @pl.when(has_north)
        def _():
            to_north(f).start()
        for copy in col_copies(f):
            copy.start()
        if f == 0:
            @pl.when(has_south)
            def _():
                corner_south.start()
        if f == 1:
            @pl.when(has_north)
            def _():
                corner_north.start()

    for m in range(NM):
        for t in range(NT):
            cols = pl.ds(t * NL, NL)
            for i, arr in enumerate((eta, tx, ty)):
                wmain[m, i, t] = arr[m, :, cols]
            wmain[m, 3, t] = depth[:, cols]
            wmain[m, 4, t] = ksrc[t]
        reads = [lambda t, rows, m=m, i=i: wmain[m, i, t, rows] for i in range(5)]
        pack_side(wside, m, 0, reads[:3], lane)
        pack_side(wside, m, 1, reads[3:], lane)
    windows = Exchange(wmain, wside, main, side, w_send, w_recv, col, row)
    windows.start()

    @pl.when(jnp.logical_not(has_north))
    def _():
        hN[...] = jnp.zeros(hN.shape, F32)
        hNW[...] = jnp.zeros(hNW.shape, F32)
        kN[...] = jnp.zeros(kN.shape, F32)

    @pl.when(jnp.logical_not(has_south))
    def _():
        hS[...] = jnp.zeros(hS.shape, F32)
        hSE[...] = jnp.zeros(hSE.shape, F32)

    for f in range(3):
        for m in range(NM):
            for i in range(NJ * NT):
                sbuf[f, m, 0, i] = zero
    for f in range(2):
        for m in range(NM):
            for i in range(NJ * NT):
                gsum[f, m, i] = zero
                bsum[f, m, i] = zero

    k_west.wait()

    @pl.when(has_south)
    def _():
        k_south.wait_send()
        corner_south.wait_send()
        corner_north.wait_recv()

    @pl.when(has_north)
    def _():
        k_south.wait_recv()
        corner_north.wait_send()
        corner_south.wait_recv()

    for f in range(NF):
        for copy in col_copies(f):
            copy.wait()

        @pl.when(has_south)
        def _():
            to_south(f).wait_send()
            to_north(f).wait_recv()

        @pl.when(has_north)
        def _():
            to_north(f).wait_send()
            to_south(f).wait_recv()

    odd = lax.rem(lane, 2)
    for m in range(NM):
        for f in range(NF):
            for i in range(NJ):
                rows = pl.ds(i * NS, NS)
                ew[f, m, rows] = jnp.where(odd == m, hE[f, rows], pltpu.roll(hW[f, rows], 2, 1))
        corner[m] = jnp.where(odd == m, hSE[pl.ds(NS - 1, NS, stride=0), :], pltpu.roll(hNW[pl.ds(0, NS, stride=0), :], 2, 1))
    for i in range(NM * NK // NS):
        rows = pl.ds(i * NS, NS)
        r = [pltpu.roll(hS[1, t, rows], NL - 1, 1) for t in range(NT)]
        sv_east[0, rows] = jnp.where(l_last, r[1], r[0])
        sv_east[1, rows] = r[1]
        r = [pltpu.roll(hN[0, t, rows], 1, 1) for t in range(NT)]
        nu_west[0, rows] = r[0]
        nu_west[1, rows] = jnp.where(l_first, r[0], r[1])

    k_mid = zipped(lambda x: x, [list(pair) for pair in zip(*[strided(ksrc.at[t]) for t in range(NT)])])
    k_east = zipped(jnp.minimum, k_mid, east(k_mid, [pltpu.roll(x, NL - 1, 1) for x in strided(kE)]))
    k_north = zipped(jnp.minimum, k_mid, north(k_mid, [kN.at[t][pl.ds(0, NS, stride=0), :] for t in range(NT)]))
    for n, mask in enumerate((k_mid, k_east, k_north)):
        for j in range(NJ):
            for t in range(NT):
                kl[n, j * NT + t] = mask[j][t].astype(jnp.int32)

    def block(f, m, k):
        return [[place(f, m, t, k)[pl.ds(j, NS, stride=NJ), :] for t in range(NT)] for j in range(NJ)]

    def momentum(m, k, carry, wet_x, wet_y, inv_x, inv_y):
        cs, cs_n, cs_e = carry
        uu, vv, tt, ss = (block(f, m, k) for f in range(NF))
        amount = NL - 1 - m - 2 * k
        eu, ev, et, es = ([pltpu.roll(x, amount, 1) for x in strided(ew.at[f, m])] for f in range(NF))
        c = pltpu.roll(corner[m], amount, 1)
        for j in range(NJ):
            ends_t[m, k, j] = et[j]
            ends_s[m, k, j] = es[j]
        nu, nv, nt, ns = (line(hN.at[f], m, k) for f in range(NF))
        su, sv = (line(hS.at[f], m, k) for f in range(2))

        half = zipped(lambda s, t: PA * s - PB * t, ss, tt)
        p = zipped(jnp.add, cs, half)
        cs = zipped(jnp.add, p, half)
        half_n = [PA * ns[t] - PB * nt[t] for t in range(NT)]
        p_n = [cs_n[t] + half_n[t] for t in range(NT)]
        cs_n = [p_n[t] + half_n[t] for t in range(NT)]
        half_e = [PA * es[j] - PB * et[j] for j in range(NJ)]
        p_e = [cs_e[j] + half_e[j] for j in range(NJ)]
        cs_e = [p_e[j] + half_e[j] for j in range(NJ)]

        u_e, u_w, v_e, v_w = east(uu, eu), west(uu, eu), east(vv, ev), west(vv, ev)
        for j in range(NJ):
            for t in range(NT):
                uw_all[m, k, j * NT + t] = u_w[j][t]
        u_n, u_s, v_n, v_s = north(uu, nu), south(uu, su), north(vv, nv), south(vv, sv)
        sve, nuw = line(sv_east, m, k), line(nu_west, m, k)
        sve[1] = jnp.where(l_last, c, sve[1])
        nuw[0] = jnp.where(l_first, c, nuw[0])
        a = zipped(jnp.add, vv, v_e)
        v_sum = zipped(jnp.add, a, south(a, [sv[t] + sve[t] for t in range(NT)]))
        b = zipped(jnp.add, uu, u_w)
        u_sum = zipped(jnp.add, b, north(b, [nu[t] + nuw[t] for t in range(NT)]))
        p_e = east(p, p_e)
        p_n = north(p, p_n)

        gu = zipped(lambda w, p, pe, u, ue, uw, vs, un, us: jnp.where(w, (p - pe) - 0.5 * (u * (ue - uw)) - 0.125 * (vs * (un - us)), 0.0),
                    wet_x, p, p_e, uu, u_e, u_w, v_sum, u_n, u_s)
        gv = zipped(lambda w, p, pn, us, ve, vw, v, vn, vs: jnp.where(w, (p - pn) - 0.125 * (us * (ve - vw)) - 0.5 * (v * (vn - vs)), 0.0),
                    wet_y, p, p_n, u_sum, v_e, v_w, vv, v_n, v_s)
        bu = zipped(jnp.add, uu, gu)
        bv = zipped(jnp.add, vv, gv)
        solve(sbuf, 0, m, k, bu, inv_x)
        solve(sbuf, 1, m, k, bv, inv_y)
        for f, (g, b) in enumerate(((gu, bu), (gv, bv))):
            for j in range(NJ):
                for t in range(NT):
                    i = j * NT + t
                    gsum[f, m, i] = gsum[f, m, i] + g[j][t]
                    bsum[f, m, i] = bsum[f, m, i] + b[j][t]
        return cs, cs_n, cs_e

    def momentum_levels(q, carry):
        for h in range(MOM_UNROLL):
            k = q * MOM_UNROLL + h
            mask_x, mask_y = read_mask(kl, 1), read_mask(kl, 2)
            a1, b1 = tab[0, k], tab[1, k]
            inv = factors(mask_x, k, a1, b1), factors(mask_y, k, a1, b1)
            wet_k = [zipped(lambda n: n > k, mask) for mask in (mask_x, mask_y)]
            carry = tuple(momentum(m, k, carry[m], *wet_k, *inv) for m in range(NM))
        return carry

    start = ([[zero] * NT for _ in range(NJ)], [zero] * NT, [zero] * NJ)
    lax.fori_loop(0, NK // MOM_UNROLL, momentum_levels, (start, start))

    for f in range(2):
        for m in range(NM):
            for t in range(NT):
                for j in range(NJ):
                    fmain.at[m, f, t][pl.ds(j, NS, stride=NJ), :] = gsum[f, m, j * NT + t]
    for m in range(NM):
        pack_side(fside, m, 0, [lambda t, rows, m=m, f=f: fmain[m, f, t, rows] for f in range(2)], lane)
    forces = Exchange(fmain, fside, fwin, fwside, f_send, f_recv, col, row)
    forces.start()

    tracer_pass(inb, lambda m: (inb_t, (m,)), ends_t, uw_all, hN.at[2], hS.at[2], hS.at[1], kl, tab, sbuf, 2)

    windows.wait()
    dep = [[window_tile(main, side, 3, j, t, lane, 1, 0) for t in range(WT)] for j in range(WJ)]
    lev = [[window_tile(main, side, 4, j, t, lane, 1, 1) for t in range(WT)] for j in range(WJ)]
    for j in range(WJ):
        row_here = WJ * subl + j
        wall = jnp.logical_and(row_here == 2 * NY - 1, chip == 1)
        dr = [pltpu.roll(dep[j][t], NL - 1, 1) for t in range(WT)]
        lr = [pltpu.roll(lev[j][t], NL - 1, 1) for t in range(WT)]
        for t in range(WT):
            d, k = dep[j][t], lev[j][t]
            de = jnp.where(l_last, dr[(t + 1) % WT], dr[t])
            ke = jnp.where(l_last, lr[(t + 1) % WT], lr[t])
            if j < WJ - 1:
                dn, kn = dep[j + 1][t], lev[j + 1][t]
            else:
                dn, kn = pltpu.roll(dep[0][t], NS - 1, 0), pltpu.roll(lev[0][t], NS - 1, 0)
            kx = jnp.minimum(k, ke)
            ky = jnp.where(wall, 0.0, jnp.minimum(k, kn))
            hx = jnp.where(kx > 0.0, 0.5 * (d + de), 0.0)
            hy = jnp.where(ky > 0.0, 0.5 * (d + dn), 0.0)
            ix = 1.0 / jnp.maximum(kx, 1.0)
            iy = 1.0 / jnp.maximum(ky, 1.0)
            n = j * WT + t
            state[0, n] = window_tile(main, side, 0, j, t, lane, 0, 0)
            for i in (1, 2):
                first = COURANT * window_tile(main, side, i, j, t, lane, 0, i)
                state[i, n] = first
                wi[1 + i, n] = first
            wi[0, n] = (COURANT * COURANT) * hx
            wi[1, n] = (COURANT * COURANT) * hy
            state[3, n] = (COURANT / NSUB) * hx * ix
            state[4, n] = (COURANT / NSUB) * hy * iy
            state[5, n] = zero
            state[6, n] = zero
            if t < NT:
                here = pl.ds(j, NS, stride=WJ)
                nat.at[0, t][here, :] = ix
                nat.at[1, t][here, :] = iy
                nat.at[2, t][here, :] = 1.0 / jnp.where(kx > 0.0, hx, 1.0)
                nat.at[3, t][here, :] = 1.0 / jnp.where(ky > 0.0, hy, 1.0)
    own = pl.ds(pl.multiple_of(core * NY, NS), NY)
    for t in range(NT):
        for i in range(NF):
            rl[i, t] = nat[i, t, own]

    def tail(i, carry):
        s1, s2, n = carry
        w = weights[NSUB - 1 - i]
        return s1 + w, s2 + n * w, n - 1.0

    total, moment, _ = lax.fori_loop(0, NSUB, tail, (0.0, 0.0, float(NSUB)))
    edge_wall = jnp.where(jnp.logical_and(s_first, chip == 0), 0.0, 1.0)
    forces.wait()
    for j in range(WJ):
        for t in range(WT):
            n = j * WT + t
            for f in range(2):
                state[3 + f, n] = state[3 + f, n] * window_tile(fwin, fwside, f, j, t, lane, 0, f)

    def subcycle(i, remain):
        w = weights[i]
        for j in range(WJ):
            r = [pltpu.roll(state[1, j * WT + t], 1, 1) for t in range(WT)]
            for t in range(WT):
                n = j * WT + t
                uw = jnp.where(l_first, r[(t + WT - 1) % WT], r[t])
                if j == 0:
                    vs = pltpu.roll(state[2, (WJ - 1) * WT + t], 1, 0) * edge_wall
                else:
                    vs = state[2, n - WT]
                e = state[0, n] - ((state[1, n] - uw) + (state[2, n] - vs))
                state[0, n] = e
                state[5, n] = state[5, n] + w * e
                state[6, n] = state[6, n] + remain * e
        for j in range(WJ):
            e = [state[0, j * WT + t] for t in range(WT)]
            r = [pltpu.roll(e[t], NL - 1, 1) for t in range(WT)]
            for t in range(WT):
                n = j * WT + t
                ee = jnp.where(l_last, r[(t + 1) % WT], r[t])
                if j == WJ - 1:
                    en = pltpu.roll(state[0, t], NS - 1, 0)
                else:
                    en = state[0, n + WT]
                state[1, n] = (state[1, n] + state[3, n]) - wi[0, n] * (ee - e[t])
                state[2, n] = (state[2, n] + state[4, n]) - wi[1, n] * (en - e[t])
        return remain - w

    lax.fori_loop(0, NSUB, subcycle, total, unroll=SUB_UNROLL)

    scale = 1.0 / COURANT
    for j in range(WJ):
        q = [state[6, j * WT + t] for t in range(WT)]
        r = [pltpu.roll(q[t], NL - 1, 1) for t in range(WT)]
        for t in range(NT):
            n = j * WT + t
            qe = jnp.where(l_last, r[t + 1], r[t])
            qn = pltpu.roll(state[6, t], NS - 1, 0) if j == WJ - 1 else state[6, n + WT]
            here = pl.ds(j, NS, stride=WJ)
            res.at[0, t][here, :] = state[5, n]
            res.at[1, t][here, :] = scale * (total * wi[2, n] + moment * state[3, n] - wi[0, n] * (qe - q[t]))
            res.at[2, t][here, :] = scale * (total * wi[3, n] + moment * state[4, n] - wi[1, n] * (qn - q[t]))
    other = 1 - core
    send = remote(res.at[:, :, pl.ds(pl.multiple_of(other * NY, NS), NY)], out.at[core], out_send, out_recv, col, chip * 2 + other)
    send.start()
    keep = pltpu.make_async_copy(res.at[:, :, pl.ds(pl.multiple_of(core * NY, NS), NY)], out.at[core], loc_sem)
    keep.start()
    keep.wait()
    send.wait()


def step_call(vel_x, vel_y, pot_temp, salinity, surf_eta, trans_x, trans_y, col_depth, wet_levels, weights, tab):
    dma = pltpu.SemaphoreType.DMA
    pair = dma((NM,))
    nreg = NJ * NT
    nwin = WJ * WT

    def vm(*shape):
        return pltpu.VMEM(shape, F32)

    return pl.pallas_call(
        step_kernel,
        out_shape=(
            vm(3, NM, NK + 1, nreg, *VR),
            vm(2, NM, nreg, *VR),
            pltpu.VMEM((3, nreg, *VR), jnp.int32),
            vm(4, NT, NY, NL),
            vm(NM, 3, NT, NY, NL),
            vm(3, NM, NT, NK, NY, NL), vm(NM, NK, NJ, *VR), vm(NM, NK, nreg, *VR), vm(4, NT, NM * NK, NL), vm(4, NT, NM * NK, NL),
        ),
        in_specs=[HBM] * 4 + [VM] * 5 + [SM] * 2,
        out_specs=(VM,) * 10,
        scratch_shapes=[
            vm(NM, NT, NK, NY, NL),
            vm(4, NM, NY, NL), vm(NM, NK, NJ, *VR), vm(NM, *VR), vm(NT, NM * NK, NL), vm(NT, NM * NK, NL),
            vm(NF, NY, NL), vm(NF, NY, NL), vm(*VR), vm(*VR),
            vm(NF, NY, NL), vm(NF, NY, NL), vm(NF, NT, NM * NK, NL), vm(NF, NT, NM * NK, NL),
            vm(NT, NY, NL), vm(NY, NL), vm(NT, *VR),
            vm(NM, 5, NT, NY, NL), vm(NM, 2, 2, NY, NL), vm(5, NT, WY, NL), vm(2, 2, WY, NL),
            vm(2, NM, nreg, *VR),
            vm(NM, 2, NT, NY, NL), vm(NM, 2, 1, NY, NL), vm(2, NT, WY, NL), vm(2, 1, WY, NL),
            vm(4, nwin, *VR), vm(4, NT, WY, NL), vm(7, nwin, *VR), vm(3, NT, WY, NL),
            dma((NF, NM, NT, NC)), dma((NM, NF)), dma((NF,)), dma((NF,)), dma((NM, NF)), dma((NF,)), dma((NF,)), pair, pair, pair, pair,
            dma((NS + NS,)), pair, dma((NS + NS,)), pair, dma, dma, dma,
        ],
        compiler_params=pltpu.CompilerParams(collective_id=0, has_side_effects=True, vmem_limit_bytes=STEP_LIMIT),
        name="ocean_step",
    )(vel_x, vel_y, pot_temp, salinity, surf_eta, trans_x, trans_y, col_depth, wet_levels, weights, tab)


def final_kernel(sbuf, bsum, kl, rl, bo, inb, ends_s, uw_all, hN, hS, tab, eta_out, tx_out, ty_out, u_out, v_out, temp_out, salt_out, xbuf, s_salt, cor, out_sem):
    outs = (u_out, v_out, temp_out, salt_out)
    parts = ((sbuf, 0), (sbuf, 1), (sbuf, 2), (s_salt, 0))

    def store(f, m, t, c):
        part = pl.ds(c * CH, CH)
        return pltpu.make_async_copy(xbuf.at[f, m, t, part], outs[f].at[part, m, :, pl.ds(t * NL, NL)], out_sem.at[f, m, t, c])

    def each_store(fs, c, op):
        for f in fs:
            for m in range(NM):
                for t in range(NT):
                    getattr(store(f, m, t, c), op)()

    zero = jnp.zeros(VR, F32)
    for m in range(NM):
        for t in range(NT):
            cols = pl.ds(t * NL, NL)
            eta_out[m, :, cols] = bo[m, 0, t]
            tx_out[m, :, cols] = bo[m, 1, t]
            ty_out[m, :, cols] = bo[m, 2, t]
            for f in range(2):
                for j in range(NJ):
                    here = pl.ds(j, NS, stride=NJ)
                    i = j * NT + t
                    cor[f, m, i] = bo.at[m, 1 + f, t][here, :] * rl.at[2 + f, t][here, :] - bsum[f, m, i] * rl.at[f, t][here, :]

    def back(fs):
        def chunk(c2, xs):
            c = NC - 1 - c2

            def step(q, xs):
                xs = list(xs)
                for h in range(2):
                    k = c * CH + CH - 1 - 2 * q - h
                    n = 0
                    for f in fs:
                        g = tab[f // 2 * 2, k]
                        for j in range(NJ):
                            for t in range(NT):
                                here = pl.ds(j, NS, stride=NJ)
                                i = j * NT + t
                                if f < 2:
                                    wet = kl[1 + f, i] > k
                                for m in range(NM):
                                    x = parts[f][0][parts[f][1], m, k + 1, i] + g * xs[n]
                                    xs[n] = x
                                    n += 1
                                    xbuf.at[f, m, t, k][here, :] = jnp.where(wet, x + cor[f, m, i], 0.0) if f < 2 else x
                return tuple(xs)

            xs = lax.fori_loop(0, CH // 2, step, xs)
            each_store(fs, c, "start")
            return xs

        lax.fori_loop(0, NC, chunk, (zero,) * (len(fs) * NM * NJ * NT))

    back((2,))
    back((0, 1))
    for m in range(NM):
        for i in range(NJ * NT):
            s_salt[0, m, 0, i] = zero
    tracer_pass(inb, lambda m: (inb, (2, m)), ends_s, uw_all, hN.at[3], hS.at[3], hS.at[1], kl, tab, s_salt, 0)
    back((3,))

    def drain(c, _):
        each_store(range(NF), c, "wait")
        return 0

    lax.fori_loop(0, NC, drain, 0)


def final_call(kept, tab):
    flat = jax.ShapeDtypeStruct((NM, NY, NX), F32)
    block = jax.ShapeDtypeStruct((NK, NM, NY, NX), F32)
    held = [pltpu.with_memory_space_constraint(x, pltpu.VMEM) for x in kept]
    return pl.pallas_call(
        final_kernel,
        out_shape=(flat,) * 3 + (block,) * 4,
        in_specs=[VM] * len(held) + [SM],
        out_specs=(VM,) * 3 + (HBM,) * 4,
        scratch_shapes=[
            pltpu.VMEM((4, NM, NT, NK, NY, NL), F32),
            pltpu.VMEM((1, NM, NK + 1, NJ * NT, *VR), F32),
            pltpu.VMEM((2, NM, NJ * NT, *VR), F32),
            pltpu.SemaphoreType.DMA((4, NM, NT, NC)),
        ],
        compiler_params=pltpu.CompilerParams(vmem_limit_bytes=VMEM_LIMIT),
        name="back_substitution",
    )(*held, tab)


def solution(mesh):
    def local_step(*args):
        tab = level_table()
        return final_call(step_call(*args, tab), tab)

    spec_3d = P(None, None, "row", "col")
    spec_2d = P(None, "row", "col")
    spec_map = P("row", "col")
    return jax.shard_map(local_step, mesh=mesh, in_specs=(spec_3d,) * 4 + (spec_2d,) * 3 + (spec_map,) * 2 + (P(),), out_specs=(spec_2d,) * 3 + (spec_3d,) * 4, check_vma=False)
```

```python
import functools
import jax
import jax.numpy as jnp
import numpy as np
from jax import lax
from jax.experimental import pallas as pl
from jax.experimental.pallas import tpu as pltpu
from jax.sharding import PartitionSpec as P

MESH = pl.DeviceIdType.MESH
F32 = jnp.float32
NK = 60
NM = 2
NY = 32
NL = 128
NS = 8
VR = (NS, NL)
NF = 4
NX = 256
NT = NX // NL
NJ = NY // 8
CH = 10
HALF = CH // 2
NC = NK // CH
HALO = 40
WY = 2 * NY + HALO
WJ = WY // 8
WT = 3
NSUB = 40
COURANT = 0.4
VMEM_LIMIT = 28 << 20
STEP_LIMIT = 28 << 20
SIDE = 40

VM = pl.BlockSpec(memory_space=pltpu.VMEM)
SM = pl.BlockSpec(memory_space=pltpu.SMEM)
HBM = pl.BlockSpec(memory_space=pl.ANY)


def level_table():
    rows = np.zeros((4, NK), np.float64)
    for row, strength in ((0, 1.0), (2, 0.5)):
        scale = 1.0 if strength == 1.0 else 0.5
        div_prev = 0.0
        for k in range(NK):
            if k == 0:
                div = 1.0 + strength
            else:
                div = 1.0 + 2.0 * strength - strength * strength / div_prev
            rows[row, k] = scale / div
            rows[row + 1, k] = scale / (div - strength)
            div_prev = div
    return jnp.asarray(rows, F32)


def lanes_iota():
    return lax.broadcasted_iota(jnp.int32, VR, 1)


def subl_iota():
    return lax.broadcasted_iota(jnp.int32, VR, 0)


def device(col, row):
    return {"col": col, "row": row}


def greet(col, row):
    barrier = pltpu.get_barrier_semaphore()
    count = 0
    for dc in (0, 1, 3):
        for dr in range(NF):
            if dc == 0 and dr == 0:
                continue
            pl.semaphore_signal(barrier, inc=1, device_id=device(lax.rem(col + dc, 4), lax.rem(row + dr, 4)), device_id_type=MESH)
            count += 1
    return lambda: pl.semaphore_wait(barrier, count)


class Exchange:
    def __init__(self, src_main, src_side, main, side, send_sem, recv_sem, col, row):
        chip = row // 2
        core = lax.rem(row, 2)
        east = lax.rem(col + 1, 4)
        west = lax.rem(col + 3, 4)
        self.full = chip != core
        self.main, self.side, self.recv_sem = main, side, recv_sem
        own = pl.ds(pl.multiple_of(core * NY, NS), NY)
        at_full = pl.ds(pl.multiple_of(jnp.where(chip == 1, 2 * NY, NY + HALO), NS), NY)
        at_part = pl.ds(pl.multiple_of(jnp.where(chip == 1, 3 * NY, 2 * NY), NS), NS)
        from_part = pl.ds(pl.multiple_of(jnp.where(chip == 1, 0, NY - NS), NS), NS)
        self.count = 0

        def remote(s, d, kind, dev):
            return pltpu.make_async_remote_copy(src_ref=s, dst_ref=d, send_sem=send_sem.at[self.count], recv_sem=recv_sem.at[kind], device_id=dev, device_id_type=MESH)

        self.always, self.whole, self.part = [], [], []
        self.local = pltpu.make_async_copy(src_main.at[core], main.at[:, :, own], recv_sem.at[0])
        self.always.append(remote(src_main.at[1 - core], main.at[:, :, own], 0, device(col, chip * 2 + 1 - core)))
        for mm in range(NM):
            near, far = chip * 2 + mm, (1 - chip) * 2 + mm
            self.count += 1
            self.whole.append(remote(src_main.at[mm], main.at[:, :, at_full], 0, device(col, far)))
            self.part.append(remote(src_main.at[mm, :, :, from_part], main.at[:, :, at_part], 0, device(col, far)))
            for e, dev in enumerate((west, east)):
                self.count += 1
                self.whole.append(remote(src_side.at[mm, e], side.at[e, :, at_full], 1, device(dev, far)))
                self.part.append(remote(src_side.at[mm, e, :, from_part], side.at[e, :, at_part], 1, device(dev, far)))
                self.count += 1
                self.always.append(remote(src_side.at[mm, e], side.at[e, :, own], 1, device(dev, near)))

    def branch(self, op):
        @pl.when(self.full)
        def _():
            for copy in self.whole:
                getattr(copy, op)()

        @pl.when(jnp.logical_not(self.full))
        def _():
            for copy in self.part:
                getattr(copy, op)()

    def start(self):
        self.branch("start")
        for copy in self.always:
            copy.start()
        self.local.start()

    def wait(self):
        pltpu.make_async_copy(self.main, self.main, self.recv_sem.at[0]).wait()
        pltpu.make_async_copy(self.side, self.side, self.recv_sem.at[1]).wait()
        for copy in self.always:
            copy.wait_send()
        self.branch("wait_send")


def pack_side(dst, m, group, fields, lane):
    for i in range(NY // NS):
        rows = pl.ds(i * NS, NS)
        first = fields[0](0, rows)
        last = fields[0](NT - 1, rows)
        for n in range(1, len(fields)):
            first = jnp.where(lane < n * SIDE, first, pltpu.roll(fields[n](0, rows), n * SIDE, 1))
            last = jnp.where(lane >= NL - n * SIDE, last, pltpu.roll(fields[n](NT - 1, rows), NL - n * SIDE, 1))
        dst[m, 0, group, rows] = first
        dst[m, 1, group, rows] = last


def window_tile(main, side, f, j, t, lane, group, place):
    here = pl.ds(j, NS, stride=WJ)
    if t < NT:
        return main.at[f, t][here, :]
    e, w = side.at[0, group][here, :], side.at[1, group][here, :]
    if place:
        e, w = pltpu.roll(e, NL - place * SIDE, 1), pltpu.roll(w, place * SIDE, 1)
    return jnp.where(lane < SIDE, e, jnp.where(lane >= NL - SIDE, w, 0.0))


PA = 0.15 * 0.5 / NK * 0.5
PB = 0.2 * 0.5 / NK * 0.5
MOM_UNROLL = 3
TRC_UNROLL = 3
BACK_UNROLL = 6
SUB_UNROLL = 4


def rolls(x, amount):
    return [[pltpu.roll(x[j][t], amount, 1) for t in range(NT)] for j in range(NJ)]


def east(x, halo):
    edge, r = lanes_iota() == NL - 1, rolls(x, NL - 1)
    return [[jnp.where(edge, r[j][1] if t == 0 else halo[j], r[j][t]) for t in range(NT)] for j in range(NJ)]


def west(x, halo):
    edge, r = lanes_iota() == 0, rolls(x, 1)
    return [[jnp.where(edge, r[j][0] if t == 1 else halo[j], r[j][t]) for t in range(NT)] for j in range(NJ)]


def north(x, halo):
    edge = subl_iota() == NS - 1
    return x[1:] + [[jnp.where(edge, halo[t], pltpu.roll(x[0][t], NS - 1, 0)) for t in range(NT)]]


def south(x, halo):
    edge = subl_iota() == 0
    return [[jnp.where(edge, halo[t], pltpu.roll(x[NJ - 1][t], 1, 0)) for t in range(NT)]] + x[:-1]


def zipped(fn, *xs):
    return [[fn(*[x[j][t] for x in xs]) for t in range(NT)] for j in range(NJ)]


def strided(ref):
    return [ref[pl.ds(j, NS, stride=NJ), :] for j in range(NJ)]


def read_mask(kl, n):
    return [[kl[n, j * NT + t] for t in range(NT)] for j in range(NJ)]


def factors(mask, k, a, b):
    return zipped(lambda n: jnp.where(n > k + 1, a, jnp.where(n == k + 1, b, 0.0)), mask)


def read_block(ref, index, k):
    return [[ref.at[(*index, t, k)][pl.ds(j, NS, stride=NJ), :] for t in range(NT)] for j in range(NJ)]


def line(ref, m, k):
    return [ref.at[t][pl.ds(m * NK + k, NS, stride=0), :] for t in range(NT)]


def solve(sbuf, f, m, k, side, scale):
    for j in range(NJ):
        for t in range(NT):
            i = j * NT + t
            sbuf[f, m, k + 1, i] = (side[j][t] + sbuf[f, m, k, i]) * scale[j][t]


def tracer_pass(inb, field, ends, uw_all, north_rows, south_rows, south_v, kl, tab, sbuf, f, unroll):
    def level(m, k, inv_c):
        uu, vv, sv = read_block(inb, (0, m), k), read_block(inb, (1, m), k), line(south_v, m, k)
        u_w = [[uw_all[m, k, j * NT + t] for t in range(NT)] for j in range(NJ)]
        x = read_block(*field(m), k)
        halo = [ends[m, k, j] for j in range(NJ)]
        x_e, x_w = east(x, halo), west(x, halo)
        x_n = north(x, line(north_rows, m, k))
        x_s = line(south_rows, m, k)
        fx = zipped(lambda u, a, b: u * (a + b), uu, x, x_e)
        fx_w = zipped(lambda u, a, b: u * (a + b), u_w, x, x_w)
        fy = zipped(lambda v, a, b: v * (a + b), vv, x, x_n)
        fy_s = south(fy, [sv[t] * (x_s[t] + x[0][t]) for t in range(NT)])
        solve(sbuf, f, m, k, zipped(lambda a, b, bw, g, gs: (a + a) - (b - bw) - (g - gs), x, fx, fx_w, fy, fy_s), inv_c)

    def levels(q, carry):
        for h in range(unroll):
            k = q * unroll + h
            inv_c = factors(read_mask(kl, 0), k, tab[2, k], tab[3, k])
            for m in range(NM):
                level(m, k, inv_c)
        return carry

    lax.fori_loop(0, NK // unroll, levels, 0)


def step_kernel(u, v, temp, salt, eta, tx, ty, depth, wet, weights, tab,
                sbuf, bsum, kl, rl, out, inb, ends_s, uw_all, hN, hS,
                inb_t, ew, ends_t, corner, sv_east, nu_west, hE, hW, hSE, hNW, colF, colL, rowF, rowL, ksrc, kE, kN,
                wmain, wside, main, side, gsum, fmain, fside, fwin, fwside, wi, nat, state, res,
                in_sem, sendC, recvE, recvW, sendR, recvN, recvS, corn_send, corn_recv, k_send, k_recv,
                w_send, w_recv, f_send, f_recv, out_send, out_recv, loc_sem):
    col = lax.axis_index("col")
    row = lax.axis_index("row")
    chip = row // 2
    core = lax.rem(row, 2)
    east_dev = lax.rem(col + 1, 4)
    west_dev = lax.rem(col + 3, 4)
    north_dev = jnp.minimum(row + 1, 3)
    south_dev = jnp.maximum(row - 1, 0)
    has_north = row < 3
    has_south = row > 0
    fields = (u, v, temp, salt)
    lane = lanes_iota()
    subl = subl_iota()
    l_last, l_first = lane == NL - 1, lane == 0
    s_last, s_first = subl == NS - 1, subl == 0
    zero = jnp.zeros(VR, F32)

    def place(f, *index):
        return inb_t.at[index] if f == 2 else inb.at[(min(f, 2), *index)]

    def held(f, *index):
        return inb_t[index] if f == 2 else inb[(min(f, 2), *index)]

    def load(f, m, t, c):
        part = pl.ds(c * CH, CH)
        return pltpu.make_async_copy(fields[f].at[part, m, :, pl.ds(t * NL, NL)], place(f, m, t, part), in_sem.at[f, m, t, c])

    def each_load(f, c, op):
        for m in range(NM):
            for t in range(NT):
                getattr(load(f, m, t, c), op)()

    for f in range(NF):
        for c in range(NC):
            each_load(f, c, "start")

    for t in range(NT):
        ksrc[t] = wet[:, pl.ds(t * NL, NL)].astype(F32)

    meet = greet(col, row)

    def remote(s, d, ssem, rsem, dc, dr):
        return pltpu.make_async_remote_copy(src_ref=s, dst_ref=d, send_sem=ssem, recv_sem=rsem, device_id=device(dc, dr), device_id_type=MESH)

    k_west = remote(ksrc.at[0], kE, k_send.at[0], k_recv.at[0], west_dev, row)
    k_south = remote(ksrc.at[:, pl.ds(0, NS)], kN, k_send.at[1], k_recv.at[1], col, south_dev)

    def col_copies(f):
        return (remote(colF.at[f], hE.at[f], sendC.at[0, f], recvE.at[f], west_dev, row),
                remote(colL.at[f], hW.at[f], sendC.at[1, f], recvW.at[f], east_dev, row))

    def to_south(f):
        return remote(rowF.at[f], hN.at[f], sendR.at[0, f], recvN.at[f], col, south_dev)

    def to_north(f):
        return remote(rowL.at[f], hS.at[f], sendR.at[1, f], recvS.at[f], col, north_dev)

    corner_north = remote(colF.at[1, pl.ds(NY - NS, NS)], hSE, corn_send.at[0], corn_recv.at[0], west_dev, north_dev)
    corner_south = remote(colL.at[0, pl.ds(0, NS)], hNW, corn_send.at[1], corn_recv.at[1], east_dev, south_dev)

    lane_next = lax.rem(lane + 1, NL)
    for f in range(NF):
        def chunk(c, acc, f=f):
            each_load(f, c, "wait")
            return lax.fori_loop(0, 2, lambda h, acc: piece(c * CH + h * HALF, acc), acc)

        def piece(k0, acc, f=f):
            acc = list(acc)
            for q in range(HALF):
                k = k0 + q
                for m in range(NM):
                    spot = 2 * k + m
                    hit, hit_last = lane == spot, lane_next == spot
                    for i in range(NJ):
                        rows = pl.ds(i * NS, NS)
                        both = pltpu.roll(jnp.where(l_first, held(f, m, 0, k, rows), held(f, m, NT - 1, k, rows)), spot, 1)
                        acc[2 * i] = jnp.where(hit, both, acc[2 * i])
                        acc[2 * i + 1] = jnp.where(hit_last, both, acc[2 * i + 1])
                    for t in range(NT):
                        rowF[f, t, pl.ds(m * NK + k, 1), :] = held(f, m, t, k, pl.ds(0, 1))
                        rowL[f, t, pl.ds(m * NK + k, 1), :] = held(f, m, t, k, pl.ds(NY - 1, 1))
            return tuple(acc)

        acc = lax.fori_loop(0, NC, chunk, (zero,) * (2 * NJ))
        for i in range(NJ):
            colF[f, pl.ds(i * NS, NS)] = acc[2 * i]
            colL[f, pl.ds(i * NS, NS)] = acc[2 * i + 1]
        if f == 0:
            meet()
            k_west.start()

            @pl.when(has_south)
            def _():
                k_south.start()

        @pl.when(has_south)
        def _():
            to_south(f).start()

        @pl.when(has_north)
        def _():
            to_north(f).start()
        for copy in col_copies(f):
            copy.start()
        if f == 0:
            @pl.when(has_south)
            def _():
                corner_south.start()
        if f == 1:
            @pl.when(has_north)
            def _():
                corner_north.start()

    for m in range(NM):
        for t in range(NT):
            cols = pl.ds(t * NL, NL)
            for i, arr in enumerate((eta, tx, ty)):
                wmain[m, i, t] = arr[m, :, cols]
            wmain[m, 3, t] = depth[:, cols]
            wmain[m, 4, t] = ksrc[t]
        reads = [lambda t, rows, m=m, i=i: wmain[m, i, t, rows] for i in range(5)]
        pack_side(wside, m, 0, reads[:3], lane)
        pack_side(wside, m, 1, reads[3:], lane)
    windows = Exchange(wmain, wside, main, side, w_send, w_recv, col, row)
    windows.start()

    @pl.when(jnp.logical_not(has_north))
    def _():
        hN[...] = jnp.zeros(hN.shape, F32)
        hNW[...] = jnp.zeros(hNW.shape, F32)
        kN[...] = jnp.zeros(kN.shape, F32)

    @pl.when(jnp.logical_not(has_south))
    def _():
        hS[...] = jnp.zeros(hS.shape, F32)
        hSE[...] = jnp.zeros(hSE.shape, F32)

    for f in range(3):
        for m in range(NM):
            for i in range(NJ * NT):
                sbuf[f, m, 0, i] = zero
    for f in range(2):
        for m in range(NM):
            for i in range(NJ * NT):
                gsum[f, m, i] = zero
                bsum[f, m, i] = zero

    k_west.wait()

    @pl.when(has_south)
    def _():
        k_south.wait_send()
        corner_south.wait_send()
        corner_north.wait_recv()

    @pl.when(has_north)
    def _():
        k_south.wait_recv()
        corner_north.wait_send()
        corner_south.wait_recv()

    for f in range(NF):
        for copy in col_copies(f):
            copy.wait()

        @pl.when(has_south)
        def _():
            to_south(f).wait_send()
            to_north(f).wait_recv()

        @pl.when(has_north)
        def _():
            to_north(f).wait_send()
            to_south(f).wait_recv()

    odd = lax.rem(lane, 2)
    for m in range(NM):
        for f in range(NF):
            for i in range(NJ):
                rows = pl.ds(i * NS, NS)
                ew[f, m, rows] = jnp.where(odd == m, hE[f, rows], pltpu.roll(hW[f, rows], 2, 1))
        corner[m] = jnp.where(odd == m, hSE[pl.ds(NS - 1, NS, stride=0), :], pltpu.roll(hNW[pl.ds(0, NS, stride=0), :], 2, 1))
    for i in range(NM * NK // NS):
        rows = pl.ds(i * NS, NS)
        r = [pltpu.roll(hS[1, t, rows], NL - 1, 1) for t in range(NT)]
        sv_east[0, rows] = jnp.where(l_last, r[1], r[0])
        sv_east[1, rows] = r[1]
        r = [pltpu.roll(hN[0, t, rows], 1, 1) for t in range(NT)]
        nu_west[0, rows] = r[0]
        nu_west[1, rows] = jnp.where(l_first, r[0], r[1])

    k_mid = zipped(lambda x: x, [list(pair) for pair in zip(*[strided(ksrc.at[t]) for t in range(NT)])])
    k_east = zipped(jnp.minimum, k_mid, east(k_mid, [pltpu.roll(x, NL - 1, 1) for x in strided(kE)]))
    k_north = zipped(jnp.minimum, k_mid, north(k_mid, [kN.at[t][pl.ds(0, NS, stride=0), :] for t in range(NT)]))
    for n, mask in enumerate((k_mid, k_east, k_north)):
        for j in range(NJ):
            for t in range(NT):
                kl[n, j * NT + t] = mask[j][t].astype(jnp.int32)

    def block(f, m, k):
        return [[place(f, m, t, k)[pl.ds(j, NS, stride=NJ), :] for t in range(NT)] for j in range(NJ)]

    def momentum(m, k, carry, wet_x, wet_y, inv_x, inv_y):
        cs, cs_n, cs_e = carry
        uu, vv, tt, ss = (block(f, m, k) for f in range(NF))
        amount = NL - 1 - m - 2 * k
        eu, ev, et, es = ([pltpu.roll(x, amount, 1) for x in strided(ew.at[f, m])] for f in range(NF))
        c = pltpu.roll(corner[m], amount, 1)
        for j in range(NJ):
            ends_t[m, k, j] = et[j]
            ends_s[m, k, j] = es[j]
        nu, nv, nt, ns = (line(hN.at[f], m, k) for f in range(NF))
        su, sv = (line(hS.at[f], m, k) for f in range(2))

        half = zipped(lambda s, t: PA * s - PB * t, ss, tt)
        p = zipped(jnp.add, cs, half)
        cs = zipped(jnp.add, p, half)
        half_n = [PA * ns[t] - PB * nt[t] for t in range(NT)]
        p_n = [cs_n[t] + half_n[t] for t in range(NT)]
        cs_n = [p_n[t] + half_n[t] for t in range(NT)]
        half_e = [PA * es[j] - PB * et[j] for j in range(NJ)]
        p_e = [cs_e[j] + half_e[j] for j in range(NJ)]
        cs_e = [p_e[j] + half_e[j] for j in range(NJ)]

        u_e, u_w, v_e, v_w = east(uu, eu), west(uu, eu), east(vv, ev), west(vv, ev)
        for j in range(NJ):
            for t in range(NT):
                uw_all[m, k, j * NT + t] = u_w[j][t]
        u_n, u_s, v_n, v_s = north(uu, nu), south(uu, su), north(vv, nv), south(vv, sv)
        sve, nuw = line(sv_east, m, k), line(nu_west, m, k)
        sve[1] = jnp.where(l_last, c, sve[1])
        nuw[0] = jnp.where(l_first, c, nuw[0])
        a = zipped(jnp.add, vv, v_e)
        v_sum = zipped(jnp.add, a, south(a, [sv[t] + sve[t] for t in range(NT)]))
        b = zipped(jnp.add, uu, u_w)
        u_sum = zipped(jnp.add, b, north(b, [nu[t] + nuw[t] for t in range(NT)]))
        p_e = east(p, p_e)
        p_n = north(p, p_n)

        gu = zipped(lambda w, p, pe, u, ue, uw, vs, un, us: jnp.where(w, (p - pe) - 0.5 * (u * (ue - uw)) - 0.125 * (vs * (un - us)), 0.0),
                    wet_x, p, p_e, uu, u_e, u_w, v_sum, u_n, u_s)
        gv = zipped(lambda w, p, pn, us, ve, vw, v, vn, vs: jnp.where(w, (p - pn) - 0.125 * (us * (ve - vw)) - 0.5 * (v * (vn - vs)), 0.0),
                    wet_y, p, p_n, u_sum, v_e, v_w, vv, v_n, v_s)
        bu = zipped(jnp.add, uu, gu)
        bv = zipped(jnp.add, vv, gv)
        solve(sbuf, 0, m, k, bu, inv_x)
        solve(sbuf, 1, m, k, bv, inv_y)
        for f, (g, b) in enumerate(((gu, bu), (gv, bv))):
            for j in range(NJ):
                for t in range(NT):
                    i = j * NT + t
                    gsum[f, m, i] = gsum[f, m, i] + g[j][t]
                    bsum[f, m, i] = bsum[f, m, i] + b[j][t]
        return cs, cs_n, cs_e

    def momentum_levels(q, carry):
        for h in range(MOM_UNROLL):
            k = q * MOM_UNROLL + h
            mask_x, mask_y = read_mask(kl, 1), read_mask(kl, 2)
            a1, b1 = tab[0, k], tab[1, k]
            inv = factors(mask_x, k, a1, b1), factors(mask_y, k, a1, b1)
            wet_k = [zipped(lambda n: n > k, mask) for mask in (mask_x, mask_y)]
            carry = tuple(momentum(m, k, carry[m], *wet_k, *inv) for m in range(NM))
        return carry

    start = ([[zero] * NT for _ in range(NJ)], [zero] * NT, [zero] * NJ)
    lax.fori_loop(0, NK // MOM_UNROLL, momentum_levels, (start, start))

    for f in range(2):
        for m in range(NM):
            for t in range(NT):
                for j in range(NJ):
                    fmain.at[m, f, t][pl.ds(j, NS, stride=NJ), :] = gsum[f, m, j * NT + t]
    for m in range(NM):
        pack_side(fside, m, 0, [lambda t, rows, m=m, f=f: fmain[m, f, t, rows] for f in range(2)], lane)
    forces = Exchange(fmain, fside, fwin, fwside, f_send, f_recv, col, row)
    forces.start()

    tracer_pass(inb, lambda m: (inb_t, (m,)), ends_t, uw_all, hN.at[2], hS.at[2], hS.at[1], kl, tab, sbuf, 2, TRC_UNROLL)

    windows.wait()
    dep = [[window_tile(main, side, 3, j, t, lane, 1, 0) for t in range(WT)] for j in range(WJ)]
    lev = [[window_tile(main, side, 4, j, t, lane, 1, 1) for t in range(WT)] for j in range(WJ)]
    for j in range(WJ):
        row_here = WJ * subl + j
        wall = jnp.logical_and(row_here == 2 * NY - 1, chip == 1)
        dr = [pltpu.roll(dep[j][t], NL - 1, 1) for t in range(WT)]
        lr = [pltpu.roll(lev[j][t], NL - 1, 1) for t in range(WT)]
        for t in range(WT):
            d, k = dep[j][t], lev[j][t]
            de = jnp.where(l_last, dr[(t + 1) % WT], dr[t])
            ke = jnp.where(l_last, lr[(t + 1) % WT], lr[t])
            if j < WJ - 1:
                dn, kn = dep[j + 1][t], lev[j + 1][t]
            else:
                dn, kn = pltpu.roll(dep[0][t], NS - 1, 0), pltpu.roll(lev[0][t], NS - 1, 0)
            kx = jnp.minimum(k, ke)
            ky = jnp.where(wall, 0.0, jnp.minimum(k, kn))
            hx = jnp.where(kx > 0.0, 0.5 * (d + de), 0.0)
            hy = jnp.where(ky > 0.0, 0.5 * (d + dn), 0.0)
            ix = 1.0 / jnp.maximum(kx, 1.0)
            iy = 1.0 / jnp.maximum(ky, 1.0)
            state[0, j, t] = window_tile(main, side, 0, j, t, lane, 0, 0)
            for i in (1, 2):
                first = COURANT * window_tile(main, side, i, j, t, lane, 0, i)
                state[i, j, t] = first
                wi[1 + i, j, t] = first
            wi[0, j, t] = (COURANT * COURANT) * hx
            wi[1, j, t] = (COURANT * COURANT) * hy
            state[3, j, t] = (COURANT / NSUB) * hx * ix
            state[4, j, t] = (COURANT / NSUB) * hy * iy
            state[5, j, t] = zero
            state[6, j, t] = zero
            if t < NT:
                here = pl.ds(j, NS, stride=WJ)
                nat.at[0, t][here, :] = ix
                nat.at[1, t][here, :] = iy
                nat.at[2, t][here, :] = 1.0 / jnp.where(kx > 0.0, hx, 1.0)
                nat.at[3, t][here, :] = 1.0 / jnp.where(ky > 0.0, hy, 1.0)
    own = pl.ds(pl.multiple_of(core * NY, NS), NY)
    for t in range(NT):
        for i in range(NF):
            rl[i, t] = nat[i, t, own]

    def tail(i, carry):
        s1, s2, n = carry
        w = weights[NSUB - 1 - i]
        return s1 + w, s2 + n * w, n - 1.0

    total, moment, _ = lax.fori_loop(0, NSUB, tail, (0.0, 0.0, float(NSUB)))
    edge_wall = jnp.where(jnp.logical_and(s_first, chip == 0), 0.0, 1.0)
    forces.wait()
    for j in range(WJ):
        for t in range(WT):
            for f in range(2):
                state[3 + f, j, t] = state[3 + f, j, t] * window_tile(fwin, fwside, f, j, t, lane, 0, f)

    lane3 = lax.broadcasted_iota(jnp.int32, (WT, *VR), 2)
    wall3 = jnp.broadcast_to(edge_wall, (WT, *VR))

    def subcycle(i, remain):
        w = weights[i]
        for j in range(WJ):
            u, v = state[1, j], state[2, j]
            r = pltpu.roll(u, 1, 2)
            uw = jnp.where(lane3 == 0, jnp.concatenate([r[WT - 1:], r[:WT - 1]], axis=0), r)
            vs = state[2, j - 1] if j else pltpu.roll(state[2, WJ - 1], 1, 1) * wall3
            e = state[0, j] - ((u - uw) + (v - vs))
            state[0, j] = e
            state[5, j] = state[5, j] + w * e
            state[6, j] = state[6, j] + remain * e
        for j in range(WJ):
            e = state[0, j]
            r = pltpu.roll(e, NL - 1, 2)
            ee = jnp.where(lane3 == NL - 1, jnp.concatenate([r[1:], r[:1]], axis=0), r)
            en = state[0, j + 1] if j < WJ - 1 else pltpu.roll(state[0, 0], NS - 1, 1)
            state[1, j] = (state[1, j] + state[3, j]) - wi[0, j] * (ee - e)
            state[2, j] = (state[2, j] + state[4, j]) - wi[1, j] * (en - e)
        return remain - w

    lax.fori_loop(0, NSUB, subcycle, total, unroll=SUB_UNROLL)

    scale = 1.0 / COURANT
    for j in range(WJ):
        q = [state[6, j, t] for t in range(WT)]
        r = [pltpu.roll(q[t], NL - 1, 1) for t in range(WT)]
        for t in range(NT):
            qe = jnp.where(l_last, r[t + 1], r[t])
            qn = pltpu.roll(state[6, 0, t], NS - 1, 0) if j == WJ - 1 else state[6, j + 1, t]
            here = pl.ds(j, NS, stride=WJ)
            res.at[0, t][here, :] = state[5, j, t]
            res.at[1, t][here, :] = scale * (total * wi[2, j, t] + moment * state[3, j, t] - wi[0, j, t] * (qe - q[t]))
            res.at[2, t][here, :] = scale * (total * wi[3, j, t] + moment * state[4, j, t] - wi[1, j, t] * (qn - q[t]))
    other = 1 - core
    send = remote(res.at[:, :, pl.ds(pl.multiple_of(other * NY, NS), NY)], out.at[core], out_send, out_recv, col, chip * 2 + other)
    send.start()
    keep = pltpu.make_async_copy(res.at[:, :, pl.ds(pl.multiple_of(core * NY, NS), NY)], out.at[core], loc_sem)
    keep.start()
    keep.wait()
    send.wait()


def step_call(vel_x, vel_y, pot_temp, salinity, surf_eta, trans_x, trans_y, col_depth, wet_levels, weights, tab):
    dma = pltpu.SemaphoreType.DMA
    pair = dma((NM,))
    nreg = NJ * NT

    def vm(*shape):
        return pltpu.VMEM(shape, F32)

    return pl.pallas_call(
        step_kernel,
        out_shape=(
            vm(3, NM, NK + 1, nreg, *VR),
            vm(2, NM, nreg, *VR),
            pltpu.VMEM((3, nreg, *VR), jnp.int32),
            vm(4, NT, NY, NL),
            vm(NM, 3, NT, NY, NL),
            vm(3, NM, NT, NK, NY, NL), vm(NM, NK, NJ, *VR), vm(NM, NK, nreg, *VR), vm(4, NT, NM * NK, NL), vm(4, NT, NM * NK, NL),
        ),
        in_specs=[HBM] * 4 + [VM] * 5 + [SM] * 2,
        out_specs=(VM,) * 10,
        scratch_shapes=[
            vm(NM, NT, NK, NY, NL),
            vm(4, NM, NY, NL), vm(NM, NK, NJ, *VR), vm(NM, *VR), vm(NT, NM * NK, NL), vm(NT, NM * NK, NL),
            vm(NF, NY, NL), vm(NF, NY, NL), vm(*VR), vm(*VR),
            vm(NF, NY, NL), vm(NF, NY, NL), vm(NF, NT, NM * NK, NL), vm(NF, NT, NM * NK, NL),
            vm(NT, NY, NL), vm(NY, NL), vm(NT, *VR),
            vm(NM, 5, NT, NY, NL), vm(NM, 2, 2, NY, NL), vm(5, NT, WY, NL), vm(2, 2, WY, NL),
            vm(2, NM, nreg, *VR),
            vm(NM, 2, NT, NY, NL), vm(NM, 2, 1, NY, NL), vm(2, NT, WY, NL), vm(2, 1, WY, NL),
            vm(4, WJ, WT, *VR), vm(4, NT, WY, NL), vm(7, WJ, WT, *VR), vm(3, NT, WY, NL),
            dma((NF, NM, NT, NC)), dma((NM, NF)), dma((NF,)), dma((NF,)), dma((NM, NF)), dma((NF,)), dma((NF,)), pair, pair, pair, pair,
            dma((NS + NS,)), pair, dma((NS + NS,)), pair, dma, dma, dma,
        ],
        compiler_params=pltpu.CompilerParams(collective_id=0, has_side_effects=True, vmem_limit_bytes=STEP_LIMIT),
        name="ocean_step",
    )(vel_x, vel_y, pot_temp, salinity, surf_eta, trans_x, trans_y, col_depth, wet_levels, weights, tab)


def final_kernel(sbuf, bsum, kl, rl, bo, inb, ends_s, uw_all, hN, hS, tab, eta_out, tx_out, ty_out, u_out, v_out, temp_out, salt_out, xbuf, s_salt, cor, out_sem):
    outs = (u_out, v_out, temp_out, salt_out)
    parts = ((sbuf, 0), (sbuf, 1), (sbuf, 2), (s_salt, 0))

    def store(f, m, t, c):
        part = pl.ds(c * CH, CH)
        return pltpu.make_async_copy(xbuf.at[f, m, t, part], outs[f].at[part, m, :, pl.ds(t * NL, NL)], out_sem.at[f, m, t, c])

    def each_store(fs, c, op):
        for f in fs:
            for m in range(NM):
                for t in range(NT):
                    getattr(store(f, m, t, c), op)()

    zero = jnp.zeros(VR, F32)
    for m in range(NM):
        for t in range(NT):
            cols = pl.ds(t * NL, NL)
            eta_out[m, :, cols] = bo[m, 0, t]
            tx_out[m, :, cols] = bo[m, 1, t]
            ty_out[m, :, cols] = bo[m, 2, t]
            for f in range(2):
                for j in range(NJ):
                    here = pl.ds(j, NS, stride=NJ)
                    i = j * NT + t
                    cor[f, m, i] = bo.at[m, 1 + f, t][here, :] * rl.at[2 + f, t][here, :] - bsum[f, m, i] * rl.at[f, t][here, :]

    def back(fs):
        def chunk(c2, xs):
            c = NC - 1 - c2

            def step(q, xs):
                xs = list(xs)
                for h in range(2):
                    k = c * CH + CH - 1 - 2 * q - h
                    n = 0
                    for f in fs:
                        g = tab[f // 2 * 2, k]
                        for j in range(NJ):
                            for t in range(NT):
                                here = pl.ds(j, NS, stride=NJ)
                                i = j * NT + t
                                if f < 2:
                                    wet = kl[1 + f, i] > k
                                for m in range(NM):
                                    x = parts[f][0][parts[f][1], m, k + 1, i] + g * xs[n]
                                    xs[n] = x
                                    n += 1
                                    xbuf.at[f, m, t, k][here, :] = jnp.where(wet, x + cor[f, m, i], 0.0) if f < 2 else x
                return tuple(xs)

            xs = lax.fori_loop(0, CH // 2, step, xs)
            each_store(fs, c, "start")
            return xs

        lax.fori_loop(0, NC, chunk, (zero,) * (len(fs) * NM * NJ * NT))

    back((2,))
    back((0, 1))
    for m in range(NM):
        for i in range(NJ * NT):
            s_salt[0, m, 0, i] = zero
    tracer_pass(inb, lambda m: (inb, (2, m)), ends_s, uw_all, hN.at[3], hS.at[3], hS.at[1], kl, tab, s_salt, 0, BACK_UNROLL)
    back((3,))

    def drain(c, _):
        each_store(range(NF), c, "wait")
        return 0

    lax.fori_loop(0, NC, drain, 0)


def final_call(kept, tab):
    flat = jax.ShapeDtypeStruct((NM, NY, NX), F32)
    block = jax.ShapeDtypeStruct((NK, NM, NY, NX), F32)
    held = [pltpu.with_memory_space_constraint(x, pltpu.VMEM) for x in kept]
    return pl.pallas_call(
        final_kernel,
        out_shape=(flat,) * 3 + (block,) * 4,
        in_specs=[VM] * len(held) + [SM],
        out_specs=(VM,) * 3 + (HBM,) * 4,
        scratch_shapes=[
            pltpu.VMEM((4, NM, NT, NK, NY, NL), F32),
            pltpu.VMEM((1, NM, NK + 1, NJ * NT, *VR), F32),
            pltpu.VMEM((2, NM, NJ * NT, *VR), F32),
            pltpu.SemaphoreType.DMA((4, NM, NT, NC)),
        ],
        compiler_params=pltpu.CompilerParams(vmem_limit_bytes=VMEM_LIMIT),
        name="back_substitution",
    )(*held, tab)


def solution(mesh):
    def local_step(*args):
        tab = level_table()
        return final_call(step_call(*args, tab), tab)

    spec_3d = P(None, None, "row", "col")
    spec_2d = P(None, "row", "col")
    spec_map = P("row", "col")
    return jax.shard_map(local_step, mesh=mesh, in_specs=(spec_3d,) * 4 + (spec_2d,) * 3 + (spec_map,) * 2 + (P(),), out_specs=(spec_2d,) * 3 + (spec_3d,) * 4, check_vma=False)
```

```python
import functools
import jax
import jax.numpy as jnp
import numpy as np
from jax import lax
from jax.experimental import pallas as pl
from jax.experimental.pallas import tpu as pltpu
from jax.sharding import PartitionSpec as P

MESH = pl.DeviceIdType.MESH
F32 = jnp.float32
NK = 60
NM = 2
NY = 32
NL = 128
NS = 8
VR = (NS, NL)
NF = 4
NX = 256
NT = NX // NL
NJ = NY // 8
CH = 10
HALF = CH
NC = NK // CH
HALO = 40
WY = 2 * NY + HALO
WJ = WY // 8
WT = 3
NSUB = 40
COURANT = 0.4
VMEM_LIMIT = 28 << 20
STEP_LIMIT = 28 << 20
SIDE = 40

VM = pl.BlockSpec(memory_space=pltpu.VMEM)
SM = pl.BlockSpec(memory_space=pltpu.SMEM)
HBM = pl.BlockSpec(memory_space=pl.ANY)


def level_table():
    rows = np.zeros((4, NK), np.float64)
    for row, strength in ((0, 1.0), (2, 0.5)):
        scale = 1.0 if strength == 1.0 else 0.5
        div_prev = 0.0
        for k in range(NK):
            if k == 0:
                div = 1.0 + strength
            else:
                div = 1.0 + 2.0 * strength - strength * strength / div_prev
            rows[row, k] = scale / div
            rows[row + 1, k] = scale / (div - strength)
            div_prev = div
    return jnp.asarray(rows, F32)


def lanes_iota():
    return lax.broadcasted_iota(jnp.int32, VR, 1)


def subl_iota():
    return lax.broadcasted_iota(jnp.int32, VR, 0)


def device(col, row):
    return {"col": col, "row": row}


def greet(col, row):
    barrier = pltpu.get_barrier_semaphore()
    count = 0
    for dc in (0, 1, 3):
        for dr in range(NF):
            if dc == 0 and dr == 0:
                continue
            pl.semaphore_signal(barrier, inc=1, device_id=device(lax.rem(col + dc, 4), lax.rem(row + dr, 4)), device_id_type=MESH)
            count += 1
    return lambda: pl.semaphore_wait(barrier, count)


class Exchange:
    def __init__(self, src_main, src_side, main, side, send_sem, recv_sem, col, row):
        chip = row // 2
        core = lax.rem(row, 2)
        east = lax.rem(col + 1, 4)
        west = lax.rem(col + 3, 4)
        self.full = chip != core
        self.main, self.side, self.recv_sem = main, side, recv_sem
        own = pl.ds(pl.multiple_of(core * NY, NS), NY)
        at_full = pl.ds(pl.multiple_of(jnp.where(chip == 1, 2 * NY, NY + HALO), NS), NY)
        at_part = pl.ds(pl.multiple_of(jnp.where(chip == 1, 3 * NY, 2 * NY), NS), NS)
        from_part = pl.ds(pl.multiple_of(jnp.where(chip == 1, 0, NY - NS), NS), NS)
        self.count = 0

        def remote(s, d, kind, dev):
            return pltpu.make_async_remote_copy(src_ref=s, dst_ref=d, send_sem=send_sem.at[self.count], recv_sem=recv_sem.at[kind], device_id=dev, device_id_type=MESH)

        self.always, self.whole, self.part = [], [], []
        self.local = pltpu.make_async_copy(src_main.at[core], main.at[:, :, own], recv_sem.at[0])
        self.always.append(remote(src_main.at[1 - core], main.at[:, :, own], 0, device(col, chip * 2 + 1 - core)))
        for mm in range(NM):
            near, far = chip * 2 + mm, (1 - chip) * 2 + mm
            self.count += 1
            self.whole.append(remote(src_main.at[mm], main.at[:, :, at_full], 0, device(col, far)))
            self.part.append(remote(src_main.at[mm, :, :, from_part], main.at[:, :, at_part], 0, device(col, far)))
            for e, dev in enumerate((west, east)):
                self.count += 1
                self.whole.append(remote(src_side.at[mm, e], side.at[e, :, at_full], 1, device(dev, far)))
                self.part.append(remote(src_side.at[mm, e, :, from_part], side.at[e, :, at_part], 1, device(dev, far)))
                self.count += 1
                self.always.append(remote(src_side.at[mm, e], side.at[e, :, own], 1, device(dev, near)))

    def branch(self, op):
        @pl.when(self.full)
        def _():
            for copy in self.whole:
                getattr(copy, op)()

        @pl.when(jnp.logical_not(self.full))
        def _():
            for copy in self.part:
                getattr(copy, op)()

    def start(self):
        self.branch("start")
        for copy in self.always:
            copy.start()
        self.local.start()

    def wait(self):
        pltpu.make_async_copy(self.main, self.main, self.recv_sem.at[0]).wait()
        pltpu.make_async_copy(self.side, self.side, self.recv_sem.at[1]).wait()
        for copy in self.always:
            copy.wait_send()
        self.branch("wait_send")


def pack_side(dst, m, group, fields, lane):
    for i in range(NY // NS):
        rows = pl.ds(i * NS, NS)
        first = fields[0](0, rows)
        last = fields[0](NT - 1, rows)
        for n in range(1, len(fields)):
            first = jnp.where(lane < n * SIDE, first, pltpu.roll(fields[n](0, rows), n * SIDE, 1))
            last = jnp.where(lane >= NL - n * SIDE, last, pltpu.roll(fields[n](NT - 1, rows), NL - n * SIDE, 1))
        dst[m, 0, group, rows] = first
        dst[m, 1, group, rows] = last


def window_tile(main, side, f, j, t, lane, group, place):
    here = pl.ds(j, NS, stride=WJ)
    if t < NT:
        return main.at[f, t][here, :]
    e, w = side.at[0, group][here, :], side.at[1, group][here, :]
    if place:
        e, w = pltpu.roll(e, NL - place * SIDE, 1), pltpu.roll(w, place * SIDE, 1)
    return jnp.where(lane < SIDE, e, jnp.where(lane >= NL - SIDE, w, 0.0))


PA = 0.15 * 0.5 / NK * 0.5
PB = 0.2 * 0.5 / NK * 0.5
MOM_UNROLL = 3
TRC_UNROLL = 3
BACK_UNROLL = 6
SUB_UNROLL = 4


def rolls(x, amount):
    return [[pltpu.roll(x[j][t], amount, 1) for t in range(NT)] for j in range(NJ)]


def east(x, halo):
    edge, r = lanes_iota() == NL - 1, rolls(x, NL - 1)
    return [[jnp.where(edge, r[j][1] if t == 0 else halo[j], r[j][t]) for t in range(NT)] for j in range(NJ)]


def west(x, halo):
    edge, r = lanes_iota() == 0, rolls(x, 1)
    return [[jnp.where(edge, r[j][0] if t == 1 else halo[j], r[j][t]) for t in range(NT)] for j in range(NJ)]


def north(x, halo):
    edge = subl_iota() == NS - 1
    return x[1:] + [[jnp.where(edge, halo[t], pltpu.roll(x[0][t], NS - 1, 0)) for t in range(NT)]]


def south(x, halo):
    edge = subl_iota() == 0
    return [[jnp.where(edge, halo[t], pltpu.roll(x[NJ - 1][t], 1, 0)) for t in range(NT)]] + x[:-1]


def zipped(fn, *xs):
    return [[fn(*[x[j][t] for x in xs]) for t in range(NT)] for j in range(NJ)]


def strided(ref):
    return [ref[pl.ds(j, NS, stride=NJ), :] for j in range(NJ)]


def read_mask(kl, n):
    return [[kl[n, j * NT + t] for t in range(NT)] for j in range(NJ)]


def factors(mask, k, a, b):
    return zipped(lambda n: jnp.where(n > k + 1, a, jnp.where(n == k + 1, b, 0.0)), mask)


def read_block(ref, index, k):
    return [[ref.at[(*index, t, k)][pl.ds(j, NS, stride=NJ), :] for t in range(NT)] for j in range(NJ)]


def line(ref, m, k):
    return [ref.at[t][pl.ds(m * NK + k, NS, stride=0), :] for t in range(NT)]


def solve(sbuf, f, m, k, side, scale):
    for j in range(NJ):
        for t in range(NT):
            i = j * NT + t
            sbuf[f, m, k + 1, i] = (side[j][t] + sbuf[f, m, k, i]) * scale[j][t]


def tracer_pass(inb, field, ends, uw_all, north_rows, south_rows, south_v, kl, tab, sbuf, f, unroll):
    def level(m, k, inv_c):
        uu, vv, sv = read_block(inb, (0, m), k), read_block(inb, (1, m), k), line(south_v, m, k)
        u_w = [[uw_all[m, k, j * NT + t] for t in range(NT)] for j in range(NJ)]
        x = read_block(*field(m), k)
        halo = [ends[m, k, j] for j in range(NJ)]
        x_e, x_w = east(x, halo), west(x, halo)
        x_n = north(x, line(north_rows, m, k))
        x_s = line(south_rows, m, k)
        fx = zipped(lambda u, a, b: u * (a + b), uu, x, x_e)
        fx_w = zipped(lambda u, a, b: u * (a + b), u_w, x, x_w)
        fy = zipped(lambda v, a, b: v * (a + b), vv, x, x_n)
        fy_s = south(fy, [sv[t] * (x_s[t] + x[0][t]) for t in range(NT)])
        solve(sbuf, f, m, k, zipped(lambda a, b, bw, g, gs: (a + a) - (b - bw) - (g - gs), x, fx, fx_w, fy, fy_s), inv_c)

    def levels(q, carry):
        for h in range(unroll):
            k = q * unroll + h
            inv_c = factors(read_mask(kl, 0), k, tab[2, k], tab[3, k])
            for m in range(NM):
                level(m, k, inv_c)
        return carry

    lax.fori_loop(0, NK // unroll, levels, 0)


def step_kernel(u, v, temp, salt, eta, tx, ty, depth, wet, weights, tab,
                sbuf, bsum, kl, rl, out, inb, ends_s, uw_all, hN, hS,
                inb_t, ew, ends_t, corner, sv_east, nu_west, hE, hW, hSE, hNW, colF, colL, rowF, rowL, ksrc, kE, kN,
                wmain, wside, main, side, gsum, fmain, fside, fwin, fwside, wi, nat, state, res,
                in_sem, sendC, recvE, recvW, sendR, recvN, recvS, corn_send, corn_recv, k_send, k_recv,
                w_send, w_recv, f_send, f_recv, out_send, out_recv, loc_sem):
    col = lax.axis_index("col")
    row = lax.axis_index("row")
    chip = row // 2
    core = lax.rem(row, 2)
    east_dev = lax.rem(col + 1, 4)
    west_dev = lax.rem(col + 3, 4)
    north_dev = jnp.minimum(row + 1, 3)
    south_dev = jnp.maximum(row - 1, 0)
    has_north = row < 3
    has_south = row > 0
    fields = (u, v, temp, salt)
    lane = lanes_iota()
    subl = subl_iota()
    l_last, l_first = lane == NL - 1, lane == 0
    s_last, s_first = subl == NS - 1, subl == 0
    zero = jnp.zeros(VR, F32)

    def place(f, *index):
        return inb_t.at[index] if f == 2 else inb.at[(min(f, 2), *index)]

    def held(f, *index):
        return inb_t[index] if f == 2 else inb[(min(f, 2), *index)]

    def load(f, m, t, c):
        part = pl.ds(c * CH, CH)
        return pltpu.make_async_copy(fields[f].at[part, m, :, pl.ds(t * NL, NL)], place(f, m, t, part), in_sem.at[f, m, t, c])

    def each_load(f, c, op):
        for m in range(NM):
            for t in range(NT):
                getattr(load(f, m, t, c), op)()

    for f in range(NF):
        for c in range(NC):
            each_load(f, c, "start")

    for t in range(NT):
        ksrc[t] = wet[:, pl.ds(t * NL, NL)].astype(F32)

    meet = greet(col, row)

    def remote(s, d, ssem, rsem, dc, dr):
        return pltpu.make_async_remote_copy(src_ref=s, dst_ref=d, send_sem=ssem, recv_sem=rsem, device_id=device(dc, dr), device_id_type=MESH)

    k_west = remote(ksrc.at[0], kE, k_send.at[0], k_recv.at[0], west_dev, row)
    k_south = remote(ksrc.at[:, pl.ds(0, NS)], kN, k_send.at[1], k_recv.at[1], col, south_dev)

    def col_copies(f):
        return (remote(colF.at[f], hE.at[f], sendC.at[0, f], recvE.at[f], west_dev, row),
                remote(colL.at[f], hW.at[f], sendC.at[1, f], recvW.at[f], east_dev, row))

    def to_south(f):
        return remote(rowF.at[f], hN.at[f], sendR.at[0, f], recvN.at[f], col, south_dev)

    def to_north(f):
        return remote(rowL.at[f], hS.at[f], sendR.at[1, f], recvS.at[f], col, north_dev)

    corner_north = remote(colF.at[1, pl.ds(NY - NS, NS)], hSE, corn_send.at[0], corn_recv.at[0], west_dev, north_dev)
    corner_south = remote(colL.at[0, pl.ds(0, NS)], hNW, corn_send.at[1], corn_recv.at[1], east_dev, south_dev)

    lane_next = lax.rem(lane + 1, NL)
    for f in range(NF):
        def chunk(c, acc, f=f):
            each_load(f, c, "wait")
            return piece(c * CH, acc)

        def piece(k0, acc, f=f):
            acc = list(acc)
            for q in range(HALF):
                k = k0 + q
                for m in range(NM):
                    spot = 2 * k + m
                    hit, hit_last = lane == spot, lane_next == spot
                    for i in range(NJ):
                        rows = pl.ds(i * NS, NS)
                        both = pltpu.roll(jnp.where(l_first, held(f, m, 0, k, rows), held(f, m, NT - 1, k, rows)), spot, 1)
                        acc[2 * i] = jnp.where(hit, both, acc[2 * i])
                        acc[2 * i + 1] = jnp.where(hit_last, both, acc[2 * i + 1])
                    for t in range(NT):
                        rowF[f, t, pl.ds(m * NK + k, 1), :] = held(f, m, t, k, pl.ds(0, 1))
                        rowL[f, t, pl.ds(m * NK + k, 1), :] = held(f, m, t, k, pl.ds(NY - 1, 1))
            return tuple(acc)

        acc = lax.fori_loop(0, NC, chunk, (zero,) * (2 * NJ))
        for i in range(NJ):
            colF[f, pl.ds(i * NS, NS)] = acc[2 * i]
            colL[f, pl.ds(i * NS, NS)] = acc[2 * i + 1]
        if f == 0:
            meet()
            k_west.start()

            @pl.when(has_south)
            def _():
                k_south.start()

        @pl.when(has_south)
        def _():
            to_south(f).start()

        @pl.when(has_north)
        def _():
            to_north(f).start()
        for copy in col_copies(f):
            copy.start()
        if f == 0:
            @pl.when(has_south)
            def _():
                corner_south.start()
        if f == 1:
            @pl.when(has_north)
            def _():
                corner_north.start()

    for m in range(NM):
        for t in range(NT):
            cols = pl.ds(t * NL, NL)
            for i, arr in enumerate((eta, tx, ty)):
                wmain[m, i, t] = arr[m, :, cols]
            wmain[m, 3, t] = depth[:, cols]
            wmain[m, 4, t] = ksrc[t]
        reads = [lambda t, rows, m=m, i=i: wmain[m, i, t, rows] for i in range(5)]
        pack_side(wside, m, 0, reads[:3], lane)
        pack_side(wside, m, 1, reads[3:], lane)
    windows = Exchange(wmain, wside, main, side, w_send, w_recv, col, row)

    @pl.when(jnp.logical_not(has_north))
    def _():
        hN[...] = jnp.zeros(hN.shape, F32)
        hNW[...] = jnp.zeros(hNW.shape, F32)
        kN[...] = jnp.zeros(kN.shape, F32)

    @pl.when(jnp.logical_not(has_south))
    def _():
        hS[...] = jnp.zeros(hS.shape, F32)
        hSE[...] = jnp.zeros(hSE.shape, F32)

    for f in range(3):
        for m in range(NM):
            for i in range(NJ * NT):
                sbuf[f, m, 0, i] = zero
    for f in range(2):
        for m in range(NM):
            for i in range(NJ * NT):
                gsum[f, m, i] = zero
                bsum[f, m, i] = zero

    k_west.wait()

    @pl.when(has_south)
    def _():
        k_south.wait_send()
        corner_south.wait_send()
        corner_north.wait_recv()

    @pl.when(has_north)
    def _():
        k_south.wait_recv()
        corner_north.wait_send()
        corner_south.wait_recv()

    for f in range(NF):
        for copy in col_copies(f):
            copy.wait()

        @pl.when(has_south)
        def _():
            to_south(f).wait_send()
            to_north(f).wait_recv()

        @pl.when(has_north)
        def _():
            to_north(f).wait_send()
            to_south(f).wait_recv()

    odd = lax.rem(lane, 2)
    for m in range(NM):
        for f in range(NF):
            for i in range(NJ):
                rows = pl.ds(i * NS, NS)
                ew[f, m, rows] = jnp.where(odd == m, hE[f, rows], pltpu.roll(hW[f, rows], 2, 1))
        corner[m] = jnp.where(odd == m, hSE[pl.ds(NS - 1, NS, stride=0), :], pltpu.roll(hNW[pl.ds(0, NS, stride=0), :], 2, 1))
    for i in range(NM * NK // NS):
        rows = pl.ds(i * NS, NS)
        r = [pltpu.roll(hS[1, t, rows], NL - 1, 1) for t in range(NT)]
        sv_east[0, rows] = jnp.where(l_last, r[1], r[0])
        sv_east[1, rows] = r[1]
        r = [pltpu.roll(hN[0, t, rows], 1, 1) for t in range(NT)]
        nu_west[0, rows] = r[0]
        nu_west[1, rows] = jnp.where(l_first, r[0], r[1])

    k_mid = zipped(lambda x: x, [list(pair) for pair in zip(*[strided(ksrc.at[t]) for t in range(NT)])])
    k_east = zipped(jnp.minimum, k_mid, east(k_mid, [pltpu.roll(x, NL - 1, 1) for x in strided(kE)]))
    k_north = zipped(jnp.minimum, k_mid, north(k_mid, [kN.at[t][pl.ds(0, NS, stride=0), :] for t in range(NT)]))
    for n, mask in enumerate((k_mid, k_east, k_north)):
        for j in range(NJ):
            for t in range(NT):
                kl[n, j * NT + t] = mask[j][t].astype(jnp.int32)

    def block(f, m, k):
        return [[place(f, m, t, k)[pl.ds(j, NS, stride=NJ), :] for t in range(NT)] for j in range(NJ)]

    def momentum(m, k, carry, wet_x, wet_y, inv_x, inv_y):
        cs, cs_n, cs_e = carry
        uu, vv, tt, ss = (block(f, m, k) for f in range(NF))
        amount = NL - 1 - m - 2 * k
        eu, ev, et, es = ([pltpu.roll(x, amount, 1) for x in strided(ew.at[f, m])] for f in range(NF))
        c = pltpu.roll(corner[m], amount, 1)
        for j in range(NJ):
            ends_t[m, k, j] = et[j]
            ends_s[m, k, j] = es[j]
        nu, nv, nt, ns = (line(hN.at[f], m, k) for f in range(NF))
        su, sv = (line(hS.at[f], m, k) for f in range(2))

        half = zipped(lambda s, t: PA * s - PB * t, ss, tt)
        p = zipped(jnp.add, cs, half)
        cs = zipped(jnp.add, p, half)
        half_n = [PA * ns[t] - PB * nt[t] for t in range(NT)]
        p_n = [cs_n[t] + half_n[t] for t in range(NT)]
        cs_n = [p_n[t] + half_n[t] for t in range(NT)]
        half_e = [PA * es[j] - PB * et[j] for j in range(NJ)]
        p_e = [cs_e[j] + half_e[j] for j in range(NJ)]
        cs_e = [p_e[j] + half_e[j] for j in range(NJ)]

        u_e, u_w, v_e, v_w = east(uu, eu), west(uu, eu), east(vv, ev), west(vv, ev)
        for j in range(NJ):
            for t in range(NT):
                uw_all[m, k, j * NT + t] = u_w[j][t]
        u_n, u_s, v_n, v_s = north(uu, nu), south(uu, su), north(vv, nv), south(vv, sv)
        sve, nuw = line(sv_east, m, k), line(nu_west, m, k)
        sve[1] = jnp.where(l_last, c, sve[1])
        nuw[0] = jnp.where(l_first, c, nuw[0])
        a = zipped(jnp.add, vv, v_e)
        v_sum = zipped(jnp.add, a, south(a, [sv[t] + sve[t] for t in range(NT)]))
        b = zipped(jnp.add, uu, u_w)
        u_sum = zipped(jnp.add, b, north(b, [nu[t] + nuw[t] for t in range(NT)]))
        p_e = east(p, p_e)
        p_n = north(p, p_n)

        gu = zipped(lambda w, p, pe, u, ue, uw, vs, un, us: jnp.where(w, (p - pe) - 0.5 * (u * (ue - uw)) - 0.125 * (vs * (un - us)), 0.0),
                    wet_x, p, p_e, uu, u_e, u_w, v_sum, u_n, u_s)
        gv = zipped(lambda w, p, pn, us, ve, vw, v, vn, vs: jnp.where(w, (p - pn) - 0.125 * (us * (ve - vw)) - 0.5 * (v * (vn - vs)), 0.0),
                    wet_y, p, p_n, u_sum, v_e, v_w, vv, v_n, v_s)
        bu = zipped(jnp.add, uu, gu)
        bv = zipped(jnp.add, vv, gv)
        solve(sbuf, 0, m, k, bu, inv_x)
        solve(sbuf, 1, m, k, bv, inv_y)
        for f, (g, b) in enumerate(((gu, bu), (gv, bv))):
            for j in range(NJ):
                for t in range(NT):
                    i = j * NT + t
                    gsum[f, m, i] = gsum[f, m, i] + g[j][t]
                    bsum[f, m, i] = bsum[f, m, i] + b[j][t]
        return cs, cs_n, cs_e

    def momentum_levels(q, carry):
        for h in range(MOM_UNROLL):
            k = q * MOM_UNROLL + h
            mask_x, mask_y = read_mask(kl, 1), read_mask(kl, 2)
            a1, b1 = tab[0, k], tab[1, k]
            inv = factors(mask_x, k, a1, b1), factors(mask_y, k, a1, b1)
            wet_k = [zipped(lambda n: n > k, mask) for mask in (mask_x, mask_y)]
            carry = tuple(momentum(m, k, carry[m], *wet_k, *inv) for m in range(NM))
        return carry

    start = ([[zero] * NT for _ in range(NJ)], [zero] * NT, [zero] * NJ)
    windows.start()
    lax.fori_loop(0, NK // MOM_UNROLL, momentum_levels, (start, start))

    for f in range(2):
        for m in range(NM):
            for t in range(NT):
                for j in range(NJ):
                    fmain.at[m, f, t][pl.ds(j, NS, stride=NJ), :] = gsum[f, m, j * NT + t]
    for m in range(NM):
        pack_side(fside, m, 0, [lambda t, rows, m=m, f=f: fmain[m, f, t, rows] for f in range(2)], lane)
    forces = Exchange(fmain, fside, fwin, fwside, f_send, f_recv, col, row)
    forces.start()

    tracer_pass(inb, lambda m: (inb_t, (m,)), ends_t, uw_all, hN.at[2], hS.at[2], hS.at[1], kl, tab, sbuf, 2, TRC_UNROLL)

    windows.wait()
    dep = [[window_tile(main, side, 3, j, t, lane, 1, 0) for t in range(WT)] for j in range(WJ)]
    lev = [[window_tile(main, side, 4, j, t, lane, 1, 1) for t in range(WT)] for j in range(WJ)]
    for j in range(WJ):
        row_here = WJ * subl + j
        wall = jnp.logical_and(row_here == 2 * NY - 1, chip == 1)
        dr = [pltpu.roll(dep[j][t], NL - 1, 1) for t in range(WT)]
        lr = [pltpu.roll(lev[j][t], NL - 1, 1) for t in range(WT)]
        for t in range(WT):
            d, k = dep[j][t], lev[j][t]
            de = jnp.where(l_last, dr[(t + 1) % WT], dr[t])
            ke = jnp.where(l_last, lr[(t + 1) % WT], lr[t])
            if j < WJ - 1:
                dn, kn = dep[j + 1][t], lev[j + 1][t]
            else:
                dn, kn = pltpu.roll(dep[0][t], NS - 1, 0), pltpu.roll(lev[0][t], NS - 1, 0)
            kx = jnp.minimum(k, ke)
            ky = jnp.where(wall, 0.0, jnp.minimum(k, kn))
            hx = jnp.where(kx > 0.0, 0.5 * (d + de), 0.0)
            hy = jnp.where(ky > 0.0, 0.5 * (d + dn), 0.0)
            ix = 1.0 / jnp.maximum(kx, 1.0)
            iy = 1.0 / jnp.maximum(ky, 1.0)
            state[0, j, t] = window_tile(main, side, 0, j, t, lane, 0, 0)
            for i in (1, 2):
                first = COURANT * window_tile(main, side, i, j, t, lane, 0, i)
                state[i, j, t] = first
                wi[1 + i, j, t] = first
            wi[0, j, t] = (COURANT * COURANT) * hx
            wi[1, j, t] = (COURANT * COURANT) * hy
            state[3, j, t] = (COURANT / NSUB) * hx * ix
            state[4, j, t] = (COURANT / NSUB) * hy * iy
            state[5, j, t] = zero
            state[6, j, t] = zero
            if t < NT:
                here = pl.ds(j, NS, stride=WJ)
                nat.at[0, t][here, :] = ix
                nat.at[1, t][here, :] = iy
                nat.at[2, t][here, :] = 1.0 / jnp.where(kx > 0.0, hx, 1.0)
                nat.at[3, t][here, :] = 1.0 / jnp.where(ky > 0.0, hy, 1.0)
    own = pl.ds(pl.multiple_of(core * NY, NS), NY)
    for t in range(NT):
        for i in range(NF):
            rl[i, t] = nat[i, t, own]

    def tail(i, carry):
        s1, s2, n = carry
        w = weights[NSUB - 1 - i]
        return s1 + w, s2 + n * w, n - 1.0

    total, moment, _ = lax.fori_loop(0, NSUB, tail, (0.0, 0.0, float(NSUB)))
    edge_wall = jnp.where(jnp.logical_and(s_first, chip == 0), 0.0, 1.0)
    forces.wait()
    for j in range(WJ):
        for t in range(WT):
            for f in range(2):
                state[3 + f, j, t] = state[3 + f, j, t] * window_tile(fwin, fwside, f, j, t, lane, 0, f)

    lane3 = lax.broadcasted_iota(jnp.int32, (WT, *VR), 2)
    wall3 = jnp.broadcast_to(edge_wall, (WT, *VR))

    def subcycle(i, remain):
        w = weights[i]
        for j in range(WJ):
            u, v = state[1, j], state[2, j]
            r = pltpu.roll(u, 1, 2)
            uw = jnp.where(lane3 == 0, jnp.concatenate([r[WT - 1:], r[:WT - 1]], axis=0), r)
            vs = state[2, j - 1] if j else pltpu.roll(state[2, WJ - 1], 1, 1) * wall3
            e = state[0, j] - ((u - uw) + (v - vs))
            state[0, j] = e
            state[5, j] = state[5, j] + w * e
            state[6, j] = state[6, j] + remain * e
        for j in range(WJ):
            e = state[0, j]
            r = pltpu.roll(e, NL - 1, 2)
            ee = jnp.where(lane3 == NL - 1, jnp.concatenate([r[1:], r[:1]], axis=0), r)
            en = state[0, j + 1] if j < WJ - 1 else pltpu.roll(state[0, 0], NS - 1, 1)
            state[1, j] = (state[1, j] + state[3, j]) - wi[0, j] * (ee - e)
            state[2, j] = (state[2, j] + state[4, j]) - wi[1, j] * (en - e)
        return remain - w

    lax.fori_loop(0, NSUB, subcycle, total, unroll=SUB_UNROLL)

    scale = 1.0 / COURANT
    for j in range(WJ):
        q = [state[6, j, t] for t in range(WT)]
        r = [pltpu.roll(q[t], NL - 1, 1) for t in range(WT)]
        for t in range(NT):
            qe = jnp.where(l_last, r[t + 1], r[t])
            qn = pltpu.roll(state[6, 0, t], NS - 1, 0) if j == WJ - 1 else state[6, j + 1, t]
            here = pl.ds(j, NS, stride=WJ)
            res.at[0, t][here, :] = state[5, j, t]
            res.at[1, t][here, :] = scale * (total * wi[2, j, t] + moment * state[3, j, t] - wi[0, j, t] * (qe - q[t]))
            res.at[2, t][here, :] = scale * (total * wi[3, j, t] + moment * state[4, j, t] - wi[1, j, t] * (qn - q[t]))
    other = 1 - core
    send = remote(res.at[:, :, pl.ds(pl.multiple_of(other * NY, NS), NY)], out.at[core], out_send, out_recv, col, chip * 2 + other)
    send.start()
    keep = pltpu.make_async_copy(res.at[:, :, pl.ds(pl.multiple_of(core * NY, NS), NY)], out.at[core], loc_sem)
    keep.start()
    keep.wait()
    send.wait()


def step_call(vel_x, vel_y, pot_temp, salinity, surf_eta, trans_x, trans_y, col_depth, wet_levels, weights, tab):
    dma = pltpu.SemaphoreType.DMA
    pair = dma((NM,))
    nreg = NJ * NT

    def vm(*shape):
        return pltpu.VMEM(shape, F32)

    return pl.pallas_call(
        step_kernel,
        out_shape=(
            vm(3, NM, NK + 1, nreg, *VR),
            vm(2, NM, nreg, *VR),
            pltpu.VMEM((3, nreg, *VR), jnp.int32),
            vm(4, NT, NY, NL),
            vm(NM, 3, NT, NY, NL),
            vm(3, NM, NT, NK, NY, NL), vm(NM, NK, NJ, *VR), vm(NM, NK, nreg, *VR), vm(4, NT, NM * NK, NL), vm(4, NT, NM * NK, NL),
        ),
        in_specs=[HBM] * 4 + [VM] * 5 + [SM] * 2,
        out_specs=(VM,) * 10,
        scratch_shapes=[
            vm(NM, NT, NK, NY, NL),
            vm(4, NM, NY, NL), vm(NM, NK, NJ, *VR), vm(NM, *VR), vm(NT, NM * NK, NL), vm(NT, NM * NK, NL),
            vm(NF, NY, NL), vm(NF, NY, NL), vm(*VR), vm(*VR),
            vm(NF, NY, NL), vm(NF, NY, NL), vm(NF, NT, NM * NK, NL), vm(NF, NT, NM * NK, NL),
            vm(NT, NY, NL), vm(NY, NL), vm(NT, *VR),
            vm(NM, 5, NT, NY, NL), vm(NM, 2, 2, NY, NL), vm(5, NT, WY, NL), vm(2, 2, WY, NL),
            vm(2, NM, nreg, *VR),
            vm(NM, 2, NT, NY, NL), vm(NM, 2, 1, NY, NL), vm(2, NT, WY, NL), vm(2, 1, WY, NL),
            vm(4, WJ, WT, *VR), vm(4, NT, WY, NL), vm(7, WJ, WT, *VR), vm(3, NT, WY, NL),
            dma((NF, NM, NT, NC)), dma((NM, NF)), dma((NF,)), dma((NF,)), dma((NM, NF)), dma((NF,)), dma((NF,)), pair, pair, pair, pair,
            dma((NS + NS,)), pair, dma((NS + NS,)), pair, dma, dma, dma,
        ],
        compiler_params=pltpu.CompilerParams(collective_id=0, has_side_effects=True, vmem_limit_bytes=STEP_LIMIT),
        name="ocean_step",
    )(vel_x, vel_y, pot_temp, salinity, surf_eta, trans_x, trans_y, col_depth, wet_levels, weights, tab)


def final_kernel(sbuf, bsum, kl, rl, bo, inb, ends_s, uw_all, hN, hS, tab, eta_out, tx_out, ty_out, u_out, v_out, temp_out, salt_out, xbuf, s_salt, cor, out_sem):
    outs = (u_out, v_out, temp_out, salt_out)
    parts = ((sbuf, 0), (sbuf, 1), (sbuf, 2), (s_salt, 0))

    def store(f, m, t, c):
        part = pl.ds(c * CH, CH)
        return pltpu.make_async_copy(xbuf.at[f, m, t, part], outs[f].at[part, m, :, pl.ds(t * NL, NL)], out_sem.at[f, m, t, c])

    def each_store(fs, c, op):
        for f in fs:
            for m in range(NM):
                for t in range(NT):
                    getattr(store(f, m, t, c), op)()

    zero = jnp.zeros(VR, F32)
    for m in range(NM):
        for t in range(NT):
            cols = pl.ds(t * NL, NL)
            eta_out[m, :, cols] = bo[m, 0, t]
            tx_out[m, :, cols] = bo[m, 1, t]
            ty_out[m, :, cols] = bo[m, 2, t]
            for f in range(2):
                for j in range(NJ):
                    here = pl.ds(j, NS, stride=NJ)
                    i = j * NT + t
                    cor[f, m, i] = bo.at[m, 1 + f, t][here, :] * rl.at[2 + f, t][here, :] - bsum[f, m, i] * rl.at[f, t][here, :]

    def back(fs):
        def chunk(c2, xs):
            c = NC - 1 - c2

            def step(q, xs):
                xs = list(xs)
                for h in range(2):
                    k = c * CH + CH - 1 - 2 * q - h
                    n = 0
                    for f in fs:
                        g = tab[f // 2 * 2, k]
                        for j in range(NJ):
                            for t in range(NT):
                                here = pl.ds(j, NS, stride=NJ)
                                i = j * NT + t
                                if f < 2:
                                    wet = kl[1 + f, i] > k
                                for m in range(NM):
                                    x = parts[f][0][parts[f][1], m, k + 1, i] + g * xs[n]
                                    xs[n] = x
                                    n += 1
                                    xbuf.at[f, m, t, k][here, :] = jnp.where(wet, x + cor[f, m, i], 0.0) if f < 2 else x
                return tuple(xs)

            xs = lax.fori_loop(0, CH // 2, step, xs)
            each_store(fs, c, "start")
            return xs

        lax.fori_loop(0, NC, chunk, (zero,) * (len(fs) * NM * NJ * NT))

    back((2,))
    back((0, 1))
    for m in range(NM):
        for i in range(NJ * NT):
            s_salt[0, m, 0, i] = zero
    tracer_pass(inb, lambda m: (inb, (2, m)), ends_s, uw_all, hN.at[3], hS.at[3], hS.at[1], kl, tab, s_salt, 0, BACK_UNROLL)
    back((3,))

    def drain(c, _):
        each_store(range(NF), c, "wait")
        return 0

    lax.fori_loop(0, NC, drain, 0)


def final_call(kept, tab):
    flat = jax.ShapeDtypeStruct((NM, NY, NX), F32)
    block = jax.ShapeDtypeStruct((NK, NM, NY, NX), F32)
    held = [pltpu.with_memory_space_constraint(x, pltpu.VMEM) for x in kept]
    return pl.pallas_call(
        final_kernel,
        out_shape=(flat,) * 3 + (block,) * 4,
        in_specs=[VM] * len(held) + [SM],
        out_specs=(VM,) * 3 + (HBM,) * 4,
        scratch_shapes=[
            pltpu.VMEM((4, NM, NT, NK, NY, NL), F32),
            pltpu.VMEM((1, NM, NK + 1, NJ * NT, *VR), F32),
            pltpu.VMEM((2, NM, NJ * NT, *VR), F32),
            pltpu.SemaphoreType.DMA((4, NM, NT, NC)),
        ],
        compiler_params=pltpu.CompilerParams(vmem_limit_bytes=VMEM_LIMIT),
        name="back_substitution",
    )(*held, tab)


def solution(mesh):
    def local_step(*args):
        tab = level_table()
        return final_call(step_call(*args, tab), tab)

    spec_3d = P(None, None, "row", "col")
    spec_2d = P(None, "row", "col")
    spec_map = P("row", "col")
    return jax.shard_map(local_step, mesh=mesh, in_specs=(spec_3d,) * 4 + (spec_2d,) * 3 + (spec_map,) * 2 + (P(),), out_specs=(spec_2d,) * 3 + (spec_3d,) * 4, check_vma=False)
```

```python
import functools
import jax
import jax.numpy as jnp
import numpy as np
from jax import lax
from jax.experimental import pallas as pl
from jax.experimental.pallas import tpu as pltpu
from jax.sharding import PartitionSpec as P

MESH = pl.DeviceIdType.MESH
F32 = jnp.float32
NK = 60
NM = 2
NY = 32
NL = 128
NS = 8
VR = (NS, NL)
NF = 4
NX = 256
NT = NX // NL
NJ = NY // 8
CH = 10
HALF = CH
NC = NK // CH
HALO = 40
WY = 2 * NY + HALO
WJ = WY // 8
WT = 3
NSUB = 40
COURANT = 0.4
VMEM_LIMIT = 28 << 20
STEP_LIMIT = 28 << 20
SIDE = 40

VM = pl.BlockSpec(memory_space=pltpu.VMEM)
SM = pl.BlockSpec(memory_space=pltpu.SMEM)
HBM = pl.BlockSpec(memory_space=pl.ANY)


def level_table():
    rows = np.zeros((4, NK), np.float64)
    for row, strength in ((0, 1.0), (2, 0.5)):
        scale = 1.0 if strength == 1.0 else 0.5
        div_prev = 0.0
        for k in range(NK):
            if k == 0:
                div = 1.0 + strength
            else:
                div = 1.0 + 2.0 * strength - strength * strength / div_prev
            rows[row, k] = scale / div
            rows[row + 1, k] = scale / (div - strength)
            div_prev = div
    return jnp.asarray(rows, F32)


def lanes_iota():
    return lax.broadcasted_iota(jnp.int32, VR, 1)


def subl_iota():
    return lax.broadcasted_iota(jnp.int32, VR, 0)


def device(col, row):
    return {"col": col, "row": row}


def greet(col, row):
    barrier = pltpu.get_barrier_semaphore()
    count = 0
    for dc in (0, 1, 3):
        for dr in range(NF):
            if dc == 0 and dr == 0:
                continue
            pl.semaphore_signal(barrier, inc=1, device_id=device(lax.rem(col + dc, 4), lax.rem(row + dr, 4)), device_id_type=MESH)
            count += 1
    return lambda: pl.semaphore_wait(barrier, count)


class Exchange:
    def __init__(self, src_main, src_side, main, side, send_sem, recv_sem, col, row):
        chip = row // 2
        core = lax.rem(row, 2)
        east = lax.rem(col + 1, 4)
        west = lax.rem(col + 3, 4)
        self.full = chip != core
        self.main, self.side, self.recv_sem = main, side, recv_sem
        own = pl.ds(pl.multiple_of(core * NY, NS), NY)
        at_full = pl.ds(pl.multiple_of(jnp.where(chip == 1, 2 * NY, NY + HALO), NS), NY)
        at_part = pl.ds(pl.multiple_of(jnp.where(chip == 1, 3 * NY, 2 * NY), NS), NS)
        from_part = pl.ds(pl.multiple_of(jnp.where(chip == 1, 0, NY - NS), NS), NS)
        self.count = 0

        def remote(s, d, kind, dev):
            return pltpu.make_async_remote_copy(src_ref=s, dst_ref=d, send_sem=send_sem.at[self.count], recv_sem=recv_sem.at[kind], device_id=dev, device_id_type=MESH)

        self.always, self.whole, self.part = [], [], []
        self.local = pltpu.make_async_copy(src_main.at[core], main.at[:, :, own], recv_sem.at[0])
        self.always.append(remote(src_main.at[1 - core], main.at[:, :, own], 0, device(col, chip * 2 + 1 - core)))
        for mm in range(NM):
            near, far = chip * 2 + mm, (1 - chip) * 2 + mm
            self.count += 1
            self.whole.append(remote(src_main.at[mm], main.at[:, :, at_full], 0, device(col, far)))
            self.part.append(remote(src_main.at[mm, :, :, from_part], main.at[:, :, at_part], 0, device(col, far)))
            for e, dev in enumerate((west, east)):
                self.count += 1
                self.whole.append(remote(src_side.at[mm, e], side.at[e, :, at_full], 1, device(dev, far)))
                self.part.append(remote(src_side.at[mm, e, :, from_part], side.at[e, :, at_part], 1, device(dev, far)))
                self.count += 1
                self.always.append(remote(src_side.at[mm, e], side.at[e, :, own], 1, device(dev, near)))

    def branch(self, op):
        @pl.when(self.full)
        def _():
            for copy in self.whole:
                getattr(copy, op)()

        @pl.when(jnp.logical_not(self.full))
        def _():
            for copy in self.part:
                getattr(copy, op)()

    def start(self):
        self.branch("start")
        for copy in self.always:
            copy.start()
        self.local.start()

    def wait(self):
        pltpu.make_async_copy(self.main, self.main, self.recv_sem.at[0]).wait()
        pltpu.make_async_copy(self.side, self.side, self.recv_sem.at[1]).wait()
        for copy in self.always:
            copy.wait_send()
        self.branch("wait_send")


def pack_side(dst, m, group, fields, lane):
    for i in range(NY // NS):
        rows = pl.ds(i * NS, NS)
        first = fields[0](0, rows)
        last = fields[0](NT - 1, rows)
        for n in range(1, len(fields)):
            first = jnp.where(lane < n * SIDE, first, pltpu.roll(fields[n](0, rows), n * SIDE, 1))
            last = jnp.where(lane >= NL - n * SIDE, last, pltpu.roll(fields[n](NT - 1, rows), NL - n * SIDE, 1))
        dst[m, 0, group, rows] = first
        dst[m, 1, group, rows] = last


def window_tile(main, side, f, j, t, lane, group, place):
    here = pl.ds(j, NS, stride=WJ)
    if t < NT:
        return main.at[f, t][here, :]
    e, w = side.at[0, group][here, :], side.at[1, group][here, :]
    if place:
        e, w = pltpu.roll(e, NL - place * SIDE, 1), pltpu.roll(w, place * SIDE, 1)
    return jnp.where(lane < SIDE, e, jnp.where(lane >= NL - SIDE, w, 0.0))


PA = 0.15 * 0.5 / NK * 0.5
PB = 0.2 * 0.5 / NK * 0.5
MOM_UNROLL = 3
TRC_UNROLL = 3
BACK_UNROLL = 10
SUB_UNROLL = 5


def rolls(x, amount):
    return [[pltpu.roll(x[j][t], amount, 1) for t in range(NT)] for j in range(NJ)]


def east(x, halo):
    edge, r = lanes_iota() == NL - 1, rolls(x, NL - 1)
    return [[jnp.where(edge, r[j][1] if t == 0 else halo[j], r[j][t]) for t in range(NT)] for j in range(NJ)]


def west(x, halo):
    edge, r = lanes_iota() == 0, rolls(x, 1)
    return [[jnp.where(edge, r[j][0] if t == 1 else halo[j], r[j][t]) for t in range(NT)] for j in range(NJ)]


def north(x, halo):
    edge = subl_iota() == NS - 1
    return x[1:] + [[jnp.where(edge, halo[t], pltpu.roll(x[0][t], NS - 1, 0)) for t in range(NT)]]


def south(x, halo):
    edge = subl_iota() == 0
    return [[jnp.where(edge, halo[t], pltpu.roll(x[NJ - 1][t], 1, 0)) for t in range(NT)]] + x[:-1]


def zipped(fn, *xs):
    return [[fn(*[x[j][t] for x in xs]) for t in range(NT)] for j in range(NJ)]


def strided(ref):
    return [ref[pl.ds(j, NS, stride=NJ), :] for j in range(NJ)]


def read_mask(kl, n):
    return [[kl[n, j * NT + t] for t in range(NT)] for j in range(NJ)]


def factors(mask, k, a, b):
    return zipped(lambda n: jnp.where(n > k + 1, a, jnp.where(n == k + 1, b, 0.0)), mask)


def read_block(ref, index, k):
    return [[ref.at[(*index, t, k)][pl.ds(j, NS, stride=NJ), :] for t in range(NT)] for j in range(NJ)]


def line(ref, m, k):
    return [ref.at[t][pl.ds(m * NK + k, NS, stride=0), :] for t in range(NT)]


def solve(sbuf, f, m, k, side, scale):
    for j in range(NJ):
        for t in range(NT):
            i = j * NT + t
            sbuf[f, m, k + 1, i] = (side[j][t] + sbuf[f, m, k, i]) * scale[j][t]


def tracer_pass(inb, field, ends, uw_all, north_rows, south_rows, south_v, kl, tab, sbuf, f, unroll):
    def level(m, k, inv_c):
        uu, vv, sv = read_block(inb, (0, m), k), read_block(inb, (1, m), k), line(south_v, m, k)
        u_w = [[uw_all[m, k, j * NT + t] for t in range(NT)] for j in range(NJ)]
        x = read_block(*field(m), k)
        halo = [ends[m, k, j] for j in range(NJ)]
        x_e, x_w = east(x, halo), west(x, halo)
        x_n = north(x, line(north_rows, m, k))
        x_s = line(south_rows, m, k)
        fx = zipped(lambda u, a, b: u * (a + b), uu, x, x_e)
        fx_w = zipped(lambda u, a, b: u * (a + b), u_w, x, x_w)
        fy = zipped(lambda v, a, b: v * (a + b), vv, x, x_n)
        fy_s = south(fy, [sv[t] * (x_s[t] + x[0][t]) for t in range(NT)])
        solve(sbuf, f, m, k, zipped(lambda a, b, bw, g, gs: (a + a) - (b - bw) - (g - gs), x, fx, fx_w, fy, fy_s), inv_c)

    def levels(q, carry):
        for h in range(unroll):
            k = q * unroll + h
            inv_c = factors(read_mask(kl, 0), k, tab[2, k], tab[3, k])
            for m in range(NM):
                level(m, k, inv_c)
        return carry

    lax.fori_loop(0, NK // unroll, levels, 0)


def step_kernel(u, v, temp, salt, eta, tx, ty, depth, wet, weights, tab,
                sbuf, bsum, kl, rl, out, inb, ends_s, uw_all, hN, hS,
                inb_t, ew, ends_t, corner, sv_east, nu_west, hE, hW, hSE, hNW, colF, colL, rowF, rowL, ksrc, kE, kN,
                wmain, wside, main, side, gsum, fmain, fside, fwin, fwside, wi, nat, state, res,
                in_sem, sendC, recvE, recvW, sendR, recvN, recvS, corn_send, corn_recv, k_send, k_recv,
                w_send, w_recv, f_send, f_recv, out_send, out_recv, loc_sem):
    col = lax.axis_index("col")
    row = lax.axis_index("row")
    chip = row // 2
    core = lax.rem(row, 2)
    east_dev = lax.rem(col + 1, 4)
    west_dev = lax.rem(col + 3, 4)
    north_dev = jnp.minimum(row + 1, 3)
    south_dev = jnp.maximum(row - 1, 0)
    has_north = row < 3
    has_south = row > 0
    fields = (u, v, temp, salt)
    lane = lanes_iota()
    subl = subl_iota()
    l_last, l_first = lane == NL - 1, lane == 0
    s_last, s_first = subl == NS - 1, subl == 0
    zero = jnp.zeros(VR, F32)

    def place(f, *index):
        return inb_t.at[index] if f == 2 else inb.at[(min(f, 2), *index)]

    def held(f, *index):
        return inb_t[index] if f == 2 else inb[(min(f, 2), *index)]

    def load(f, m, t, c):
        part = pl.ds(c * CH, CH)
        return pltpu.make_async_copy(fields[f].at[part, m, :, pl.ds(t * NL, NL)], place(f, m, t, part), in_sem.at[f, m, t, c])

    def each_load(f, c, op):
        for m in range(NM):
            for t in range(NT):
                getattr(load(f, m, t, c), op)()

    for f in range(NF):
        for c in range(NC):
            each_load(f, c, "start")

    for t in range(NT):
        ksrc[t] = wet[:, pl.ds(t * NL, NL)].astype(F32)

    meet = greet(col, row)

    def remote(s, d, ssem, rsem, dc, dr):
        return pltpu.make_async_remote_copy(src_ref=s, dst_ref=d, send_sem=ssem, recv_sem=rsem, device_id=device(dc, dr), device_id_type=MESH)

    k_west = remote(ksrc.at[0], kE, k_send.at[0], k_recv.at[0], west_dev, row)
    k_south = remote(ksrc.at[:, pl.ds(0, NS)], kN, k_send.at[1], k_recv.at[1], col, south_dev)

    def col_copies(f):
        return (remote(colF.at[f], hE.at[f], sendC.at[0, f], recvE.at[f], west_dev, row),
                remote(colL.at[f], hW.at[f], sendC.at[1, f], recvW.at[f], east_dev, row))

    def to_south(f):
        return remote(rowF.at[f], hN.at[f], sendR.at[0, f], recvN.at[f], col, south_dev)

    def to_north(f):
        return remote(rowL.at[f], hS.at[f], sendR.at[1, f], recvS.at[f], col, north_dev)

    corner_north = remote(colF.at[1, pl.ds(NY - NS, NS)], hSE, corn_send.at[0], corn_recv.at[0], west_dev, north_dev)
    corner_south = remote(colL.at[0, pl.ds(0, NS)], hNW, corn_send.at[1], corn_recv.at[1], east_dev, south_dev)

    lane_next = lax.rem(lane + 1, NL)
    for f in range(NF):
        def chunk(c, acc, f=f):
            each_load(f, c, "wait")
            return piece(c * CH, acc)

        def piece(k0, acc, f=f):
            acc = list(acc)
            for q in range(HALF):
                k = k0 + q
                for m in range(NM):
                    spot = 2 * k + m
                    hit, hit_last = lane == spot, lane_next == spot
                    for i in range(NJ):
                        rows = pl.ds(i * NS, NS)
                        both = pltpu.roll(jnp.where(l_first, held(f, m, 0, k, rows), held(f, m, NT - 1, k, rows)), spot, 1)
                        acc[2 * i] = jnp.where(hit, both, acc[2 * i])
                        acc[2 * i + 1] = jnp.where(hit_last, both, acc[2 * i + 1])
                    for t in range(NT):
                        rowF[f, t, pl.ds(m * NK + k, 1), :] = held(f, m, t, k, pl.ds(0, 1))
                        rowL[f, t, pl.ds(m * NK + k, 1), :] = held(f, m, t, k, pl.ds(NY - 1, 1))
            return tuple(acc)

        acc = lax.fori_loop(0, NC, chunk, (zero,) * (2 * NJ))
        for i in range(NJ):
            colF[f, pl.ds(i * NS, NS)] = acc[2 * i]
            colL[f, pl.ds(i * NS, NS)] = acc[2 * i + 1]
        if f == 0:
            meet()
            k_west.start()

            @pl.when(has_south)
            def _():
                k_south.start()

        @pl.when(has_south)
        def _():
            to_south(f).start()

        @pl.when(has_north)
        def _():
            to_north(f).start()
        for copy in col_copies(f):
            copy.start()
        if f == 0:
            @pl.when(has_south)
            def _():
                corner_south.start()
        if f == 1:
            @pl.when(has_north)
            def _():
                corner_north.start()

    for m in range(NM):
        for t in range(NT):
            cols = pl.ds(t * NL, NL)
            for i, arr in enumerate((eta, tx, ty)):
                wmain[m, i, t] = arr[m, :, cols]
            wmain[m, 3, t] = depth[:, cols]
            wmain[m, 4, t] = ksrc[t]
        reads = [lambda t, rows, m=m, i=i: wmain[m, i, t, rows] for i in range(5)]
        pack_side(wside, m, 0, reads[:3], lane)
        pack_side(wside, m, 1, reads[3:], lane)
    windows = Exchange(wmain, wside, main, side, w_send, w_recv, col, row)

    @pl.when(jnp.logical_not(has_north))
    def _():
        hN[...] = jnp.zeros(hN.shape, F32)
        hNW[...] = jnp.zeros(hNW.shape, F32)
        kN[...] = jnp.zeros(kN.shape, F32)

    @pl.when(jnp.logical_not(has_south))
    def _():
        hS[...] = jnp.zeros(hS.shape, F32)
        hSE[...] = jnp.zeros(hSE.shape, F32)

    for f in range(3):
        for m in range(NM):
            for i in range(NJ * NT):
                sbuf[f, m, 0, i] = zero
    for f in range(2):
        for m in range(NM):
            for i in range(NJ * NT):
                gsum[f, m, i] = zero
                bsum[f, m, i] = zero

    k_west.wait()

    @pl.when(has_south)
    def _():
        k_south.wait_send()
        corner_south.wait_send()
        corner_north.wait_recv()

    @pl.when(has_north)
    def _():
        k_south.wait_recv()
        corner_north.wait_send()
        corner_south.wait_recv()

    for f in range(NF):
        for copy in col_copies(f):
            copy.wait()

        @pl.when(has_south)
        def _():
            to_south(f).wait_send()
            to_north(f).wait_recv()

        @pl.when(has_north)
        def _():
            to_north(f).wait_send()
            to_south(f).wait_recv()

    odd = lax.rem(lane, 2)
    for m in range(NM):
        for f in range(NF):
            for i in range(NJ):
                rows = pl.ds(i * NS, NS)
                ew[f, m, rows] = jnp.where(odd == m, hE[f, rows], pltpu.roll(hW[f, rows], 2, 1))
        corner[m] = jnp.where(odd == m, hSE[pl.ds(NS - 1, NS, stride=0), :], pltpu.roll(hNW[pl.ds(0, NS, stride=0), :], 2, 1))
    for i in range(NM * NK // NS):
        rows = pl.ds(i * NS, NS)
        r = [pltpu.roll(hS[1, t, rows], NL - 1, 1) for t in range(NT)]
        sv_east[0, rows] = jnp.where(l_last, r[1], r[0])
        sv_east[1, rows] = r[1]
        r = [pltpu.roll(hN[0, t, rows], 1, 1) for t in range(NT)]
        nu_west[0, rows] = r[0]
        nu_west[1, rows] = jnp.where(l_first, r[0], r[1])

    k_mid = zipped(lambda x: x, [list(pair) for pair in zip(*[strided(ksrc.at[t]) for t in range(NT)])])
    k_east = zipped(jnp.minimum, k_mid, east(k_mid, [pltpu.roll(x, NL - 1, 1) for x in strided(kE)]))
    k_north = zipped(jnp.minimum, k_mid, north(k_mid, [kN.at[t][pl.ds(0, NS, stride=0), :] for t in range(NT)]))
    for n, mask in enumerate((k_mid, k_east, k_north)):
        for j in range(NJ):
            for t in range(NT):
                kl[n, j * NT + t] = mask[j][t].astype(jnp.int32)

    def block(f, m, k):
        return [[place(f, m, t, k)[pl.ds(j, NS, stride=NJ), :] for t in range(NT)] for j in range(NJ)]

    def momentum(m, k, carry, wet_x, wet_y, inv_x, inv_y):
        cs, cs_n, cs_e = carry
        uu, vv, tt, ss = (block(f, m, k) for f in range(NF))
        amount = NL - 1 - m - 2 * k
        eu, ev, et, es = ([pltpu.roll(x, amount, 1) for x in strided(ew.at[f, m])] for f in range(NF))
        c = pltpu.roll(corner[m], amount, 1)
        for j in range(NJ):
            ends_t[m, k, j] = et[j]
            ends_s[m, k, j] = es[j]
        nu, nv, nt, ns = (line(hN.at[f], m, k) for f in range(NF))
        su, sv = (line(hS.at[f], m, k) for f in range(2))

        half = zipped(lambda s, t: PA * s - PB * t, ss, tt)
        p = zipped(jnp.add, cs, half)
        cs = zipped(jnp.add, p, half)
        half_n = [PA * ns[t] - PB * nt[t] for t in range(NT)]
        p_n = [cs_n[t] + half_n[t] for t in range(NT)]
        cs_n = [p_n[t] + half_n[t] for t in range(NT)]
        half_e = [PA * es[j] - PB * et[j] for j in range(NJ)]
        p_e = [cs_e[j] + half_e[j] for j in range(NJ)]
        cs_e = [p_e[j] + half_e[j] for j in range(NJ)]

        u_e, u_w, v_e, v_w = east(uu, eu), west(uu, eu), east(vv, ev), west(vv, ev)
        for j in range(NJ):
            for t in range(NT):
                uw_all[m, k, j * NT + t] = u_w[j][t]
        u_n, u_s, v_n, v_s = north(uu, nu), south(uu, su), north(vv, nv), south(vv, sv)
        sve, nuw = line(sv_east, m, k), line(nu_west, m, k)
        sve[1] = jnp.where(l_last, c, sve[1])
        nuw[0] = jnp.where(l_first, c, nuw[0])
        a = zipped(jnp.add, vv, v_e)
        v_sum = zipped(jnp.add, a, south(a, [sv[t] + sve[t] for t in range(NT)]))
        b = zipped(jnp.add, uu, u_w)
        u_sum = zipped(jnp.add, b, north(b, [nu[t] + nuw[t] for t in range(NT)]))
        p_e = east(p, p_e)
        p_n = north(p, p_n)

        gu = zipped(lambda w, p, pe, u, ue, uw, vs, un, us: jnp.where(w, (p - pe) - 0.5 * (u * (ue - uw)) - 0.125 * (vs * (un - us)), 0.0),
                    wet_x, p, p_e, uu, u_e, u_w, v_sum, u_n, u_s)
        gv = zipped(lambda w, p, pn, us, ve, vw, v, vn, vs: jnp.where(w, (p - pn) - 0.125 * (us * (ve - vw)) - 0.5 * (v * (vn - vs)), 0.0),
                    wet_y, p, p_n, u_sum, v_e, v_w, vv, v_n, v_s)
        bu = zipped(jnp.add, uu, gu)
        bv = zipped(jnp.add, vv, gv)
        solve(sbuf, 0, m, k, bu, inv_x)
        solve(sbuf, 1, m, k, bv, inv_y)
        for f, (g, b) in enumerate(((gu, bu), (gv, bv))):
            for j in range(NJ):
                for t in range(NT):
                    i = j * NT + t
                    gsum[f, m, i] = gsum[f, m, i] + g[j][t]
                    bsum[f, m, i] = bsum[f, m, i] + b[j][t]
        return cs, cs_n, cs_e

    def momentum_levels(q, carry):
        for h in range(MOM_UNROLL):
            k = q * MOM_UNROLL + h
            mask_x, mask_y = read_mask(kl, 1), read_mask(kl, 2)
            a1, b1 = tab[0, k], tab[1, k]
            inv = factors(mask_x, k, a1, b1), factors(mask_y, k, a1, b1)
            wet_k = [zipped(lambda n: n > k, mask) for mask in (mask_x, mask_y)]
            carry = tuple(momentum(m, k, carry[m], *wet_k, *inv) for m in range(NM))
        return carry

    start = ([[zero] * NT for _ in range(NJ)], [zero] * NT, [zero] * NJ)
    windows.start()
    lax.fori_loop(0, NK // MOM_UNROLL, momentum_levels, (start, start))

    for f in range(2):
        for m in range(NM):
            for t in range(NT):
                for j in range(NJ):
                    fmain.at[m, f, t][pl.ds(j, NS, stride=NJ), :] = gsum[f, m, j * NT + t]
    for m in range(NM):
        pack_side(fside, m, 0, [lambda t, rows, m=m, f=f: fmain[m, f, t, rows] for f in range(2)], lane)
    forces = Exchange(fmain, fside, fwin, fwside, f_send, f_recv, col, row)
    forces.start()

    tracer_pass(inb, lambda m: (inb_t, (m,)), ends_t, uw_all, hN.at[2], hS.at[2], hS.at[1], kl, tab, sbuf, 2, TRC_UNROLL)

    windows.wait()
    dep = [[window_tile(main, side, 3, j, t, lane, 1, 0) for t in range(WT)] for j in range(WJ)]
    lev = [[window_tile(main, side, 4, j, t, lane, 1, 1) for t in range(WT)] for j in range(WJ)]
    for j in range(WJ):
        row_here = WJ * subl + j
        wall = jnp.logical_and(row_here == 2 * NY - 1, chip == 1)
        dr = [pltpu.roll(dep[j][t], NL - 1, 1) for t in range(WT)]
        lr = [pltpu.roll(lev[j][t], NL - 1, 1) for t in range(WT)]
        for t in range(WT):
            d, k = dep[j][t], lev[j][t]
            de = jnp.where(l_last, dr[(t + 1) % WT], dr[t])
            ke = jnp.where(l_last, lr[(t + 1) % WT], lr[t])
            if j < WJ - 1:
                dn, kn = dep[j + 1][t], lev[j + 1][t]
            else:
                dn, kn = pltpu.roll(dep[0][t], NS - 1, 0), pltpu.roll(lev[0][t], NS - 1, 0)
            kx = jnp.minimum(k, ke)
            ky = jnp.where(wall, 0.0, jnp.minimum(k, kn))
            hx = jnp.where(kx > 0.0, 0.5 * (d + de), 0.0)
            hy = jnp.where(ky > 0.0, 0.5 * (d + dn), 0.0)
            ix = 1.0 / jnp.maximum(kx, 1.0)
            iy = 1.0 / jnp.maximum(ky, 1.0)
            state[0, j, t] = window_tile(main, side, 0, j, t, lane, 0, 0)
            for i in (1, 2):
                first = COURANT * window_tile(main, side, i, j, t, lane, 0, i)
                state[i, j, t] = first
                wi[1 + i, j, t] = first
            wi[0, j, t] = (COURANT * COURANT) * hx
            wi[1, j, t] = (COURANT * COURANT) * hy
            state[3, j, t] = (COURANT / NSUB) * hx * ix
            state[4, j, t] = (COURANT / NSUB) * hy * iy
            state[5, j, t] = zero
            state[6, j, t] = zero
            if t < NT:
                here = pl.ds(j, NS, stride=WJ)
                nat.at[0, t][here, :] = ix
                nat.at[1, t][here, :] = iy
                nat.at[2, t][here, :] = 1.0 / jnp.where(kx > 0.0, hx, 1.0)
                nat.at[3, t][here, :] = 1.0 / jnp.where(ky > 0.0, hy, 1.0)
    own = pl.ds(pl.multiple_of(core * NY, NS), NY)
    for t in range(NT):
        for i in range(NF):
            rl[i, t] = nat[i, t, own]

    def tail(i, carry):
        s1, s2, n = carry
        w = weights[NSUB - 1 - i]
        return s1 + w, s2 + n * w, n - 1.0

    total, moment, _ = lax.fori_loop(0, NSUB, tail, (0.0, 0.0, float(NSUB)))
    edge_wall = jnp.where(jnp.logical_and(s_first, chip == 0), 0.0, 1.0)
    forces.wait()
    for j in range(WJ):
        for t in range(WT):
            for f in range(2):
                state[3 + f, j, t] = state[3 + f, j, t] * window_tile(fwin, fwside, f, j, t, lane, 0, f)

    lane3 = lax.broadcasted_iota(jnp.int32, (WT, *VR), 2)
    wall3 = jnp.broadcast_to(edge_wall, (WT, *VR))

    def subcycle(i, remain):
        w = weights[i]
        for j in range(WJ):
            u, v = state[1, j], state[2, j]
            r = pltpu.roll(u, 1, 2)
            uw = jnp.where(lane3 == 0, jnp.concatenate([r[WT - 1:], r[:WT - 1]], axis=0), r)
            vs = state[2, j - 1] if j else pltpu.roll(state[2, WJ - 1], 1, 1) * wall3
            e = state[0, j] - ((u - uw) + (v - vs))
            state[0, j] = e
            state[5, j] = state[5, j] + w * e
            state[6, j] = state[6, j] + remain * e
        for j in range(WJ):
            e = state[0, j]
            r = pltpu.roll(e, NL - 1, 2)
            ee = jnp.where(lane3 == NL - 1, jnp.concatenate([r[1:], r[:1]], axis=0), r)
            en = state[0, j + 1] if j < WJ - 1 else pltpu.roll(state[0, 0], NS - 1, 1)
            state[1, j] = (state[1, j] + state[3, j]) - wi[0, j] * (ee - e)
            state[2, j] = (state[2, j] + state[4, j]) - wi[1, j] * (en - e)
        return remain - w

    lax.fori_loop(0, NSUB, subcycle, total, unroll=SUB_UNROLL)

    scale = 1.0 / COURANT
    for j in range(WJ):
        q = [state[6, j, t] for t in range(WT)]
        r = [pltpu.roll(q[t], NL - 1, 1) for t in range(WT)]
        for t in range(NT):
            qe = jnp.where(l_last, r[t + 1], r[t])
            qn = pltpu.roll(state[6, 0, t], NS - 1, 0) if j == WJ - 1 else state[6, j + 1, t]
            here = pl.ds(j, NS, stride=WJ)
            res.at[0, t][here, :] = state[5, j, t]
            res.at[1, t][here, :] = scale * (total * wi[2, j, t] + moment * state[3, j, t] - wi[0, j, t] * (qe - q[t]))
            res.at[2, t][here, :] = scale * (total * wi[3, j, t] + moment * state[4, j, t] - wi[1, j, t] * (qn - q[t]))
    other = 1 - core
    send = remote(res.at[:, :, pl.ds(pl.multiple_of(other * NY, NS), NY)], out.at[core], out_send, out_recv, col, chip * 2 + other)
    send.start()
    keep = pltpu.make_async_copy(res.at[:, :, pl.ds(pl.multiple_of(core * NY, NS), NY)], out.at[core], loc_sem)
    keep.start()
    keep.wait()
    send.wait()


def step_call(vel_x, vel_y, pot_temp, salinity, surf_eta, trans_x, trans_y, col_depth, wet_levels, weights, tab):
    dma = pltpu.SemaphoreType.DMA
    pair = dma((NM,))
    nreg = NJ * NT

    def vm(*shape):
        return pltpu.VMEM(shape, F32)

    return pl.pallas_call(
        step_kernel,
        out_shape=(
            vm(3, NM, NK + 1, nreg, *VR),
            vm(2, NM, nreg, *VR),
            pltpu.VMEM((3, nreg, *VR), jnp.int32),
            vm(4, NT, NY, NL),
            vm(NM, 3, NT, NY, NL),
            vm(3, NM, NT, NK, NY, NL), vm(NM, NK, NJ, *VR), vm(NM, NK, nreg, *VR), vm(4, NT, NM * NK, NL), vm(4, NT, NM * NK, NL),
        ),
        in_specs=[HBM] * 4 + [VM] * 5 + [SM] * 2,
        out_specs=(VM,) * 10,
        scratch_shapes=[
            vm(NM, NT, NK, NY, NL),
            vm(4, NM, NY, NL), vm(NM, NK, NJ, *VR), vm(NM, *VR), vm(NT, NM * NK, NL), vm(NT, NM * NK, NL),
            vm(NF, NY, NL), vm(NF, NY, NL), vm(*VR), vm(*VR),
            vm(NF, NY, NL), vm(NF, NY, NL), vm(NF, NT, NM * NK, NL), vm(NF, NT, NM * NK, NL),
            vm(NT, NY, NL), vm(NY, NL), vm(NT, *VR),
            vm(NM, 5, NT, NY, NL), vm(NM, 2, 2, NY, NL), vm(5, NT, WY, NL), vm(2, 2, WY, NL),
            vm(2, NM, nreg, *VR),
            vm(NM, 2, NT, NY, NL), vm(NM, 2, 1, NY, NL), vm(2, NT, WY, NL), vm(2, 1, WY, NL),
            vm(4, WJ, WT, *VR), vm(4, NT, WY, NL), vm(7, WJ, WT, *VR), vm(3, NT, WY, NL),
            dma((NF, NM, NT, NC)), dma((NM, NF)), dma((NF,)), dma((NF,)), dma((NM, NF)), dma((NF,)), dma((NF,)), pair, pair, pair, pair,
            dma((NS + NS,)), pair, dma((NS + NS,)), pair, dma, dma, dma,
        ],
        compiler_params=pltpu.CompilerParams(collective_id=0, has_side_effects=True, vmem_limit_bytes=STEP_LIMIT),
        name="ocean_step",
    )(vel_x, vel_y, pot_temp, salinity, surf_eta, trans_x, trans_y, col_depth, wet_levels, weights, tab)


def final_kernel(sbuf, bsum, kl, rl, bo, inb, ends_s, uw_all, hN, hS, tab, eta_out, tx_out, ty_out, u_out, v_out, temp_out, salt_out, xbuf, s_salt, cor, out_sem):
    outs = (u_out, v_out, temp_out, salt_out)
    parts = ((sbuf, 0), (sbuf, 1), (sbuf, 2), (s_salt, 0))

    def store(f, m, t, c):
        part = pl.ds(c * CH, CH)
        return pltpu.make_async_copy(xbuf.at[f, m, t, part], outs[f].at[part, m, :, pl.ds(t * NL, NL)], out_sem.at[f, m, t, c])

    def each_store(fs, c, op):
        for f in fs:
            for m in range(NM):
                for t in range(NT):
                    getattr(store(f, m, t, c), op)()

    zero = jnp.zeros(VR, F32)
    for m in range(NM):
        for t in range(NT):
            cols = pl.ds(t * NL, NL)
            eta_out[m, :, cols] = bo[m, 0, t]
            tx_out[m, :, cols] = bo[m, 1, t]
            ty_out[m, :, cols] = bo[m, 2, t]
            for f in range(2):
                for j in range(NJ):
                    here = pl.ds(j, NS, stride=NJ)
                    i = j * NT + t
                    cor[f, m, i] = bo.at[m, 1 + f, t][here, :] * rl.at[2 + f, t][here, :] - bsum[f, m, i] * rl.at[f, t][here, :]

    def back(fs):
        def chunk(c2, xs):
            c = NC - 1 - c2

            def step(q, xs):
                xs = list(xs)
                for h in range(2):
                    k = c * CH + CH - 1 - 2 * q - h
                    n = 0
                    for f in fs:
                        g = tab[f // 2 * 2, k]
                        for j in range(NJ):
                            for t in range(NT):
                                here = pl.ds(j, NS, stride=NJ)
                                i = j * NT + t
                                if f < 2:
                                    wet = kl[1 + f, i] > k
                                for m in range(NM):
                                    x = parts[f][0][parts[f][1], m, k + 1, i] + g * xs[n]
                                    xs[n] = x
                                    n += 1
                                    xbuf.at[f, m, t, k][here, :] = jnp.where(wet, x + cor[f, m, i], 0.0) if f < 2 else x
                return tuple(xs)

            xs = lax.fori_loop(0, CH // 2, step, xs)
            each_store(fs, c, "start")
            return xs

        lax.fori_loop(0, NC, chunk, (zero,) * (len(fs) * NM * NJ * NT))

    back((2,))
    back((0, 1))
    for m in range(NM):
        for i in range(NJ * NT):
            s_salt[0, m, 0, i] = zero
    tracer_pass(inb, lambda m: (inb, (2, m)), ends_s, uw_all, hN.at[3], hS.at[3], hS.at[1], kl, tab, s_salt, 0, BACK_UNROLL)
    back((3,))

    def drain(c, _):
        each_store(range(NF), c, "wait")
        return 0

    lax.fori_loop(0, NC, drain, 0)


def final_call(kept, tab):
    flat = jax.ShapeDtypeStruct((NM, NY, NX), F32)
    block = jax.ShapeDtypeStruct((NK, NM, NY, NX), F32)
    held = [pltpu.with_memory_space_constraint(x, pltpu.VMEM) for x in kept]
    return pl.pallas_call(
        final_kernel,
        out_shape=(flat,) * 3 + (block,) * 4,
        in_specs=[VM] * len(held) + [SM],
        out_specs=(VM,) * 3 + (HBM,) * 4,
        scratch_shapes=[
            pltpu.VMEM((4, NM, NT, NK, NY, NL), F32),
            pltpu.VMEM((1, NM, NK + 1, NJ * NT, *VR), F32),
            pltpu.VMEM((2, NM, NJ * NT, *VR), F32),
            pltpu.SemaphoreType.DMA((4, NM, NT, NC)),
        ],
        compiler_params=pltpu.CompilerParams(vmem_limit_bytes=VMEM_LIMIT),
        name="back_substitution",
    )(*held, tab)


def solution(mesh):
    def local_step(*args):
        tab = level_table()
        return final_call(step_call(*args, tab), tab)

    spec_3d = P(None, None, "row", "col")
    spec_2d = P(None, "row", "col")
    spec_map = P("row", "col")
    return jax.shard_map(local_step, mesh=mesh, in_specs=(spec_3d,) * 4 + (spec_2d,) * 3 + (spec_map,) * 2 + (P(),), out_specs=(spec_2d,) * 3 + (spec_3d,) * 4, check_vma=False)
```

```python
import functools
import jax
import jax.numpy as jnp
import numpy as np
from jax import lax
from jax.experimental import pallas as pl
from jax.experimental.pallas import tpu as pltpu
from jax.sharding import PartitionSpec as P

MESH = pl.DeviceIdType.MESH
F32 = jnp.float32
NK = 60
NM = 2
NY = 32
NL = 128
NS = 8
VR = (NS, NL)
NF = 4
NX = 256
NT = NX // NL
NJ = NY // 8
CH = 10
HALF = CH
GROUP = 5
NC = NK // CH
HALO = 40
WY = 2 * NY + HALO
WJ = WY // 8
WT = 3
NSUB = 40
COURANT = 0.4
VMEM_LIMIT = 28 << 20
STEP_LIMIT = 28 << 20
SIDE = 40

VM = pl.BlockSpec(memory_space=pltpu.VMEM)
SM = pl.BlockSpec(memory_space=pltpu.SMEM)
HBM = pl.BlockSpec(memory_space=pl.ANY)


def level_table():
    rows = np.zeros((4, NK), np.float64)
    for row, strength in ((0, 1.0), (2, 0.5)):
        scale = 1.0 if strength == 1.0 else 0.5
        div_prev = 0.0
        for k in range(NK):
            if k == 0:
                div = 1.0 + strength
            else:
                div = 1.0 + 2.0 * strength - strength * strength / div_prev
            rows[row, k] = scale / div
            rows[row + 1, k] = scale / (div - strength)
            div_prev = div
    return jnp.asarray(rows, F32)


def lanes_iota():
    return lax.broadcasted_iota(jnp.int32, VR, 1)


def subl_iota():
    return lax.broadcasted_iota(jnp.int32, VR, 0)


def device(col, row):
    return {"col": col, "row": row}


def greet(col, row):
    barrier = pltpu.get_barrier_semaphore()
    count = 0
    for dc in (0, 1, 3):
        for dr in range(NF):
            if dc == 0 and dr == 0:
                continue
            pl.semaphore_signal(barrier, inc=1, device_id=device(lax.rem(col + dc, 4), lax.rem(row + dr, 4)), device_id_type=MESH)
            count += 1
    return lambda: pl.semaphore_wait(barrier, count)


class Exchange:
    def __init__(self, src_main, src_side, main, side, send_sem, recv_sem, col, row):
        chip = row // 2
        core = lax.rem(row, 2)
        east = lax.rem(col + 1, 4)
        west = lax.rem(col + 3, 4)
        self.full = chip != core
        self.main, self.side, self.recv_sem = main, side, recv_sem
        own = pl.ds(pl.multiple_of(core * NY, NS), NY)
        at_full = pl.ds(pl.multiple_of(jnp.where(chip == 1, 2 * NY, NY + HALO), NS), NY)
        at_part = pl.ds(pl.multiple_of(jnp.where(chip == 1, 3 * NY, 2 * NY), NS), NS)
        from_part = pl.ds(pl.multiple_of(jnp.where(chip == 1, 0, NY - NS), NS), NS)
        self.count = 0

        def remote(s, d, kind, dev):
            return pltpu.make_async_remote_copy(src_ref=s, dst_ref=d, send_sem=send_sem.at[self.count], recv_sem=recv_sem.at[kind], device_id=dev, device_id_type=MESH)

        self.always, self.whole, self.part = [], [], []
        self.local = pltpu.make_async_copy(src_main.at[core], main.at[:, :, own], recv_sem.at[0])
        self.always.append(remote(src_main.at[1 - core], main.at[:, :, own], 0, device(col, chip * 2 + 1 - core)))
        for mm in range(NM):
            near, far = chip * 2 + mm, (1 - chip) * 2 + mm
            self.count += 1
            self.whole.append(remote(src_main.at[mm], main.at[:, :, at_full], 0, device(col, far)))
            self.part.append(remote(src_main.at[mm, :, :, from_part], main.at[:, :, at_part], 0, device(col, far)))
            for e, dev in enumerate((west, east)):
                self.count += 1
                self.whole.append(remote(src_side.at[mm, e], side.at[e, :, at_full], 1, device(dev, far)))
                self.part.append(remote(src_side.at[mm, e, :, from_part], side.at[e, :, at_part], 1, device(dev, far)))
                self.count += 1
                self.always.append(remote(src_side.at[mm, e], side.at[e, :, own], 1, device(dev, near)))

    def branch(self, op):
        @pl.when(self.full)
        def _():
            for copy in self.whole:
                getattr(copy, op)()

        @pl.when(jnp.logical_not(self.full))
        def _():
            for copy in self.part:
                getattr(copy, op)()

    def start(self):
        self.branch("start")
        for copy in self.always:
            copy.start()
        self.local.start()

    def wait(self):
        pltpu.make_async_copy(self.main, self.main, self.recv_sem.at[0]).wait()
        pltpu.make_async_copy(self.side, self.side, self.recv_sem.at[1]).wait()
        for copy in self.always:
            copy.wait_send()
        self.branch("wait_send")


def pack_side(dst, m, group, fields, lane):
    for i in range(NY // NS):
        rows = pl.ds(i * NS, NS)
        first = fields[0](0, rows)
        last = fields[0](NT - 1, rows)
        for n in range(1, len(fields)):
            first = jnp.where(lane < n * SIDE, first, pltpu.roll(fields[n](0, rows), n * SIDE, 1))
            last = jnp.where(lane >= NL - n * SIDE, last, pltpu.roll(fields[n](NT - 1, rows), NL - n * SIDE, 1))
        dst[m, 0, group, rows] = first
        dst[m, 1, group, rows] = last


def window_tile(main, side, f, j, t, lane, group, place):
    here = pl.ds(j, NS, stride=WJ)
    if t < NT:
        return main.at[f, t][here, :]
    e, w = side.at[0, group][here, :], side.at[1, group][here, :]
    if place:
        e, w = pltpu.roll(e, NL - place * SIDE, 1), pltpu.roll(w, place * SIDE, 1)
    return jnp.where(lane < SIDE, e, jnp.where(lane >= NL - SIDE, w, 0.0))


PA = 0.15 * 0.5 / NK * 0.5
PB = 0.2 * 0.5 / NK * 0.5
MOM_UNROLL = 3
TRC_UNROLL = 3
BACK_UNROLL = 10
SUB_UNROLL = 5


def rolls(x, amount):
    return [[pltpu.roll(x[j][t], amount, 1) for t in range(NT)] for j in range(NJ)]


def east(x, halo):
    edge, r = lanes_iota() == NL - 1, rolls(x, NL - 1)
    return [[jnp.where(edge, r[j][1] if t == 0 else halo[j], r[j][t]) for t in range(NT)] for j in range(NJ)]


def west(x, halo):
    edge, r = lanes_iota() == 0, rolls(x, 1)
    return [[jnp.where(edge, r[j][0] if t == 1 else halo[j], r[j][t]) for t in range(NT)] for j in range(NJ)]


def north(x, halo):
    edge = subl_iota() == NS - 1
    return x[1:] + [[jnp.where(edge, halo[t], pltpu.roll(x[0][t], NS - 1, 0)) for t in range(NT)]]


def south(x, halo):
    edge = subl_iota() == 0
    return [[jnp.where(edge, halo[t], pltpu.roll(x[NJ - 1][t], 1, 0)) for t in range(NT)]] + x[:-1]


def zipped(fn, *xs):
    return [[fn(*[x[j][t] for x in xs]) for t in range(NT)] for j in range(NJ)]


def strided(ref):
    return [ref[pl.ds(j, NS, stride=NJ), :] for j in range(NJ)]


def read_mask(kl, n):
    return [[kl[n, j * NT + t] for t in range(NT)] for j in range(NJ)]


def factors(mask, k, a, b):
    return zipped(lambda n: jnp.where(n > k + 1, a, jnp.where(n == k + 1, b, 0.0)), mask)


def read_block(ref, index, k):
    return [[ref.at[(*index, t, k)][pl.ds(j, NS, stride=NJ), :] for t in range(NT)] for j in range(NJ)]


def line(ref, m, k):
    return [ref.at[t][pl.ds(m * NK + k, NS, stride=0), :] for t in range(NT)]


def solve(sbuf, f, m, k, side, scale):
    for j in range(NJ):
        for t in range(NT):
            i = j * NT + t
            sbuf[f, m, k + 1, i] = (side[j][t] + sbuf[f, m, k, i]) * scale[j][t]


def tracer_pass(inb, field, ends, uw_all, north_rows, south_rows, south_v, kl, tab, sbuf, f, unroll):
    def level(m, k, inv_c):
        uu, vv, sv = read_block(inb, (0, m), k), read_block(inb, (1, m), k), line(south_v, m, k)
        u_w = [[uw_all[m, k, j * NT + t] for t in range(NT)] for j in range(NJ)]
        x = read_block(*field(m), k)
        halo = [ends[m, k, j] for j in range(NJ)]
        x_e, x_w = east(x, halo), west(x, halo)
        x_n = north(x, line(north_rows, m, k))
        x_s = line(south_rows, m, k)
        fx = zipped(lambda u, a, b: u * (a + b), uu, x, x_e)
        fx_w = zipped(lambda u, a, b: u * (a + b), u_w, x, x_w)
        fy = zipped(lambda v, a, b: v * (a + b), vv, x, x_n)
        fy_s = south(fy, [sv[t] * (x_s[t] + x[0][t]) for t in range(NT)])
        solve(sbuf, f, m, k, zipped(lambda a, b, bw, g, gs: (a + a) - (b - bw) - (g - gs), x, fx, fx_w, fy, fy_s), inv_c)

    def levels(q, carry):
        for h in range(unroll):
            k = q * unroll + h
            inv_c = factors(read_mask(kl, 0), k, tab[2, k], tab[3, k])
            for m in range(NM):
                level(m, k, inv_c)
        return carry

    lax.fori_loop(0, NK // unroll, levels, 0)


def step_kernel(u, v, temp, salt, eta, tx, ty, depth, wet, weights, tab,
                sbuf, bsum, kl, rl, out, inb, ends_s, uw_all, hN, hS,
                inb_t, ew, ends_t, corner, sv_east, nu_west, hE, hW, hSE, hNW, colF, colL, rowF, rowL, ksrc, kE, kN,
                wmain, wside, main, side, gsum, fmain, fside, fwin, fwside, wi, nat, state, res,
                in_sem, sendC, recvE, recvW, sendR, recvN, recvS, corn_send, corn_recv, k_send, k_recv,
                w_send, w_recv, f_send, f_recv, out_send, out_recv, loc_sem):
    col = lax.axis_index("col")
    row = lax.axis_index("row")
    chip = row // 2
    core = lax.rem(row, 2)
    east_dev = lax.rem(col + 1, 4)
    west_dev = lax.rem(col + 3, 4)
    north_dev = jnp.minimum(row + 1, 3)
    south_dev = jnp.maximum(row - 1, 0)
    has_north = row < 3
    has_south = row > 0
    fields = (u, v, temp, salt)
    lane = lanes_iota()
    subl = subl_iota()
    l_last, l_first = lane == NL - 1, lane == 0
    s_last, s_first = subl == NS - 1, subl == 0
    zero = jnp.zeros(VR, F32)

    def place(f, *index):
        return inb_t.at[index] if f == 2 else inb.at[(min(f, 2), *index)]

    def held(f, *index):
        return inb_t[index] if f == 2 else inb[(min(f, 2), *index)]

    def load(f, m, t, c):
        part = pl.ds(c * CH, CH)
        return pltpu.make_async_copy(fields[f].at[part, m, :, pl.ds(t * NL, NL)], place(f, m, t, part), in_sem.at[f, m, t, c])

    def each_load(f, c, op):
        for m in range(NM):
            for t in range(NT):
                getattr(load(f, m, t, c), op)()

    for f in range(NF):
        for c in range(NC):
            each_load(f, c, "start")

    for t in range(NT):
        ksrc[t] = wet[:, pl.ds(t * NL, NL)].astype(F32)

    meet = greet(col, row)

    def remote(s, d, ssem, rsem, dc, dr):
        return pltpu.make_async_remote_copy(src_ref=s, dst_ref=d, send_sem=ssem, recv_sem=rsem, device_id=device(dc, dr), device_id_type=MESH)

    k_west = remote(ksrc.at[0], kE, k_send.at[0], k_recv.at[0], west_dev, row)
    k_south = remote(ksrc.at[:, pl.ds(0, NS)], kN, k_send.at[1], k_recv.at[1], col, south_dev)

    def col_copies(f):
        return (remote(colF.at[f], hE.at[f], sendC.at[0, f], recvE.at[f], west_dev, row),
                remote(colL.at[f], hW.at[f], sendC.at[1, f], recvW.at[f], east_dev, row))

    def to_south(f):
        return remote(rowF.at[f], hN.at[f], sendR.at[0, f], recvN.at[f], col, south_dev)

    def to_north(f):
        return remote(rowL.at[f], hS.at[f], sendR.at[1, f], recvS.at[f], col, north_dev)

    corner_north = remote(colF.at[1, pl.ds(NY - NS, NS)], hSE, corn_send.at[0], corn_recv.at[0], west_dev, north_dev)
    corner_south = remote(colL.at[0, pl.ds(0, NS)], hNW, corn_send.at[1], corn_recv.at[1], east_dev, south_dev)

    lane_next = lax.rem(lane + 1, NL)
    for f in range(NF):
        def chunk(c, acc, f=f):
            each_load(f, c, "wait")
            return piece(c * CH, acc)

        def piece(k0, acc, f=f):
            acc = list(acc)
            for q in range(HALF):
                k = k0 + q
                for m in range(NM):
                    spot = 2 * k + m
                    hit, hit_last = lane == spot, lane_next == spot
                    for i in range(NJ):
                        rows = pl.ds(i * NS, NS)
                        both = pltpu.roll(jnp.where(l_first, held(f, m, 0, k, rows), held(f, m, NT - 1, k, rows)), spot, 1)
                        acc[2 * i] = jnp.where(hit, both, acc[2 * i])
                        acc[2 * i + 1] = jnp.where(hit_last, both, acc[2 * i + 1])
                    for t in range(NT):
                        rowF[f, t, pl.ds(m * NK + k, 1), :] = held(f, m, t, k, pl.ds(0, 1))
                        rowL[f, t, pl.ds(m * NK + k, 1), :] = held(f, m, t, k, pl.ds(NY - 1, 1))
            return tuple(acc)

        acc = lax.fori_loop(0, NC, chunk, (zero,) * (2 * NJ))
        for i in range(NJ):
            colF[f, pl.ds(i * NS, NS)] = acc[2 * i]
            colL[f, pl.ds(i * NS, NS)] = acc[2 * i + 1]
        if f == 0:
            meet()
            k_west.start()

            @pl.when(has_south)
            def _():
                k_south.start()

        @pl.when(has_south)
        def _():
            to_south(f).start()

        @pl.when(has_north)
        def _():
            to_north(f).start()
        for copy in col_copies(f):
            copy.start()
        if f == 0:
            @pl.when(has_south)
            def _():
                corner_south.start()
        if f == 1:
            @pl.when(has_north)
            def _():
                corner_north.start()

    for m in range(NM):
        for t in range(NT):
            cols = pl.ds(t * NL, NL)
            for i, arr in enumerate((eta, tx, ty)):
                wmain[m, i, t] = arr[m, :, cols]
            wmain[m, 3, t] = depth[:, cols]
            wmain[m, 4, t] = ksrc[t]
        reads = [lambda t, rows, m=m, i=i: wmain[m, i, t, rows] for i in range(5)]
        pack_side(wside, m, 0, reads[:3], lane)
        pack_side(wside, m, 1, reads[3:], lane)
    windows = Exchange(wmain, wside, main, side, w_send, w_recv, col, row)

    @pl.when(jnp.logical_not(has_north))
    def _():
        hN[...] = jnp.zeros(hN.shape, F32)
        hNW[...] = jnp.zeros(hNW.shape, F32)
        kN[...] = jnp.zeros(kN.shape, F32)

    @pl.when(jnp.logical_not(has_south))
    def _():
        hS[...] = jnp.zeros(hS.shape, F32)
        hSE[...] = jnp.zeros(hSE.shape, F32)

    for f in range(3):
        for m in range(NM):
            for i in range(NJ * NT):
                sbuf[f, m, 0, i] = zero
    for f in range(2):
        for m in range(NM):
            for i in range(NJ * NT):
                gsum[f, m, i] = zero
                bsum[f, m, i] = zero

    k_west.wait()

    @pl.when(has_south)
    def _():
        k_south.wait_send()
        corner_south.wait_send()
        corner_north.wait_recv()

    @pl.when(has_north)
    def _():
        k_south.wait_recv()
        corner_north.wait_send()
        corner_south.wait_recv()

    for f in range(NF):
        for copy in col_copies(f):
            copy.wait()

        @pl.when(has_south)
        def _():
            to_south(f).wait_send()
            to_north(f).wait_recv()

        @pl.when(has_north)
        def _():
            to_north(f).wait_send()
            to_south(f).wait_recv()

    odd = lax.rem(lane, 2)
    for m in range(NM):
        for f in range(NF):
            for i in range(NJ):
                rows = pl.ds(i * NS, NS)
                ew[f, m, rows] = jnp.where(odd == m, hE[f, rows], pltpu.roll(hW[f, rows], 2, 1))
        corner[m] = jnp.where(odd == m, hSE[pl.ds(NS - 1, NS, stride=0), :], pltpu.roll(hNW[pl.ds(0, NS, stride=0), :], 2, 1))
    for i in range(NM * NK // NS):
        rows = pl.ds(i * NS, NS)
        r = [pltpu.roll(hS[1, t, rows], NL - 1, 1) for t in range(NT)]
        sv_east[0, rows] = jnp.where(l_last, r[1], r[0])
        sv_east[1, rows] = r[1]
        r = [pltpu.roll(hN[0, t, rows], 1, 1) for t in range(NT)]
        nu_west[0, rows] = r[0]
        nu_west[1, rows] = jnp.where(l_first, r[0], r[1])

    k_mid = zipped(lambda x: x, [list(pair) for pair in zip(*[strided(ksrc.at[t]) for t in range(NT)])])
    k_east = zipped(jnp.minimum, k_mid, east(k_mid, [pltpu.roll(x, NL - 1, 1) for x in strided(kE)]))
    k_north = zipped(jnp.minimum, k_mid, north(k_mid, [kN.at[t][pl.ds(0, NS, stride=0), :] for t in range(NT)]))
    for n, mask in enumerate((k_mid, k_east, k_north)):
        for j in range(NJ):
            for t in range(NT):
                kl[n, j * NT + t] = mask[j][t].astype(jnp.int32)

    def block(f, m, k):
        return [[place(f, m, t, k)[pl.ds(j, NS, stride=NJ), :] for t in range(NT)] for j in range(NJ)]

    def momentum(m, k, carry, wet_x, wet_y, inv_x, inv_y):
        cs, cs_n, cs_e = carry
        uu, vv, tt, ss = (block(f, m, k) for f in range(NF))
        amount = NL - 1 - m - 2 * k
        eu, ev, et, es = ([pltpu.roll(x, amount, 1) for x in strided(ew.at[f, m])] for f in range(NF))
        c = pltpu.roll(corner[m], amount, 1)
        for j in range(NJ):
            ends_t[m, k, j] = et[j]
            ends_s[m, k, j] = es[j]
        nu, nv, nt, ns = (line(hN.at[f], m, k) for f in range(NF))
        su, sv = (line(hS.at[f], m, k) for f in range(2))

        half = zipped(lambda s, t: PA * s - PB * t, ss, tt)
        p = zipped(jnp.add, cs, half)
        cs = zipped(jnp.add, p, half)
        half_n = [PA * ns[t] - PB * nt[t] for t in range(NT)]
        p_n = [cs_n[t] + half_n[t] for t in range(NT)]
        cs_n = [p_n[t] + half_n[t] for t in range(NT)]
        half_e = [PA * es[j] - PB * et[j] for j in range(NJ)]
        p_e = [cs_e[j] + half_e[j] for j in range(NJ)]
        cs_e = [p_e[j] + half_e[j] for j in range(NJ)]

        u_e, u_w, v_e, v_w = east(uu, eu), west(uu, eu), east(vv, ev), west(vv, ev)
        for j in range(NJ):
            for t in range(NT):
                uw_all[m, k, j * NT + t] = u_w[j][t]
        u_n, u_s, v_n, v_s = north(uu, nu), south(uu, su), north(vv, nv), south(vv, sv)
        sve, nuw = line(sv_east, m, k), line(nu_west, m, k)
        sve[1] = jnp.where(l_last, c, sve[1])
        nuw[0] = jnp.where(l_first, c, nuw[0])
        a = zipped(jnp.add, vv, v_e)
        v_sum = zipped(jnp.add, a, south(a, [sv[t] + sve[t] for t in range(NT)]))
        b = zipped(jnp.add, uu, u_w)
        u_sum = zipped(jnp.add, b, north(b, [nu[t] + nuw[t] for t in range(NT)]))
        p_e = east(p, p_e)
        p_n = north(p, p_n)

        gu = zipped(lambda w, p, pe, u, ue, uw, vs, un, us: jnp.where(w, (p - pe) - 0.5 * (u * (ue - uw)) - 0.125 * (vs * (un - us)), 0.0),
                    wet_x, p, p_e, uu, u_e, u_w, v_sum, u_n, u_s)
        gv = zipped(lambda w, p, pn, us, ve, vw, v, vn, vs: jnp.where(w, (p - pn) - 0.125 * (us * (ve - vw)) - 0.5 * (v * (vn - vs)), 0.0),
                    wet_y, p, p_n, u_sum, v_e, v_w, vv, v_n, v_s)
        bu = zipped(jnp.add, uu, gu)
        bv = zipped(jnp.add, vv, gv)
        solve(sbuf, 0, m, k, bu, inv_x)
        solve(sbuf, 1, m, k, bv, inv_y)
        for f, (g, b) in enumerate(((gu, bu), (gv, bv))):
            for j in range(NJ):
                for t in range(NT):
                    i = j * NT + t
                    gsum[f, m, i] = gsum[f, m, i] + g[j][t]
                    bsum[f, m, i] = bsum[f, m, i] + b[j][t]
        return cs, cs_n, cs_e

    def momentum_levels(q, carry):
        for h in range(MOM_UNROLL):
            k = q * MOM_UNROLL + h
            mask_x, mask_y = read_mask(kl, 1), read_mask(kl, 2)
            a1, b1 = tab[0, k], tab[1, k]
            inv = factors(mask_x, k, a1, b1), factors(mask_y, k, a1, b1)
            wet_k = [zipped(lambda n: n > k, mask) for mask in (mask_x, mask_y)]
            carry = tuple(momentum(m, k, carry[m], *wet_k, *inv) for m in range(NM))
        return carry

    start = ([[zero] * NT for _ in range(NJ)], [zero] * NT, [zero] * NJ)
    windows.start()
    lax.fori_loop(0, NK // MOM_UNROLL, momentum_levels, (start, start))

    for f in range(2):
        for m in range(NM):
            for t in range(NT):
                for j in range(NJ):
                    fmain.at[m, f, t][pl.ds(j, NS, stride=NJ), :] = gsum[f, m, j * NT + t]
    for m in range(NM):
        pack_side(fside, m, 0, [lambda t, rows, m=m, f=f: fmain[m, f, t, rows] for f in range(2)], lane)
    forces = Exchange(fmain, fside, fwin, fwside, f_send, f_recv, col, row)
    forces.start()

    tracer_pass(inb, lambda m: (inb_t, (m,)), ends_t, uw_all, hN.at[2], hS.at[2], hS.at[1], kl, tab, sbuf, 2, TRC_UNROLL)

    windows.wait()
    dep = [[window_tile(main, side, 3, j, t, lane, 1, 0) for t in range(WT)] for j in range(WJ)]
    lev = [[window_tile(main, side, 4, j, t, lane, 1, 1) for t in range(WT)] for j in range(WJ)]
    for j in range(WJ):
        row_here = WJ * subl + j
        wall = jnp.logical_and(row_here == 2 * NY - 1, chip == 1)
        dr = [pltpu.roll(dep[j][t], NL - 1, 1) for t in range(WT)]
        lr = [pltpu.roll(lev[j][t], NL - 1, 1) for t in range(WT)]
        for t in range(WT):
            d, k = dep[j][t], lev[j][t]
            de = jnp.where(l_last, dr[(t + 1) % WT], dr[t])
            ke = jnp.where(l_last, lr[(t + 1) % WT], lr[t])
            if j < WJ - 1:
                dn, kn = dep[j + 1][t], lev[j + 1][t]
            else:
                dn, kn = pltpu.roll(dep[0][t], NS - 1, 0), pltpu.roll(lev[0][t], NS - 1, 0)
            kx = jnp.minimum(k, ke)
            ky = jnp.where(wall, 0.0, jnp.minimum(k, kn))
            hx = jnp.where(kx > 0.0, 0.5 * (d + de), 0.0)
            hy = jnp.where(ky > 0.0, 0.5 * (d + dn), 0.0)
            ix = 1.0 / jnp.maximum(kx, 1.0)
            iy = 1.0 / jnp.maximum(ky, 1.0)
            state[0, j, t] = window_tile(main, side, 0, j, t, lane, 0, 0)
            for i in (1, 2):
                first = COURANT * window_tile(main, side, i, j, t, lane, 0, i)
                state[i, j, t] = first
                wi[1 + i, j, t] = first
            wi[0, j, t] = (COURANT * COURANT) * hx
            wi[1, j, t] = (COURANT * COURANT) * hy
            state[3, j, t] = (COURANT / NSUB) * hx * ix
            state[4, j, t] = (COURANT / NSUB) * hy * iy
            state[5, j, t] = zero
            state[6, j, t] = zero
            if t < NT:
                here = pl.ds(j, NS, stride=WJ)
                nat.at[0, t][here, :] = ix
                nat.at[1, t][here, :] = iy
                nat.at[2, t][here, :] = 1.0 / jnp.where(kx > 0.0, hx, 1.0)
                nat.at[3, t][here, :] = 1.0 / jnp.where(ky > 0.0, hy, 1.0)
    own = pl.ds(pl.multiple_of(core * NY, NS), NY)
    for t in range(NT):
        for i in range(NF):
            rl[i, t] = nat[i, t, own]

    def tail(i, carry):
        s1, s2, n = carry
        w = weights[NSUB - 1 - i]
        return s1 + w, s2 + n * w, n - 1.0

    total, moment, _ = lax.fori_loop(0, NSUB, tail, (0.0, 0.0, float(NSUB)))
    edge_wall = jnp.where(jnp.logical_and(s_first, chip == 0), 0.0, 1.0)
    forces.wait()
    for j in range(WJ):
        for t in range(WT):
            for f in range(2):
                state[3 + f, j, t] = state[3 + f, j, t] * window_tile(fwin, fwside, f, j, t, lane, 0, f)

    lane3 = lax.broadcasted_iota(jnp.int32, (WT, *VR), 2)
    wall3 = jnp.broadcast_to(edge_wall, (WT, *VR))

    def subcycle(i, remain):
        w = weights[i]
        for j in range(WJ):
            u, v = state[1, j], state[2, j]
            r = pltpu.roll(u, 1, 2)
            uw = jnp.where(lane3 == 0, jnp.concatenate([r[WT - 1:], r[:WT - 1]], axis=0), r)
            vs = state[2, j - 1] if j else pltpu.roll(state[2, WJ - 1], 1, 1) * wall3
            e = state[0, j] - ((u - uw) + (v - vs))
            state[0, j] = e
            state[5, j] = state[5, j] + w * e
            state[6, j] = state[6, j] + remain * e
        for j in range(WJ):
            e = state[0, j]
            r = pltpu.roll(e, NL - 1, 2)
            ee = jnp.where(lane3 == NL - 1, jnp.concatenate([r[1:], r[:1]], axis=0), r)
            en = state[0, j + 1] if j < WJ - 1 else pltpu.roll(state[0, 0], NS - 1, 1)
            state[1, j] = (state[1, j] + state[3, j]) - wi[0, j] * (ee - e)
            state[2, j] = (state[2, j] + state[4, j]) - wi[1, j] * (en - e)
        return remain - w

    lax.fori_loop(0, NSUB, subcycle, total, unroll=SUB_UNROLL)

    scale = 1.0 / COURANT
    for j in range(WJ):
        q = [state[6, j, t] for t in range(WT)]
        r = [pltpu.roll(q[t], NL - 1, 1) for t in range(WT)]
        for t in range(NT):
            qe = jnp.where(l_last, r[t + 1], r[t])
            qn = pltpu.roll(state[6, 0, t], NS - 1, 0) if j == WJ - 1 else state[6, j + 1, t]
            here = pl.ds(j, NS, stride=WJ)
            res.at[0, t][here, :] = state[5, j, t]
            res.at[1, t][here, :] = scale * (total * wi[2, j, t] + moment * state[3, j, t] - wi[0, j, t] * (qe - q[t]))
            res.at[2, t][here, :] = scale * (total * wi[3, j, t] + moment * state[4, j, t] - wi[1, j, t] * (qn - q[t]))
    other = 1 - core
    send = remote(res.at[:, :, pl.ds(pl.multiple_of(other * NY, NS), NY)], out.at[core], out_send, out_recv, col, chip * 2 + other)
    send.start()
    keep = pltpu.make_async_copy(res.at[:, :, pl.ds(pl.multiple_of(core * NY, NS), NY)], out.at[core], loc_sem)
    keep.start()
    keep.wait()
    send.wait()


def step_call(vel_x, vel_y, pot_temp, salinity, surf_eta, trans_x, trans_y, col_depth, wet_levels, weights, tab):
    dma = pltpu.SemaphoreType.DMA
    pair = dma((NM,))
    nreg = NJ * NT

    def vm(*shape):
        return pltpu.VMEM(shape, F32)

    return pl.pallas_call(
        step_kernel,
        out_shape=(
            vm(3, NM, NK + 1, nreg, *VR),
            vm(2, NM, nreg, *VR),
            pltpu.VMEM((3, nreg, *VR), jnp.int32),
            vm(4, NT, NY, NL),
            vm(NM, 3, NT, NY, NL),
            vm(3, NM, NT, NK, NY, NL), vm(NM, NK, NJ, *VR), vm(NM, NK, nreg, *VR), vm(4, NT, NM * NK, NL), vm(4, NT, NM * NK, NL),
        ),
        in_specs=[HBM] * 4 + [VM] * 5 + [SM] * 2,
        out_specs=(VM,) * 10,
        scratch_shapes=[
            vm(NM, NT, NK, NY, NL),
            vm(4, NM, NY, NL), vm(NM, NK, NJ, *VR), vm(NM, *VR), vm(NT, NM * NK, NL), vm(NT, NM * NK, NL),
            vm(NF, NY, NL), vm(NF, NY, NL), vm(*VR), vm(*VR),
            vm(NF, NY, NL), vm(NF, NY, NL), vm(NF, NT, NM * NK, NL), vm(NF, NT, NM * NK, NL),
            vm(NT, NY, NL), vm(NY, NL), vm(NT, *VR),
            vm(NM, 5, NT, NY, NL), vm(NM, 2, 2, NY, NL), vm(5, NT, WY, NL), vm(2, 2, WY, NL),
            vm(2, NM, nreg, *VR),
            vm(NM, 2, NT, NY, NL), vm(NM, 2, 1, NY, NL), vm(2, NT, WY, NL), vm(2, 1, WY, NL),
            vm(4, WJ, WT, *VR), vm(4, NT, WY, NL), vm(7, WJ, WT, *VR), vm(3, NT, WY, NL),
            dma((NF, NM, NT, NC)), dma((NM, NF)), dma((NF,)), dma((NF,)), dma((NM, NF)), dma((NF,)), dma((NF,)), pair, pair, pair, pair,
            dma((NS + NS,)), pair, dma((NS + NS,)), pair, dma, dma, dma,
        ],
        compiler_params=pltpu.CompilerParams(collective_id=0, has_side_effects=True, vmem_limit_bytes=STEP_LIMIT),
        name="ocean_step",
    )(vel_x, vel_y, pot_temp, salinity, surf_eta, trans_x, trans_y, col_depth, wet_levels, weights, tab)


def final_kernel(sbuf, bsum, kl, rl, bo, inb, ends_s, uw_all, hN, hS, tab, eta_out, tx_out, ty_out, u_out, v_out, temp_out, salt_out, xbuf, s_salt, cor, out_sem):
    outs = (u_out, v_out, temp_out, salt_out)
    parts = ((sbuf, 0), (sbuf, 1), (sbuf, 2), (s_salt, 0))

    def store(f, m, t, c):
        part = pl.ds(c * CH, CH)
        return pltpu.make_async_copy(xbuf.at[f, m, t, part], outs[f].at[part, m, :, pl.ds(t * NL, NL)], out_sem.at[f, m, t, c])

    def each_store(fs, c, op):
        for f in fs:
            for m in range(NM):
                for t in range(NT):
                    getattr(store(f, m, t, c), op)()

    zero = jnp.zeros(VR, F32)
    for m in range(NM):
        for t in range(NT):
            cols = pl.ds(t * NL, NL)
            eta_out[m, :, cols] = bo[m, 0, t]
            tx_out[m, :, cols] = bo[m, 1, t]
            ty_out[m, :, cols] = bo[m, 2, t]
            for f in range(2):
                for j in range(NJ):
                    here = pl.ds(j, NS, stride=NJ)
                    i = j * NT + t
                    cor[f, m, i] = bo.at[m, 1 + f, t][here, :] * rl.at[2 + f, t][here, :] - bsum[f, m, i] * rl.at[f, t][here, :]

    def back(fs):
        def chunk(c2, xs):
            c = NC - 1 - c2

            def step(q, xs):
                xs = list(xs)
                for h in range(GROUP):
                    k = c * CH + CH - 1 - GROUP * q - h
                    n = 0
                    for f in fs:
                        g = tab[f // 2 * 2, k]
                        for j in range(NJ):
                            for t in range(NT):
                                here = pl.ds(j, NS, stride=NJ)
                                i = j * NT + t
                                if f < 2:
                                    wet = kl[1 + f, i] > k
                                for m in range(NM):
                                    x = parts[f][0][parts[f][1], m, k + 1, i] + g * xs[n]
                                    xs[n] = x
                                    n += 1
                                    xbuf.at[f, m, t, k][here, :] = jnp.where(wet, x + cor[f, m, i], 0.0) if f < 2 else x
                return tuple(xs)

            xs = lax.fori_loop(0, CH // GROUP, step, xs)
            each_store(fs, c, "start")
            return xs

        lax.fori_loop(0, NC, chunk, (zero,) * (len(fs) * NM * NJ * NT))

    back((2,))
    back((0, 1))
    for m in range(NM):
        for i in range(NJ * NT):
            s_salt[0, m, 0, i] = zero
    tracer_pass(inb, lambda m: (inb, (2, m)), ends_s, uw_all, hN.at[3], hS.at[3], hS.at[1], kl, tab, s_salt, 0, BACK_UNROLL)
    back((3,))

    def drain(c, _):
        each_store(range(NF), c, "wait")
        return 0

    lax.fori_loop(0, NC, drain, 0)


def final_call(kept, tab):
    flat = jax.ShapeDtypeStruct((NM, NY, NX), F32)
    block = jax.ShapeDtypeStruct((NK, NM, NY, NX), F32)
    held = [pltpu.with_memory_space_constraint(x, pltpu.VMEM) for x in kept]
    return pl.pallas_call(
        final_kernel,
        out_shape=(flat,) * 3 + (block,) * 4,
        in_specs=[VM] * len(held) + [SM],
        out_specs=(VM,) * 3 + (HBM,) * 4,
        scratch_shapes=[
            pltpu.VMEM((4, NM, NT, NK, NY, NL), F32),
            pltpu.VMEM((1, NM, NK + 1, NJ * NT, *VR), F32),
            pltpu.VMEM((2, NM, NJ * NT, *VR), F32),
            pltpu.SemaphoreType.DMA((4, NM, NT, NC)),
        ],
        compiler_params=pltpu.CompilerParams(vmem_limit_bytes=VMEM_LIMIT),
        name="back_substitution",
    )(*held, tab)


def solution(mesh):
    def local_step(*args):
        tab = level_table()
        return final_call(step_call(*args, tab), tab)

    spec_3d = P(None, None, "row", "col")
    spec_2d = P(None, "row", "col")
    spec_map = P("row", "col")
    return jax.shard_map(local_step, mesh=mesh, in_specs=(spec_3d,) * 4 + (spec_2d,) * 3 + (spec_map,) * 2 + (P(),), out_specs=(spec_2d,) * 3 + (spec_3d,) * 4, check_vma=False)
```
